32 devices in a mesh: dp: 8 (over z, x), head: 4 (over y, core).
Axes of the slice: x: 2, y: 2, z: 4, core: 2. Of those that a mesh axis runs over, the one named last changes fastest.
Arguments:
- tokens: bfloat16 [11840, 768], P(('dp', 'head')), may hold values from -6 to 6
- caption_len: int32 [64], P('dp'), may hold values from 5 to 40, as said below
- first_gain: bfloat16 [768], P(('dp', 'head')), may hold values from 0.5 to 1.5
- first_shift: bfloat16 [768], P(('dp', 'head')), may hold values from -3 to 3
- qkv_weight: bfloat16 [768, 3, 768], P('dp', None, 'head'), may hold values from -0.21875 to 0.21875
- qkv_bias: bfloat16 [2, 768], P(None, ('head', 'dp')), may hold values from -3 to 3
- out_weight: bfloat16 [768, 768], P(('dp', 'head')), may hold values from -1.25 to 1.25
- out_bias: bfloat16 [768], P(('dp', 'head')), may hold values from -3 to 3
- second_gain: bfloat16 [768], P(('dp', 'head')), may hold values from 0.5 to 1.5
- second_shift: bfloat16 [768], P(('dp', 'head')), may hold values from -3 to 3
- up_weight: bfloat16 [768, 3072], P('dp', 'head'), may hold values from -0.21875 to 0.21875
- up_bias: bfloat16 [3072], P(('head', 'dp')), may hold values from -3 to 3
- down_weight: bfloat16 [3072, 768], P('head', 'dp'), may hold values from -0.109375 to 0.109375
- down_bias: bfloat16 [768], P(('dp', 'head')), may hold values from -3 to 3
- output_grad: bfloat16 [11840, 768], P(('dp', 'head')), may hold values from -6 to 6
Outputs:
- layer_out: bfloat16 [11840, 768], P(('dp', 'head'))
- tokens_grad: bfloat16 [11840, 768], P(('dp', 'head'))
- first_gain_grad: float32 [768], P(('dp', 'head'))
- first_shift_grad: float32 [768], P(('dp', 'head'))
- qkv_weight_grad: float32 [768, 3, 768], P('dp', None, 'head')
- qkv_bias_grad: float32 [2, 768], P(None, ('head', 'dp'))
- out_weight_grad: float32 [768, 768], P(('dp', 'head'))
- out_bias_grad: float32 [768], P(('dp', 'head'))
- second_gain_grad: float32 [768], P(('dp', 'head'))
- second_shift_grad: float32 [768], P(('dp', 'head'))
- up_weight_grad: float32 [768, 3072], P('dp', 'head')
- up_bias_grad: float32 [3072], P(('head', 'dp'))
- down_weight_grad: float32 [3072, 768], P('head', 'dp')
- down_bias_grad: float32 [768], P(('dp', 'head'))
The draws below stay inside these ranges and needn't reach their ends.
Inputs may be any that keep to these rules, and one draw needn't show every extreme that they name: Each pair's caption fills its first caption_len slots; some pair's caption fills all 40 slots.
All inputs are finite; a program needn't handle non-finite values.
Results may differ from the reference program's by a relative error of at most 0.014.
Values may be sent and summed in bfloat16 or wider, within the bound.
No kernel may reach another device: no remote copies, remote signals or barrier semaphores. Data moves between devices by JAX's collectives and lax.ppermute only.
A program may use at most 128 MiB of HBM per device.

```python
import jax
import jax.numpy as jnp
from jax import lax

D = 768
HEADS = 12
HEAD_DIM = 64
FF = 3072
TEXT = 40
ITEMS = 8
SEQ = 185
ITEMS_ALL = 64
TOKENS = 11840
N_DP = 8


def draw_caption_len(key, part):
    lowest = max(1, TEXT // 8)
    drawn = jax.random.randint(key, (ITEMS_ALL,), lowest, TEXT + 1, dtype=jnp.int32)
    return drawn.at[0].set(TEXT)


def shard_levels(key, dims, cuts, least, high):
    def one(axis_at, parts):
        draws = jax.random.uniform(jax.random.fold_in(jax.random.fold_in(key, 6), axis_at), (parts,), jnp.float32, least / len(cuts), high / len(cuts))
        return jnp.repeat(jnp.exp(draws), dims[axis_at] // parts).reshape((-1,) + (1,) * (len(dims) - axis_at - 1))

    factor_of = one(*cuts[0])
    for cut in cuts[1:]:
        factor_of = factor_of * one(*cut)
    return factor_of


def gaussian(stream_key, dims, width, reach, cuts=(), kind=jnp.bfloat16):
    loudness = shard_levels(stream_key, dims, cuts, -0.22, 0.18) if cuts else 1.0
    array = jax.random.normal(stream_key, dims, jnp.float32) * width * loudness
    return jnp.minimum(jnp.maximum(array, -reach), reach).astype(kind)


def setup_inputs(seed: int = 0) -> dict:
    keys = jax.random.split(jax.random.key(seed), 16)
    tokens = gaussian(keys[0], (TOKENS, D), 1.0, 6.0, ((0, 32),))
    caption_len = draw_caption_len(jax.random.fold_in(keys[15], 71), 0)
    first_gain = jnp.clip(1.0 + 0.1 * jax.random.normal(keys[2], (D,), jnp.float32), 0.5, 1.5).astype(jnp.bfloat16)
    first_shift = gaussian(keys[3], (D,), 0.5, 3.0, ((0, 32),))
    qkv_weight = gaussian(keys[4], (D, 3, D), D ** -0.5, 0.21875, ((0, 8), (2, 4)))
    qkv_bias = gaussian(keys[5], (2, D), 0.5, 3.0, ((1, 32),))
    out_weight = gaussian(keys[6], (D, D), (D // 32) ** -0.5, 1.25, ((0, 32),))
    out_bias = gaussian(keys[7], (D,), 0.5, 3.0, ((0, 32),))
    second_gain = jnp.clip(1.0 + 0.1 * jax.random.normal(keys[8], (D,), jnp.float32), 0.5, 1.5).astype(jnp.bfloat16)
    second_shift = gaussian(keys[9], (D,), 0.5, 3.0, ((0, 32),))
    up_weight = gaussian(keys[10], (D, FF), D ** -0.5, 0.21875, ((0, 8), (1, 4)))
    up_bias = gaussian(keys[11], (FF,), 0.5, 3.0, ((0, 32),))
    down_weight = gaussian(keys[12], (FF, D), FF ** -0.5, 0.109375, ((0, 4), (1, 8)))
    down_bias = gaussian(keys[13], (D,), 0.5, 3.0, ((0, 32),))
    output_grad = gaussian(keys[14], (TOKENS, D), 1.0, 6.0, ((0, 32),))
    return {"tokens": tokens, "caption_len": caption_len, "first_gain": first_gain, "first_shift": first_shift, "qkv_weight": qkv_weight, "qkv_bias": qkv_bias, "out_weight": out_weight, "out_bias": out_bias, "second_gain": second_gain, "second_shift": second_shift, "up_weight": up_weight, "up_bias": up_bias, "down_weight": down_weight, "down_bias": down_bias, "output_grad": output_grad}


@jax.custom_vjp
def low(v):
    return lax.optimization_barrier(v.astype(jnp.bfloat16)).astype(jnp.float32)

@jax.custom_vjp
def low_back(v):
    return v

def low_keep(v):
    return (low(v), None)

def low_pass(kept, grad):
    return (grad,)

def back_keep(v):
    return (v, None)

def back_low(kept, grad):
    return (low(grad),)
low.defvjp(low_keep, low_pass)
low_back.defvjp(back_keep, back_low)

def norm_rows(values, gain, shift):
    centre = lax.optimization_barrier(jnp.mean(values, axis=-1, keepdims=True))
    spread = values - centre
    second = lax.optimization_barrier(jnp.mean(spread * spread, axis=-1, keepdims=True))
    return spread * lax.rsqrt(second + 1e-06) * gain + shift

def block_forward(params, tok_rows, lengths):
    first_gain, first_shift, qkv_weight, qkv_bias, out_weight, out_bias, second_gain, second_shift, up_weight, up_bias, down_weight, down_bias = params
    highest = lax.Precision.HIGHEST
    item_count = lengths.shape[0]
    normed = low(norm_rows(tok_rows, first_gain, first_shift))
    projected = jnp.dot(normed, qkv_weight.reshape(D, 3 * D), precision=highest).reshape(-1, 3, D)
    bias_rows = jnp.stack([qkv_bias[0], jnp.zeros_like(qkv_bias[0]), qkv_bias[1]])
    packed = low(low_back(projected + bias_rows)).reshape(item_count, SEQ, 3, HEADS, HEAD_DIM)
    queries = packed[:, :, 0]
    key_rows = packed[:, :, 1]
    value_rows = packed[:, :, 2]
    score_scale = HEAD_DIM ** (-0.5)
    scores = low_back(jnp.einsum('ishd,ithd->ihst', queries, key_rows, precision=highest) * score_scale)
    position = jnp.arange(SEQ, dtype=jnp.int32)
    visible = (position[None, :] >= TEXT) | (position[None, :] < lengths[:, None])
    scores = jnp.where(visible[:, None, None, :], scores, -1000000000.0)
    attn_probs = low(jax.nn.softmax(scores, axis=-1))
    context = jnp.einsum('ihst,ithd->ishd', attn_probs, value_rows, precision=highest)
    context = low(low_back(context)).reshape(item_count * SEQ, D)
    middle = tok_rows + low_back(jnp.dot(context, out_weight, precision=highest) + out_bias)
    hidden_in = low(norm_rows(middle, second_gain, second_shift))
    up_proj = low_back(jnp.dot(hidden_in, up_weight, precision=highest) + up_bias)
    active = low(jax.nn.gelu(up_proj, approximate=False))
    return middle + low_back(jnp.dot(active, down_weight, precision=highest) + down_bias)

def reference(tokens, caption_len, first_gain, first_shift, qkv_weight, qkv_bias, out_weight, out_bias, second_gain, second_shift, up_weight, up_bias, down_weight, down_bias, output_grad):
    params = tuple((member.astype(jnp.float32) for member in (first_gain, first_shift, qkv_weight, qkv_bias, out_weight, out_bias, second_gain, second_shift, up_weight, up_bias, down_weight, down_bias)))
    tok_rows = tokens.astype(jnp.float32).reshape(N_DP, ITEMS * SEQ, D)
    lengths = caption_len.reshape(N_DP, ITEMS)
    cotangent = output_grad.astype(jnp.float32).reshape(N_DP, ITEMS * SEQ, D)

    def one_block(totals, inputs):
        block_rows, block_lengths, block_grad = inputs

        def forward(weights, source):
            return block_forward(weights, source, block_lengths)
        result, pull = jax.vjp(forward, params, block_rows)
        param_grads, row_grads = pull(block_grad)
        totals = jax.tree.map(lambda running, fresh: running + fresh, totals, param_grads)
        return (totals, (result.astype(jnp.bfloat16), row_grads.astype(jnp.bfloat16)))
    initial = jax.tree.map(jnp.zeros_like, params)
    totals, (layer_out, tokens_grad) = lax.scan(one_block, initial, (tok_rows, lengths, cotangent))
    return (layer_out.reshape(N_DP * ITEMS * SEQ, D), tokens_grad.reshape(N_DP * ITEMS * SEQ, D), totals[0], totals[1], totals[2], totals[3], totals[4], totals[5], totals[6], totals[7], totals[8], totals[9], totals[10], totals[11])
```

```python
import jax
import jax.numpy as jnp
from jax import lax
from jax.sharding import PartitionSpec as P

HEAD_DIM = 64
TEXT = 40
ALL = ("dp", "head")
F32 = jnp.float32
BF16 = jnp.bfloat16


def mm(a, b):
    return jnp.dot(a, b, preferred_element_type=F32)


def mm_t(a, b):
    return lax.dot_general(a, b, (((1,), (1,)), ((), ())), preferred_element_type=F32)


def t_mm(a, b):
    return lax.dot_general(a, b, (((0,), (0,)), ((), ())), preferred_element_type=F32)


def norm_parts(values):
    spread = values - jnp.mean(values, axis=-1, keepdims=True)
    root = lax.rsqrt(jnp.mean(spread * spread, axis=-1, keepdims=True) + 1e-06)
    return spread * root, root


def norm_back(grad, gain, hat, root):
    scaled = grad * gain
    first = jnp.mean(scaled, axis=-1, keepdims=True)
    second = jnp.mean(scaled * hat, axis=-1, keepdims=True)
    return root * (scaled - first - hat * second)


def local(
    n_dp,
    n_head,
    tokens,
    caption_len,
    first_gain,
    first_shift,
    qkv_weight,
    qkv_bias,
    out_weight,
    out_bias,
    second_gain,
    second_shift,
    up_weight,
    up_bias,
    down_weight,
    down_bias,
    output_grad,
):
    rows, width = tokens.shape
    hidden = up_weight.shape[1] * n_head
    devices = n_dp * n_head
    item_count = caption_len.shape[0] // n_head
    seq = rows // item_count
    heads = width // HEAD_DIM

    def gather(piece):
        return lax.all_gather(piece, ALL, axis=0)

    per = first_gain.shape[0]
    smalls = gather(
        jnp.concatenate(
            [
                first_gain,
                first_shift,
                out_bias,
                second_gain,
                second_shift,
                down_bias,
                qkv_bias.reshape(-1),
                up_bias,
            ]
        )
    ).astype(F32)

    def plain(index):
        return smalls[:, index * per : (index + 1) * per].reshape(width)

    def by_head(piece):
        return piece.reshape(n_dp, n_head, -1).transpose(1, 0, 2).reshape(-1)

    gain_one, shift_one, b_out, gain_two, shift_two, b_down = (plain(i) for i in range(6))
    b_query = by_head(smalls[:, 6 * per : 7 * per])
    b_value = by_head(smalls[:, 7 * per : 8 * per])
    b_up = by_head(smalls[:, 8 * per :])

    w_qkv = gather(qkv_weight)
    w_out = gather(out_weight).reshape(width, width)
    w_up = gather(up_weight)
    w_down_t = gather(down_weight.T)
    w_qkv = (
        w_qkv.reshape(n_dp, n_head, width // n_dp, 3, width // n_head)
        .transpose(0, 2, 3, 1, 4)
        .reshape(width, 3 * width)
    )

    def square(tiles):
        return (
            tiles.reshape(n_dp, n_head, width // n_dp, hidden // n_head)
            .transpose(0, 2, 1, 3)
            .reshape(width, hidden)
        )

    w_up = square(w_up)
    w_down_t = square(w_down_t)

    x = tokens.astype(F32)
    hat_one, root_one = norm_parts(x)
    normed = (hat_one * gain_one + shift_one).astype(BF16)
    bias = jnp.concatenate([b_query, jnp.zeros_like(b_query), b_value])
    packed = (mm(normed, w_qkv) + bias).astype(BF16).reshape(item_count, seq, 3, heads, HEAD_DIM)
    query, key, value = packed[:, :, 0], packed[:, :, 1], packed[:, :, 2]
    mine = lax.axis_index("head") * item_count
    lengths = lax.dynamic_slice_in_dim(caption_len, mine, item_count)
    position = jnp.arange(seq, dtype=jnp.int32)
    visible = (position[None, :] >= TEXT) | (position[None, :] < lengths[:, None])
    scale = HEAD_DIM**-0.5
    scores = jnp.einsum("ishd,ithd->ihst", query, key, preferred_element_type=F32) * scale
    scores = jnp.where(visible[:, None, None, :], scores, -1000000000.0)
    probs = jax.nn.softmax(scores, axis=-1)
    probs_low = probs.astype(BF16)
    context = (
        jnp.einsum("ihst,ithd->ishd", probs_low, value, preferred_element_type=F32)
        .astype(BF16)
        .reshape(rows, width)
    )
    middle = x + (mm(context, w_out) + b_out)
    hat_two, root_two = norm_parts(middle)
    hidden_in = (hat_two * gain_two + shift_two).astype(BF16)
    up = mm(hidden_in, w_up) + b_up
    phi = 0.5 * (1.0 + lax.erf(up * (0.5**0.5)))
    active = (up * phi).astype(BF16)
    slope = phi + up * jnp.exp(-0.5 * up * up) * ((2.0 * jnp.pi) ** -0.5)
    layer_out = (middle + (mm_t(active, w_down_t) + b_down)).astype(BF16)

    grad_low = output_grad
    grad_top = output_grad.astype(F32)

    def tiles_of(matrix):
        return (
            matrix.reshape(n_dp, width // n_dp, n_head, -1)
            .transpose(0, 2, 1, 3)
            .reshape(devices, width // n_dp, -1)
        )

    def scatter(tiles):
        return lax.psum_scatter(tiles.astype(BF16), ALL, scatter_dimension=0, tiled=True)[0].astype(
            F32
        )

    g_down_t = scatter(tiles_of(t_mm(grad_low, active)))
    grad_up = (mm(grad_low, w_down_t) * slope).astype(BF16)
    g_up = scatter(tiles_of(t_mm(hidden_in, grad_up)))
    grad_hidden = mm_t(grad_up, w_up)
    grad_middle = grad_top + norm_back(grad_hidden, gain_two, hat_two, root_two)
    grad_attn = grad_middle.astype(BF16)
    g_out = scatter(t_mm(context, grad_attn).reshape(devices, width // devices, width))
    grad_context = mm_t(grad_attn, w_out).astype(BF16).reshape(item_count, seq, heads, HEAD_DIM)
    grad_probs = jnp.einsum("ishd,ithd->ihst", grad_context, value, preferred_element_type=F32)
    value_grad = jnp.einsum(
        "ihst,ishd->ithd", probs_low, grad_context, preferred_element_type=F32
    ).astype(BF16)
    grad_scores = (
        probs * (grad_probs - jnp.sum(probs * grad_probs, axis=-1, keepdims=True))
    ).astype(BF16)
    query_grad = (
        jnp.einsum("ihst,ithd->ishd", grad_scores, key, preferred_element_type=F32) * scale
    ).astype(BF16)
    key_grad = (
        jnp.einsum("ihst,ishd->ithd", grad_scores, query, preferred_element_type=F32) * scale
    ).astype(BF16)
    grad_packed = jnp.stack([query_grad, key_grad, value_grad], axis=2).reshape(rows, 3 * width)
    g_qkv = t_mm(normed, grad_packed)
    g_qkv = (
        g_qkv.reshape(n_dp, width // n_dp, 3, n_head, width // n_head)
        .transpose(0, 3, 1, 2, 4)
        .reshape(devices, width // n_dp, 3 * (width // n_head))
    )
    g_qkv = scatter(g_qkv).reshape(width // n_dp, 3, width // n_head)
    grad_normed = mm_t(grad_packed, w_qkv)
    tokens_grad = (grad_middle + norm_back(grad_normed, gain_one, hat_one, root_one)).astype(BF16)

    def total(matrix):
        return jnp.sum(matrix.astype(F32), axis=0)

    def from_head(vector):
        return vector.reshape(n_head, n_dp, -1).transpose(1, 0, 2).reshape(devices, -1)

    packed_total = total(grad_packed)
    sums = jnp.concatenate(
        [
            v.reshape(devices, per)
            for v in (
                total(grad_normed * hat_one),
                total(grad_normed),
                total(grad_attn),
                total(grad_hidden * hat_two),
                total(grad_hidden),
                total(grad_low),
            )
        ]
        + [
            from_head(packed_total[:width]),
            from_head(packed_total[2 * width :]),
            from_head(total(grad_up)),
        ],
        axis=1,
    )
    sums = lax.psum_scatter(sums, ALL, scatter_dimension=0, tiled=True)[0]

    def part(index):
        return sums[index * per : (index + 1) * per]

    return (
        layer_out,
        tokens_grad,
        part(0),
        part(1),
        g_qkv,
        sums[6 * per : 8 * per].reshape(2, per),
        g_out,
        part(2),
        part(3),
        part(4),
        g_up,
        sums[8 * per :],
        g_down_t.T,
        part(5),
    )


def solution(mesh):
    n_dp, n_head = mesh.shape["dp"], mesh.shape["head"]

    def run(*args):
        return local(n_dp, n_head, *args)

    return jax.shard_map(
        run,
        mesh=mesh,
        in_specs=(
            P(ALL, None),
            P("dp"),
            P(ALL),
            P(ALL),
            P("dp", None, "head"),
            P(None, ("head", "dp")),
            P(ALL, None),
            P(ALL),
            P(ALL),
            P(ALL),
            P("dp", "head"),
            P(("head", "dp")),
            P("head", "dp"),
            P(ALL),
            P(ALL, None),
        ),
        out_specs=(
            P(ALL, None),
            P(ALL, None),
            P(ALL),
            P(ALL),
            P("dp", None, "head"),
            P(None, ("head", "dp")),
            P(ALL, None),
            P(ALL),
            P(ALL),
            P(ALL),
            P("dp", "head"),
            P(("head", "dp")),
            P("head", "dp"),
            P(ALL),
        ),
        check_vma=False,
    )
```

```python
import jax
import jax.numpy as jnp
from jax import lax
from jax.sharding import PartitionSpec as P

HEAD_DIM = 64
TEXT = 40
ALL = ("dp", "head")
F32 = jnp.float32
BF16 = jnp.bfloat16


def mm(a, b):
    return jnp.dot(a, b, preferred_element_type=F32)


def mm_t(a, b):
    return lax.dot_general(a, b, (((1,), (1,)), ((), ())), preferred_element_type=F32)


def t_mm(a, b):
    return lax.dot_general(a, b, (((0,), (0,)), ((), ())), preferred_element_type=F32)


def norm_parts(values):
    spread = values - jnp.mean(values, axis=-1, keepdims=True)
    root = lax.rsqrt(jnp.mean(spread * spread, axis=-1, keepdims=True) + 1e-06)
    return spread * root, root


def norm_back(grad, gain, hat, root):
    scaled = grad * gain
    first = jnp.mean(scaled, axis=-1, keepdims=True)
    second = jnp.mean(scaled * hat, axis=-1, keepdims=True)
    return root * (scaled - first - hat * second)


def local(
    n_dp,
    n_head,
    tokens,
    caption_len,
    first_gain,
    first_shift,
    qkv_weight,
    qkv_bias,
    out_weight,
    out_bias,
    second_gain,
    second_shift,
    up_weight,
    up_bias,
    down_weight,
    down_bias,
    output_grad,
):
    rows, width = tokens.shape
    hidden = up_weight.shape[1] * n_head
    devices = n_dp * n_head
    item_count = caption_len.shape[0] // n_head
    seq = rows // item_count
    heads = width // HEAD_DIM

    dp_bits = [("dp", 1 << i) for i in reversed(range(n_dp.bit_length() - 1))]
    head_bits = [("head", 1 << i) for i in reversed(range(n_head.bit_length() - 1))]
    natural = head_bits + dp_bits
    order_dp = dp_bits + head_bits
    order_head = dp_bits[:-1] + head_bits[:-1] + dp_bits[-1:] + head_bits[-1:]

    def flip(piece, axis, bit):
        count = n_dp if axis == "dp" else n_head
        return lax.ppermute(piece, axis, [(i, i ^ bit) for i in range(count)])

    def my_bit(axis, bit):
        return (lax.axis_index(axis) & bit) != 0

    def gather(piece, order):
        have = []
        for step in order:
            other = flip(piece, *step)
            place = sum(natural.index(h) < natural.index(step) for h in have)
            mine = my_bit(*step)
            piece = jnp.stack(
                [jnp.where(mine, other, piece), jnp.where(mine, piece, other)], axis=place
            )
            have.append(step)
        return piece.reshape((n_head, n_dp) + piece.shape[len(natural) :])

    def scatter(tiles, order):
        tile = tiles.shape[2:]
        piece = tiles.astype(BF16).reshape((2,) * len(natural) + tile)
        have = list(natural)
        for step in reversed(order):
            place = have.index(step)
            mine = my_bit(*step).astype(jnp.int32)
            away = lax.dynamic_index_in_dim(piece, 1 - mine, place, keepdims=False)
            stay = lax.dynamic_index_in_dim(piece, mine, place, keepdims=False)
            have.remove(step)
            piece = stay.astype(F32) + flip(away, *step).astype(F32)
            if have:
                piece = piece.astype(BF16)
        return piece

    def exchange(blocks):
        return lax.all_to_all(blocks, ALL, 0, 0, tiled=True)

    per = first_gain.shape[0]
    smalls = jnp.concatenate(
        [
            first_gain,
            first_shift,
            out_bias,
            second_gain,
            second_shift,
            down_bias,
            qkv_bias.reshape(-1),
            up_bias,
        ]
    )
    smalls = exchange(jnp.broadcast_to(smalls[None], (devices,) + smalls.shape)).astype(F32)

    def plain(index):
        return smalls[:, index * per : (index + 1) * per].reshape(width)

    def by_head(piece):
        return piece.reshape(n_dp, n_head, -1).transpose(1, 0, 2).reshape(-1)

    gain_one, shift_one, b_out, gain_two, shift_two, b_down = (plain(i) for i in range(6))
    b_query = by_head(smalls[:, 6 * per : 7 * per])
    b_value = by_head(smalls[:, 7 * per : 8 * per])
    b_up = by_head(smalls[:, 8 * per :])

    part_rows = width // n_dp
    part_cols = width // n_head

    def out_pack(piece):
        return piece.reshape(-1, n_head, part_cols).transpose(1, 0, 2).reshape(part_rows, part_cols)

    pack_dp = qkv_weight[:, :2].reshape(part_rows, 2 * part_cols)
    pack_head = jnp.concatenate([qkv_weight[:, 2], out_pack(out_weight)], axis=1)
    pack_dp = gather(pack_dp, order_dp)
    pack_head = gather(pack_head, order_head)
    w_up = gather(up_weight, order_dp)
    w_down_t = gather(down_weight.T, order_head)

    def columns(tiles):
        return tiles.reshape(n_head, width, -1)

    def wide(tiles):
        return columns(tiles).transpose(1, 0, 2).reshape(width, -1)

    w_qkv = jnp.concatenate(
        [
            wide(pack_dp[..., :part_cols]),
            wide(pack_dp[..., part_cols:]),
            wide(pack_head[..., :part_cols]),
        ],
        axis=1,
    )
    w_out = (
        pack_head[..., part_cols:]
        .reshape(n_head, n_dp, n_head, part_rows // n_head, part_cols)
        .transpose(1, 0, 3, 2, 4)
        .reshape(width, width)
    )
    w_up = wide(w_up)
    w_down_t = wide(w_down_t)

    x = tokens.astype(F32)
    hat_one, root_one = norm_parts(x)
    normed = (hat_one * gain_one + shift_one).astype(BF16)
    bias = jnp.concatenate([b_query, jnp.zeros_like(b_query), b_value])
    packed = (mm(normed, w_qkv) + bias).astype(BF16).reshape(item_count, seq, 3, heads, HEAD_DIM)
    query, key, value = packed[:, :, 0], packed[:, :, 1], packed[:, :, 2]
    mine = lax.axis_index("head") * item_count
    lengths = lax.dynamic_slice_in_dim(caption_len, mine, item_count)
    position = jnp.arange(seq, dtype=jnp.int32)
    visible = (position[None, :] >= TEXT) | (position[None, :] < lengths[:, None])
    scale = HEAD_DIM**-0.5
    scores = jnp.einsum("ishd,ithd->ihst", query, key, preferred_element_type=F32) * scale
    scores = jnp.where(visible[:, None, None, :], scores, -1000000000.0)
    probs = jax.nn.softmax(scores, axis=-1)
    probs_low = probs.astype(BF16)
    context = (
        jnp.einsum("ihst,ithd->ishd", probs_low, value, preferred_element_type=F32)
        .astype(BF16)
        .reshape(rows, width)
    )
    middle = x + (mm(context, w_out) + b_out)
    hat_two, root_two = norm_parts(middle)
    hidden_in = (hat_two * gain_two + shift_two).astype(BF16)
    up = mm(hidden_in, w_up) + b_up
    phi = 0.5 * (1.0 + lax.erf(up * (0.5**0.5)))
    active = (up * phi).astype(BF16)
    slope = phi + up * jnp.exp(-0.5 * up * up) * ((2.0 * jnp.pi) ** -0.5)
    layer_out = (middle + (mm_t(active, w_down_t) + b_down)).astype(BF16)

    grad_low = output_grad
    grad_top = output_grad.astype(F32)

    def tiles_of(matrix):
        return matrix.reshape(n_dp, part_rows, n_head, -1).transpose(2, 0, 1, 3)

    g_down_t = scatter(tiles_of(t_mm(grad_low, active)), order_head)
    grad_up = (mm(grad_low, w_down_t) * slope).astype(BF16)
    g_up = scatter(tiles_of(t_mm(hidden_in, grad_up)), order_dp)
    grad_hidden = mm_t(grad_up, w_up)
    grad_middle = grad_top + norm_back(grad_hidden, gain_two, hat_two, root_two)
    grad_attn = grad_middle.astype(BF16)
    g_out = t_mm(context, grad_attn).reshape(n_dp, n_head, part_rows // n_head, width)
    g_out = scatter(g_out.transpose(1, 0, 2, 3), order_dp)
    grad_context = mm_t(grad_attn, w_out).astype(BF16).reshape(item_count, seq, heads, HEAD_DIM)
    grad_probs = jnp.einsum("ishd,ithd->ihst", grad_context, value, preferred_element_type=F32)
    value_grad = jnp.einsum(
        "ihst,ishd->ithd", probs_low, grad_context, preferred_element_type=F32
    ).astype(BF16)
    grad_scores = (
        probs * (grad_probs - jnp.sum(probs * grad_probs, axis=-1, keepdims=True))
    ).astype(BF16)
    query_grad = (
        jnp.einsum("ihst,ithd->ishd", grad_scores, key, preferred_element_type=F32) * scale
    ).astype(BF16)
    key_grad = (
        jnp.einsum("ihst,ishd->ithd", grad_scores, query, preferred_element_type=F32) * scale
    ).astype(BF16)
    grad_packed = jnp.stack([query_grad, key_grad, value_grad], axis=2).reshape(rows, 3 * width)
    g_qkv = t_mm(normed, grad_packed)
    g_qkv = g_qkv.reshape(n_dp, part_rows, 3, n_head, part_cols).transpose(3, 0, 1, 2, 4)
    half = part_rows // 2
    g_qkv = g_qkv.reshape(n_head, n_dp, part_rows, 3 * part_cols)
    g_qkv = jnp.concatenate(
        [scatter(g_qkv[:, :, :half], order_dp), scatter(g_qkv[:, :, half:], order_head)], axis=0
    ).reshape(part_rows, 3, part_cols)
    grad_normed = mm_t(grad_packed, w_qkv)
    tokens_grad = (grad_middle + norm_back(grad_normed, gain_one, hat_one, root_one)).astype(BF16)

    def total(matrix):
        return jnp.sum(matrix.astype(F32), axis=0)

    def from_head(vector):
        return vector.reshape(n_head, n_dp, -1).transpose(1, 0, 2).reshape(devices, -1)

    packed_total = total(grad_packed)
    sums = jnp.concatenate(
        [
            v.reshape(devices, per)
            for v in (
                total(grad_normed * hat_one),
                total(grad_normed),
                total(grad_attn),
                total(grad_hidden * hat_two),
                total(grad_hidden),
                total(grad_low),
            )
        ]
        + [
            from_head(packed_total[:width]),
            from_head(packed_total[2 * width :]),
            from_head(total(grad_up)),
        ],
        axis=1,
    )
    sums = jnp.sum(exchange(sums), axis=0)

    def part(index):
        return sums[index * per : (index + 1) * per]

    return (
        layer_out,
        tokens_grad,
        part(0),
        part(1),
        g_qkv,
        sums[6 * per : 8 * per].reshape(2, per),
        g_out,
        part(2),
        part(3),
        part(4),
        g_up,
        sums[8 * per :],
        g_down_t.T,
        part(5),
    )


def solution(mesh):
    n_dp, n_head = mesh.shape["dp"], mesh.shape["head"]

    def run(*args):
        return local(n_dp, n_head, *args)

    return jax.shard_map(
        run,
        mesh=mesh,
        in_specs=(
            P(ALL, None),
            P("dp"),
            P(ALL),
            P(ALL),
            P("dp", None, "head"),
            P(None, ("head", "dp")),
            P(ALL, None),
            P(ALL),
            P(ALL),
            P(ALL),
            P("dp", "head"),
            P(("head", "dp")),
            P("head", "dp"),
            P(ALL),
            P(ALL, None),
        ),
        out_specs=(
            P(ALL, None),
            P(ALL, None),
            P(ALL),
            P(ALL),
            P("dp", None, "head"),
            P(None, ("head", "dp")),
            P(ALL, None),
            P(ALL),
            P(ALL),
            P(ALL),
            P("dp", "head"),
            P(("head", "dp")),
            P("head", "dp"),
            P(ALL),
        ),
        check_vma=False,
    )
```

```python
import functools

import jax
import jax.numpy as jnp
from jax import lax
from jax.experimental.layout import Layout, with_layout_constraint
from jax.experimental import pallas as pl
from jax.experimental.pallas import tpu as pltpu
from jax.sharding import PartitionSpec as P

HEAD_DIM = 64
TEXT = 40
ALL = ("dp", "head")
F32 = jnp.float32
BF16 = jnp.bfloat16


def mm(a, b):
    return jnp.dot(a, b, preferred_element_type=F32)


def mm_t(a, b):
    return lax.dot_general(a, b, (((1,), (1,)), ((), ())), preferred_element_type=F32)


def t_mm(a, b):
    return lax.dot_general(a, b, (((0,), (0,)), ((), ())), preferred_element_type=F32)


def norm_parts(values):
    spread = values - jnp.mean(values, axis=-1, keepdims=True)
    root = lax.rsqrt(jnp.mean(spread * spread, axis=-1, keepdims=True) + 1e-06)
    return spread * root, root


def norm_back(grad, gain, hat, root):
    scaled = grad * gain
    first = jnp.mean(scaled, axis=-1, keepdims=True)
    second = jnp.mean(scaled * hat, axis=-1, keepdims=True)
    return root * (scaled - first - hat * second)


VMEM = pltpu.VMEM


def spec(shape, index):
    return pl.BlockSpec(shape, index, memory_space=VMEM)


def whole(shape):
    return spec(shape, lambda *_: (0,) * len(shape))


def chunk(shape):
    return spec((1,) + shape, lambda j, *_: (j,) + (0,) * len(shape))


def nearer(t, near, far):
    return jnp.where(t < pl.num_programs(0) // 2, near[0], far[0])


def store(t, near, far, value):
    half = pl.num_programs(0) // 2

    @pl.when(t < half)
    def _():
        near[0] = value

    @pl.when(t >= half)
    def _():
        far[0] = value


def column_sum(matrix):
    return jnp.sum(matrix.astype(F32), axis=0, keepdims=True)


def attention_forward(
    items,
    seq,
    lengths,
    order,
    x,
    vectors,
    qk_near,
    qk_far,
    vo_near,
    vo_far,
    b_qv,
    out_q,
    out_k,
    out_v,
    out_p,
    out_c,
    normed,
):
    t = pl.program_id(0)
    rows = x.shape[0] // items
    cols = out_q.shape[2]
    scale = HEAD_DIM**-0.5

    @pl.when(t == 0)
    def _():
        hat, _ = norm_parts(x[...].astype(F32))
        normed[...] = (hat * vectors[0:1, :] + vectors[1:2, :]).astype(BF16)

    bias = b_qv[order[t]]
    both = mm(normed[...], nearer(t, qk_near, qk_far))
    query = (both[:, :cols] + bias[0:1, :]).astype(BF16)
    key = both[:, cols:].astype(BF16)
    value = (mm(normed[...], nearer(t, vo_near, vo_far)[:, :cols]) + bias[1:2, :]).astype(BF16)
    out_q[0] = query
    out_k[0] = key
    out_v[0] = value
    heads = cols // HEAD_DIM
    at = lax.broadcasted_iota(jnp.int32, (rows, rows), 1)
    for item in range(items):
        mine = slice(item * rows, (item + 1) * rows)
        visible = ((at >= TEXT) & (at < seq)) | (at < lengths[item])
        parts = []
        for head in range(heads):
            lanes = slice(head * HEAD_DIM, (head + 1) * HEAD_DIM)
            scores = mm_t(query[mine, lanes], key[mine, lanes]) * scale
            scores = jnp.where(visible, scores, -1000000000.0)
            raised = jnp.exp(scores - jnp.max(scores, axis=-1, keepdims=True))
            probs = raised / jnp.sum(raised, axis=-1, keepdims=True)
            out_p[0, item * heads + head] = probs
            parts.append(mm(probs.astype(BF16), value[mine, lanes]))
        out_c[0, mine, :] = jnp.concatenate(parts, axis=1).astype(BF16)


def feed_forward(
    order,
    x,
    ctx,
    w_out,
    vectors,
    top,
    turn,
    up_near,
    up_far,
    down_near,
    down_far,
    b_up,
    out_y,
    out_gm,
    out_gc,
    out_go,
    gup_near,
    gup_far,
    gdown_near,
    gdown_far,
    out_bu,
    out_sums,
    middle,
    hat,
    root,
    hidden,
    hidden_t,
    top_t,
    sum_y,
    sum_h,
):
    t, n = pl.program_id(0), pl.program_id(1)
    chunks, _, cols = ctx.shape
    gain = vectors[3:4, :]

    def span(c):
        return pl.ds(pl.multiple_of(order[c] * cols, cols), cols)

    @pl.when((t == 0) & (n == 0))
    def _():
        total = x[...].astype(F32) + vectors[2:3, :]
        for c in range(chunks):
            total += mm(ctx[c], w_out[span(c), :])
        middle[...] = total
        hat_two, root_two = norm_parts(total)
        hat[...] = hat_two
        root[...] = root_two
        low = hat_two * gain + vectors[4:5, :]
        hidden[...] = low.astype(BF16)
        hidden_t[...] = low.T.astype(BF16)
        top_t[...] = top[...].astype(F32).T.astype(BF16)
        sum_y[...] = jnp.zeros_like(sum_y)
        sum_h[...] = jnp.zeros_like(sum_h)

    def work(up_ref, down_ref, gup, gdown):
        w_up, w_down_t = up_ref[0], down_ref[0]
        up = mm(hidden[...], w_up) + b_up[0]
        phi = 0.5 * (1.0 + lax.erf(up * (0.5**0.5)))
        active = (up * phi).astype(BF16)
        slope = phi + up * jnp.exp(-0.5 * up * up) * ((2.0 * jnp.pi) ** -0.5)
        grad_up = (mm(top[...], w_down_t) * slope).astype(BF16)
        sum_y[...] += mm_t(active, w_down_t)
        sum_h[...] += mm_t(grad_up, w_up)
        gdown[0] = mm(top_t[...], active).astype(BF16)
        gup[0] = mm(hidden_t[...], grad_up).astype(BF16)
        out_bu[0] = column_sum(grad_up)

    @pl.when(t < pl.num_programs(0) // 2)
    def _():
        work(up_near, down_near, gup_near, gdown_near)

    @pl.when(t >= pl.num_programs(0) // 2)
    def _():
        work(up_far, down_far, gup_far, gdown_far)

    @pl.when((t == pl.num_programs(0) - 1) & (n == pl.num_programs(1) - 1))
    def _():
        out_y[...] = (middle[...] + (sum_y[...] + vectors[5:6, :])).astype(BF16)
        grad_hidden = sum_h[...]
        grad_top = top[...].astype(F32)
        grad_middle = grad_top + norm_back(grad_hidden, gain, hat[...], root[...])
        out_gm[...] = grad_middle
        grad_attn = grad_middle.astype(BF16)
        out_sums[0:1, :] = column_sum(grad_attn)
        out_sums[1:2, :] = column_sum(grad_hidden * hat[...])
        out_sums[2:3, :] = column_sum(grad_hidden)
        out_sums[3:4, :] = column_sum(grad_top)
        for c in range(chunks):
            out_gc[c] = mm_t(grad_attn, w_out[span(c), :]).astype(BF16)
            grad_out = t_mm(ctx[c], grad_attn).astype(BF16)
            out_go[span(c), :] = mm_t(grad_out, turn[...]).astype(BF16)


def attention_backward(
    items,
    x,
    vectors,
    qk_near,
    qk_far,
    vo_near,
    vo_far,
    grad_out,
    query,
    key,
    value,
    probs,
    grad_ctx,
    grad_middle,
    out_x,
    gqk_near,
    gqk_far,
    gvo_near,
    gvo_far,
    out_b,
    out_sums,
    hat,
    root,
    normed_t,
    sum_n,
):
    rows = x.shape[0] // items
    cols = query.shape[2]
    heads = cols // HEAD_DIM
    scale = HEAD_DIM**-0.5
    t = pl.program_id(0)
    gain = vectors[0:1, :]

    @pl.when(t == 0)
    def _():
        hat_one, root_one = norm_parts(x[...].astype(F32))
        hat[...] = hat_one
        root[...] = root_one
        normed_t[...] = (hat_one * gain + vectors[1:2, :]).T.astype(BF16)
        sum_n[...] = jnp.zeros_like(sum_n)

    whole_q, whole_k, whole_v = [], [], []
    for item in range(items):
        mine = slice(item * rows, (item + 1) * rows)
        parts_q, parts_k, parts_v = [], [], []
        for head in range(heads):
            lanes = slice(head * HEAD_DIM, (head + 1) * HEAD_DIM)
            p = probs[0, item * heads + head]
            g = grad_ctx[0, mine, lanes]
            grad_p = mm_t(g, value[0, mine, lanes])
            parts_v.append(t_mm(p.astype(BF16), g))
            row = jnp.sum(p * grad_p, axis=-1, keepdims=True)
            grad_s = (p * (grad_p - row)).astype(BF16)
            parts_q.append(mm(grad_s, key[0, mine, lanes]) * scale)
            parts_k.append(t_mm(grad_s, query[0, mine, lanes]) * scale)
        whole_q.append(jnp.concatenate(parts_q, axis=1))
        whole_k.append(jnp.concatenate(parts_k, axis=1))
        whole_v.append(jnp.concatenate(parts_v, axis=1))
    grad_all = jnp.concatenate(
        [jnp.concatenate(parts, axis=0) for parts in (whole_q, whole_k, whole_v)], axis=1
    ).astype(BF16)
    out_b[0] = column_sum(grad_all)
    grad_qk, grad_v = grad_all[:, : 2 * cols], grad_all[:, 2 * cols :]
    store(t, gqk_near, gqk_far, mm(normed_t[...], grad_qk).astype(BF16))
    grad_weight = mm(normed_t[...], grad_v).astype(BF16)
    store(t, gvo_near, gvo_far, jnp.concatenate([grad_weight, grad_out[0]], axis=1))
    sum_n[...] += mm_t(grad_qk, nearer(t, qk_near, qk_far))
    sum_n[...] += mm_t(grad_v, nearer(t, vo_near, vo_far)[:, :cols])

    @pl.when(t == pl.num_programs(0) - 1)
    def _():
        grad_normed = sum_n[...]
        back = norm_back(grad_normed, gain, hat[...], root[...])
        out_x[...] = (grad_middle[...] + back).astype(BF16)
        out_sums[0:1, :] = column_sum(grad_normed * hat[...])
        out_sums[1:2, :] = column_sum(grad_normed)


def call(body, grid, in_specs, outs, scratch, flops, moved, *args):
    return pl.pallas_call(
        body,
        grid=grid,
        in_specs=in_specs,
        out_specs=[o[1] for o in outs],
        out_shape=[jax.ShapeDtypeStruct(*o[0]) for o in outs],
        scratch_shapes=scratch,
        compiler_params=pltpu.CompilerParams(
            dimension_semantics=("arbitrary",) * len(grid), vmem_limit_bytes=60 * 1024 * 1024
        ),
        cost_estimate=pl.CostEstimate(flops=flops, bytes_accessed=moved, transcendentals=0),
    )(*args)


def local(
    n_dp,
    n_head,
    tokens,
    caption_len,
    first_gain,
    first_shift,
    qkv_weight,
    qkv_bias,
    out_weight,
    out_bias,
    second_gain,
    second_shift,
    up_weight,
    up_bias,
    down_weight,
    down_bias,
    output_grad,
):
    rows, width = tokens.shape
    hidden = up_weight.shape[1] * n_head
    devices = n_dp * n_head
    item_count = caption_len.shape[0] // n_head
    seq = rows // item_count
    dp_bits = [("dp", 1 << i) for i in reversed(range(n_dp.bit_length() - 1))]
    head_bits = [("head", 1 << i) for i in reversed(range(n_head.bit_length() - 1))]
    held = (dp_bits + head_bits)[::-1]
    along_z, along_x, along_y = dp_bits[:-1], dp_bits[-1:], head_bits[:-1]
    core = head_bits[-1]

    def flip(piece, step):
        axis, bit = step
        count = n_dp if axis == "dp" else n_head
        rows_first = Layout(tuple(range(piece.ndim)))
        piece = with_layout_constraint(piece, rows_first)
        piece = lax.ppermute(piece, axis, [(i, i ^ bit) for i in range(count)])
        return with_layout_constraint(piece, rows_first)

    def together(*values):
        return lax.optimization_barrier(values)

    def place_of(step, have):
        return sum(held.index(h) < held.index(step) for h in have)

    def grow(piece, step, have):
        other = flip(piece, step)
        piece = jnp.stack([piece, other], axis=place_of(step, have))
        have.append(step)
        return piece

    def add(terms, which, place):
        terms = [lax.index_in_dim(term, which, place, False) for term in terms]
        return (terms[0].astype(F32) + terms[1].astype(F32)).astype(BF16)

    def shrink(terms, step, have):
        place = have.index(step)
        have.remove(step)
        near, far = add(terms, 0, place), add(terms, 1, place)
        return near, far

    def reverse_bits(value, count):
        return sum(
            ((value >> i) & 1) << (count.bit_length() - 2 - i) for i in range(count.bit_length() - 1)
        )

    my_dp, my_head = lax.axis_index("dp"), lax.axis_index("head")
    order_chunks = my_head ^ reverse_bits(jnp.arange(n_head, dtype=jnp.int32), n_head)
    order_blocks = my_dp ^ reverse_bits(jnp.arange(n_dp, dtype=jnp.int32), n_dp)

    def exchange(blocks):
        return lax.all_to_all(blocks, ALL, 0, 0, tiled=True)

    per = first_gain.shape[0]
    pieces = [first_gain, first_shift, out_bias, second_gain, second_shift, down_bias]
    pieces += [qkv_bias[0], qkv_bias[1], up_bias]
    small_size = sum(piece.shape[0] for piece in pieces)
    smalls, start = 0, 0
    for piece in pieces:
        stop = start + piece.shape[0]
        smalls += jnp.pad(piece, (start, small_size - stop))
        start = stop
    part_rows = width // n_dp
    part_cols = width // n_head
    part_hidden = up_weight.shape[1]
    part_hidden = up_weight.shape[1]
    features = jnp.arange(width, dtype=jnp.int32)
    place = jnp.repeat(order_blocks, part_rows) * part_rows + features % part_rows
    turn = (features[:, None] == place[None, :]).astype(BF16)

    def turned(piece):
        return mm(piece, turn).astype(BF16)

    def turned_back(piece):
        return mm_t(piece, turn).astype(BF16)

    ranks = order_blocks[None, :] * n_head + order_chunks[:, None]
    ranks = ranks.reshape(-1)
    chunk_of = reverse_bits(my_head ^ jnp.arange(n_head, dtype=jnp.int32), n_head)
    block_of = reverse_bits(my_dp ^ jnp.arange(n_dp, dtype=jnp.int32), n_dp)
    ranks_back = (chunk_of[None, :] * n_dp + block_of[:, None]).reshape(-1)
    padded = -(-seq // 16) * 16
    total_rows = item_count * padded

    def pad(piece):
        piece = piece.reshape(item_count, seq, width)
        return jnp.pad(piece, ((0, 0), (0, padded - seq), (0, 0))).reshape(total_rows, width)

    def unpad(piece):
        return piece.reshape(item_count, padded, width)[:, :seq].reshape(rows, width)

    def out_pack(piece):
        return piece.reshape(-1, n_head, part_cols).transpose(1, 0, 2).reshape(part_rows, part_cols)

    have, have_rest = [], []
    first = [qkv_weight.reshape(part_rows, 3 * part_cols), out_pack(out_weight)]
    first = jnp.concatenate(first, axis=1)
    rest = jnp.concatenate([up_weight, down_weight.T])
    for step in along_z[:-1]:
        first = grow(first, step, have)
    first, smalls, turn = together(first, smalls, turn)
    x, top = turned(pad(tokens)), turned(pad(output_grad))
    smalls = exchange(jnp.broadcast_to(smalls[None], (devices,) + smalls.shape))

    smalls = smalls.reshape(n_dp, n_head, -1)
    vectors = smalls[..., : 6 * per].reshape(n_dp, n_head, 6, per).transpose(2, 0, 1, 3)
    vectors = vectors.reshape(6, width)
    b_qv = smalls[..., 6 * per : 8 * per].reshape(n_dp, n_head, 2, per).transpose(1, 2, 0, 3)
    b_qv = b_qv.reshape(n_head, 2, n_dp * per).astype(F32)
    b_up = smalls[..., 8 * per :].transpose(1, 0, 2).reshape(n_head, 1, -1).astype(F32)

    first = grow(first, along_z[-1], have)
    first, rest, x, top, vectors, b_qv, b_up = together(
        first, rest, x, top, vectors, b_qv, b_up
    )
    vectors = turned(vectors).astype(F32)
    w_qk, w_vo = first[..., : 2 * part_cols], first[..., 2 * part_cols :]
    have_qk, have_vo = list(have), list(have)
    w_qk, w_vo = grow(w_qk, along_x[0], have_qk), grow(w_vo, along_y[0], have_vo)
    rest = grow(rest, along_z[0], have_rest)
    w_qk, w_vo, rest = together(w_qk, w_vo, rest)
    for step in along_z[1:-1]:
        rest = grow(rest, step, have_rest)
    for step in along_y[:-1]:
        w_qk = grow(w_qk, step, have_qk)
    for step in along_y[1:]:
        w_vo = grow(w_vo, step, have_vo)
    w_qk, w_vo = grow(w_qk, along_y[-1], have_qk), grow(w_vo, along_x[0], have_vo)
    rest = grow(rest, along_z[-1], have_rest)
    w_up, w_down = rest[..., :part_rows, :], rest[..., part_rows:, :]
    pair_shape = (-1, width, 2 * part_cols)
    near_qk, near_vo, w_up, w_down = together(
        w_qk.reshape(pair_shape), w_vo.reshape(pair_shape), w_up, w_down
    )
    far_qk, far_vo = flip(near_qk, core), flip(near_vo, core)
    have_up, have_down = list(have_rest), have_rest
    w_up_sent = flip(w_up, along_x[0])
    w_down_sent = flip(w_down, along_y[0])


    lengths = lax.dynamic_slice_in_dim(caption_len, my_head * item_count, item_count)
    pairs = item_count * (part_cols // HEAD_DIM)

    full = (total_rows, width)
    slab = (total_rows, part_cols)
    slab_out = (((n_head,) + slab, BF16), chunk(slab))
    probs_out = (((n_head, pairs, padded, padded), F32), chunk((pairs, padded, padded)))
    smem = pl.BlockSpec(memory_space=pltpu.SMEM)
    weights = width * width

    half = n_head // 2

    def near(shape):
        return spec((1,) + shape, lambda t: (jnp.minimum(t, half - 1), 0, 0))

    def far(shape):
        return spec((1,) + shape, lambda t: (jnp.maximum(t - half, 0), 0, 0))

    two_cols = (width, 2 * part_cols)
    first_specs = [near(two_cols), far(two_cols)] * 2
    query, key, value, probs, context = call(
        functools.partial(attention_forward, item_count, seq),
        (n_head,),
        [smem, smem, whole(full), whole(vectors.shape)]
        + first_specs
        + [whole(b_qv.shape)],
        [slab_out, slab_out, slab_out, probs_out, slab_out],
        [pltpu.VMEM(full, BF16)],
        8 * total_rows * weights,
        12 * weights,
        lengths,
        order_chunks,
        x,
        vectors,
        near_qk,
        far_qk,
        near_vo,
        far_vo,
        b_qv,
    )

    w_up, w_down, w_up_sent, w_down_sent, context = together(
        w_up, w_down, w_up_sent, w_down_sent, context
    )
    w_up = jnp.stack([w_up, w_up_sent], axis=place_of(along_x[0], have_up))
    w_down = jnp.stack([w_down, w_down_sent], axis=place_of(along_y[0], have_down))
    have_up.append(along_x[0])
    have_down.append(along_y[0])
    for step in along_y[:-1]:
        w_up = grow(w_up, step, have_up)
    for step in along_y[1:]:
        w_down = grow(w_down, step, have_down)
    w_up, w_down = together(w_up, w_down)
    w_up, w_down = grow(w_up, along_y[-1], have_up), grow(w_down, along_x[-1], have_down)
    w_out = jnp.concatenate([near_vo[..., part_cols:], far_vo[..., part_cols:]])
    w_out = w_out.reshape(devices, n_head, -1, part_cols).transpose(0, 2, 1, 3)
    w_out = w_out.reshape(devices, -1, width)
    w_out = turned(w_out[ranks_back].reshape(width, width))
    near_up, near_down, w_out = together(
        w_up.reshape(-1, width, part_hidden), w_down.reshape(-1, width, part_hidden), w_out
    )
    far_up, far_down = flip(near_up, core), flip(near_down, core)

    block = 256 if part_hidden % 256 == 0 else part_hidden
    steps = part_hidden // block

    def strip(index):
        return spec((1, width, block), index)

    near_strip = strip(lambda t, n: (jnp.minimum(t, half - 1), 0, jnp.where(t < half, n, steps - 1)))
    far_strip = strip(lambda t, n: (jnp.maximum(t - half, 0), 0, jnp.where(t < half, 0, n)))
    bias_out = spec((1, 1, block), lambda t, n: (t, 0, n))
    half_hidden = (half, width, part_hidden)
    (
        layer_out,
        grad_middle,
        grad_context,
        g_out,
        gup_near,
        gup_far,
        gdown_near,
        gdown_far,
        g_bu,
        sums_two,
    ) = call(
        feed_forward,
        (n_head, steps),
        [smem, whole(full), whole((n_head,) + slab), whole((width, width))]
        + [whole(vectors.shape), whole(full), whole((width, width))]
        + [near_strip, far_strip, near_strip, far_strip, bias_out],
        [
            ((full, BF16), whole(full)),
            ((full, F32), whole(full)),
            (((n_head,) + slab, BF16), whole((n_head,) + slab)),
            (((width, width), BF16), whole((width, width))),
            ((half_hidden, BF16), near_strip),
            ((half_hidden, BF16), far_strip),
            ((half_hidden, BF16), near_strip),
            ((half_hidden, BF16), far_strip),
            (((n_head, 1, part_hidden), F32), bias_out),
            (((4, width), F32), whole((4, width))),
        ],
        [
            pltpu.VMEM(full, F32),
            pltpu.VMEM(full, F32),
            pltpu.VMEM((total_rows, 1), F32),
            pltpu.VMEM(full, BF16),
            pltpu.VMEM(full[::-1], BF16),
            pltpu.VMEM(full[::-1], BF16),
            pltpu.VMEM(full, F32),
            pltpu.VMEM(full, F32),
        ],
        12 * total_rows * width * hidden,
        16 * weights,
        order_chunks,
        x,
        context,
        w_out,
        vectors,
        top,
        turn,
        near_up,
        far_up,
        near_down,
        far_down,
        b_up[order_chunks],
    )
    rest_bits = held[1:]
    shape = (2,) * len(rest_bits)
    tile = (part_rows, part_hidden)
    def pair(near, far, tile):
        return near.reshape(shape + tile), flip(far.reshape(shape + tile), core)

    down_terms = pair(gdown_near, gdown_far, tile)
    up_terms = pair(gup_near, gup_far, tile)

    have_down, have_up = list(rest_bits), list(rest_bits)
    first_x, first_y = have_down.index(along_x[0]), have_up.index(along_y[0])
    down_away = add(down_terms, 1, first_x)
    up_away = add(up_terms, 1, first_y)
    have_down.remove(along_x[0])
    have_up.remove(along_y[0])
    down_sent, up_sent = flip(down_away, along_x[0]), flip(up_away, along_y[0])
    grad_context, down_away, up_away = together(grad_context, down_away, up_away)
    g_out = g_out.reshape(devices, -1, width)[ranks]
    g_out = g_out.reshape(devices, -1, n_head, part_cols).transpose(0, 2, 1, 3)
    g_out = g_out.reshape(n_head, width, part_cols)

    tokens_grad, gqk_near, gqk_far, gvo_near, gvo_far, g_b, sums_one = call(
        functools.partial(attention_backward, item_count),
        (n_head,),
        [whole(full), whole(vectors.shape)]
        + first_specs
        + [chunk((width, part_cols))]
        + [chunk(slab)] * 3
        + [chunk((pairs, padded, padded)), chunk(slab), whole(full)],
        [
            ((full, BF16), whole(full)),
            (((half,) + two_cols, BF16), near(two_cols)),
            (((half,) + two_cols, BF16), far(two_cols)),
            (((half,) + two_cols, BF16), near(two_cols)),
            (((half,) + two_cols, BF16), far(two_cols)),
            (((n_head, 1, 3 * part_cols), F32), chunk((1, 3 * part_cols))),
            (((2, width), F32), whole((2, width))),
        ],
        [
            pltpu.VMEM(full, F32),
            pltpu.VMEM((total_rows, 1), F32),
            pltpu.VMEM(full[::-1], BF16),
            pltpu.VMEM(full, F32),
        ],
        16 * total_rows * weights,
        12 * weights,
        x,
        vectors,
        near_qk,
        far_qk,
        near_vo,
        far_vo,
        g_out,
        query,
        key,
        value,
        probs,
        grad_context,
        grad_middle,
    )
    two = (part_rows, 2 * part_cols)
    down_sent, up_sent, gqk_near, gqk_far, gvo_near, gvo_far = together(
        down_sent, up_sent, gqk_near, gqk_far, gvo_near, gvo_far
    )
    qk_terms, vo_terms = pair(gqk_near, gqk_far, two), pair(gvo_near, gvo_far, two)
    have_qk, have_vo = list(rest_bits), list(rest_bits)
    down_terms = (add(down_terms, 0, first_x), down_sent)
    up_terms = (add(up_terms, 0, first_y), up_sent)

    def descend(terms, steps, have):
        for step in steps:
            near, away = shrink(terms, step, have)
            terms = (near, flip(away, step))
        return terms

    def lockstep(*pairs):
        flat = together(*(term for terms in pairs for term in terms))
        return [tuple(flat[i : i + 2]) for i in range(0, len(flat), 2)]

    def descend_joined(one, other, axis, step, have):
        place = have.index(step)
        have.remove(step)
        near, away = (
            jnp.concatenate([add(one, which, place), add(other, which, place)], axis=axis)
            for which in (0, 1)
        )
        return near, flip(away, step)

    up_terms = descend(up_terms, along_y[1:] + along_x, have_up)
    down_terms = descend(down_terms, along_x[1:] + along_y, have_down)
    up_terms, down_terms, qk_terms, vo_terms = lockstep(up_terms, down_terms, qk_terms, vo_terms)
    qk_terms = descend(qk_terms, along_y[:1], have_qk)
    vo_terms = descend(vo_terms, along_x, have_vo)
    back_z = along_z[::-1]
    rest_terms = descend_joined(up_terms, down_terms, -2, back_z[0], have_up)
    rest_terms, qk_terms, vo_terms = lockstep(rest_terms, qk_terms, vo_terms)
    qk_terms = descend(qk_terms, along_y[1:] + along_x, have_qk)
    vo_terms = descend(vo_terms, along_y, have_vo)
    rest_terms = descend(rest_terms, back_z[1:], have_up)
    rest_terms, qk_terms, vo_terms = lockstep(rest_terms, qk_terms, vo_terms)
    first_terms = descend_joined(qk_terms, vo_terms, -1, back_z[0], have_qk)
    first_terms = descend(first_terms, back_z[1:], have_qk)
    rest = rest_terms[0].astype(F32) + rest_terms[1].astype(F32)
    g_up, g_down_t = rest[:part_rows], rest[part_rows:]
    first = first_terms[0].astype(F32) + first_terms[1].astype(F32)
    g_qkv = first[:, : 3 * part_cols].reshape(part_rows, 3, part_cols)
    g_out = first[:, 3 * part_cols :].reshape(n_head, -1, part_cols).transpose(1, 0, 2)
    g_out = g_out.reshape(out_weight.shape)
    layer_out = unpad(turned_back(layer_out))
    tokens_grad = unpad(turned_back(tokens_grad))

    sums = lax.dot_general(
        jnp.concatenate([sums_one, sums_two]),
        turn.astype(F32),
        (((1,), (1,)), ((), ())),
        precision=lax.Precision.HIGHEST,
        preferred_element_type=F32,
    )
    g_b = g_b[chunk_of].reshape(n_head, 3, n_dp, per).transpose(2, 0, 1, 3)
    g_bu = g_bu[chunk_of].reshape(n_head, n_dp, -1).transpose(1, 0, 2)
    sums = jnp.concatenate(
        [
            sums.reshape(6, devices, per).transpose(1, 0, 2).reshape(devices, 6 * per),
            g_b[:, :, ::2].reshape(devices, 2 * per),
            g_bu.reshape(devices, -1),
        ],
        axis=1,
    )
    sums = jnp.sum(exchange(sums), axis=0)

    def part(index):
        return sums[index * per : (index + 1) * per]

    return (
        layer_out,
        tokens_grad,
        part(0),
        part(1),
        g_qkv,
        sums[6 * per : 8 * per].reshape(2, per),
        g_out,
        part(2),
        part(3),
        part(4),
        g_up,
        sums[8 * per :],
        g_down_t.T,
        part(5),
    )


def solution(mesh):
    n_dp, n_head = mesh.shape["dp"], mesh.shape["head"]

    def run(*args):
        return local(n_dp, n_head, *args)

    return jax.shard_map(
        run,
        mesh=mesh,
        in_specs=(
            P(ALL, None),
            P("dp"),
            P(ALL),
            P(ALL),
            P("dp", None, "head"),
            P(None, ("head", "dp")),
            P(ALL, None),
            P(ALL),
            P(ALL),
            P(ALL),
            P("dp", "head"),
            P(("head", "dp")),
            P("head", "dp"),
            P(ALL),
            P(ALL, None),
        ),
        out_specs=(
            P(ALL, None),
            P(ALL, None),
            P(ALL),
            P(ALL),
            P("dp", None, "head"),
            P(None, ("head", "dp")),
            P(ALL, None),
            P(ALL),
            P(ALL),
            P(ALL),
            P("dp", "head"),
            P(("head", "dp")),
            P("head", "dp"),
            P(ALL),
        ),
        check_vma=False,
    )
```

```python
import functools

import jax
import jax.numpy as jnp
from jax import lax
from jax.experimental.layout import Layout, with_layout_constraint
from jax.experimental import pallas as pl
from jax.experimental.pallas import tpu as pltpu
from jax.sharding import PartitionSpec as P

HEAD_DIM = 64
TEXT = 40
ALL = ("dp", "head")
F32 = jnp.float32
BF16 = jnp.bfloat16


def mm(a, b):
    return jnp.dot(a, b, preferred_element_type=F32)


def mm_t(a, b):
    return lax.dot_general(a, b, (((1,), (1,)), ((), ())), preferred_element_type=F32)


def t_mm(a, b):
    return lax.dot_general(a, b, (((0,), (0,)), ((), ())), preferred_element_type=F32)


def norm_parts(values):
    spread = values - jnp.mean(values, axis=-1, keepdims=True)
    root = lax.rsqrt(jnp.mean(spread * spread, axis=-1, keepdims=True) + 1e-06)
    return spread * root, root


def norm_back(grad, gain, hat, root):
    scaled = grad * gain
    first = jnp.mean(scaled, axis=-1, keepdims=True)
    second = jnp.mean(scaled * hat, axis=-1, keepdims=True)
    return root * (scaled - first - hat * second)


VMEM = pltpu.VMEM


def spec(shape, index):
    return pl.BlockSpec(shape, index, memory_space=VMEM)


def whole(shape):
    return spec(shape, lambda *_: (0,) * len(shape))


def chunk(shape):
    return spec((1,) + shape, lambda j, *_: (j,) + (0,) * len(shape))


def nearer(t, near, far):
    return jnp.where(t < pl.num_programs(0) // 2, near[0], far[0])


def store(t, near, far, value):
    half = pl.num_programs(0) // 2

    @pl.when(t < half)
    def _():
        near[0] = value

    @pl.when(t >= half)
    def _():
        far[0] = value


def column_sum(matrix):
    return jnp.sum(matrix.astype(F32), axis=0, keepdims=True)


def counting(shape, axis):
    return lax.broadcasted_iota(jnp.int32, shape, axis)


def repeats(part, size):
    return (counting((part, size), 1) % part == counting((part, size), 0)).astype(F32)


def owners(devices, part, size):
    return counting((devices, size), 1) // part, counting((devices, size), 0)


def spread_vectors(per, order, smalls, turn, vectors, b_qv, b_up):
    devices, width = smalls.shape[0], turn.shape[0]
    chunks, _, part = b_up.shape
    values = smalls[...].astype(F32)
    plain = vectors.shape[0]
    pattern = repeats(per, width).astype(BF16)
    block, device = owners(devices, per, width)
    rows = []
    for v in range(plain):
        row = mm(values[:, v * per : (v + 1) * per].astype(BF16), pattern)
        rows.append(jnp.sum(jnp.where(block == device, row, 0.0), axis=0, keepdims=True))
    vectors[...] = mm(jnp.concatenate(rows, axis=0).astype(BF16), turn[...])

    def by_chunk(first, size, length, out):
        tall = mm(
            values[:, first : first + size].astype(BF16), repeats(size, length).astype(BF16)
        )
        block, device = owners(devices, size, length)
        for t in range(chunks):
            mine = device == block * chunks + order[t]
            out(t, jnp.sum(jnp.where(mine, tall, 0.0), axis=0, keepdims=True))

    def set_query(t, row):
        b_qv[t, 0:1, :] = row

    def set_value(t, row):
        b_qv[t, 1:2, :] = row

    def set_up(t, row):
        b_up[t] = row

    cols = b_qv.shape[2]
    by_chunk(plain * per, per, cols, set_query)
    by_chunk((plain + 1) * per, per, cols, set_value)
    by_chunk((plain + 2) * per, values.shape[1] - (plain + 2) * per, part, set_up)


def collect_vectors(per, order, sums_one, sums_two, g_b, g_bu, turn, out):
    devices, width = out.shape[0], turn.shape[0]
    chunks, _, part = g_bu.shape

    def exact(a, b):
        dims = (((1,), (1,)), ((), ()))
        return lax.dot_general(
            a, b, dims, precision=lax.Precision.HIGHEST, preferred_element_type=F32
        )

    plain = sums_one.shape[0] + sums_two.shape[0]
    rows = jnp.concatenate([sums_one[...], sums_two[...]], axis=0)
    rows = exact(rows, turn[...].astype(F32))
    block, device = owners(devices, per, width)
    tall = [jnp.where(block == device, rows[v : v + 1, :], 0.0) for v in range(plain)]
    tall = exact(jnp.concatenate(tall, axis=0), repeats(per, width))
    columns = [tall[v * devices : (v + 1) * devices, :] for v in range(plain)]

    def by_chunk(row_of, size, length):
        block, device = owners(devices, size, length)
        tall = jnp.zeros((devices, length), F32)
        for t in range(chunks):
            tall = jnp.where(device == block * chunks + order[t], row_of(t), tall)
        columns.append(exact(tall, repeats(size, length)))

    cols = g_b.shape[2] // 3
    by_chunk(lambda t: g_b[t][:, :cols], per, cols)
    by_chunk(lambda t: g_b[t][:, 2 * cols :], per, cols)
    by_chunk(lambda t: g_bu[t], out.shape[1] - (plain + 2) * per, part)
    out[...] = jnp.concatenate(columns, axis=1)


def attention_forward(
    items,
    seq,
    lengths,
    order,
    x,
    vectors,
    qk_near,
    qk_far,
    vo_near,
    vo_far,
    b_qv,
    out_q,
    out_k,
    out_v,
    out_p,
    out_c,
    normed,
):
    t = pl.program_id(0)
    rows = x.shape[0] // items
    cols = out_q.shape[2]
    scale = HEAD_DIM**-0.5

    @pl.when(t == 0)
    def _():
        hat, _ = norm_parts(x[...].astype(F32))
        normed[...] = (hat * vectors[0:1, :] + vectors[1:2, :]).astype(BF16)

    bias = b_qv[t]
    both = mm(normed[...], nearer(t, qk_near, qk_far))
    query = (both[:, :cols] + bias[0:1, :]).astype(BF16)
    key = both[:, cols:].astype(BF16)
    value = (mm(normed[...], nearer(t, vo_near, vo_far)[:, :cols]) + bias[1:2, :]).astype(BF16)
    out_q[0] = query
    out_k[0] = key
    out_v[0] = value
    heads = cols // HEAD_DIM
    at = lax.broadcasted_iota(jnp.int32, (rows, rows), 1)
    for item in range(items):
        mine = slice(item * rows, (item + 1) * rows)
        visible = ((at >= TEXT) & (at < seq)) | (at < lengths[item])
        parts = []
        for head in range(heads):
            lanes = slice(head * HEAD_DIM, (head + 1) * HEAD_DIM)
            scores = mm_t(query[mine, lanes], key[mine, lanes]) * scale
            scores = jnp.where(visible, scores, -1000000000.0)
            raised = jnp.exp(scores - jnp.max(scores, axis=-1, keepdims=True))
            probs = raised / jnp.sum(raised, axis=-1, keepdims=True)
            out_p[0, item * heads + head] = probs
            parts.append(mm(probs.astype(BF16), value[mine, lanes]))
        out_c[0, mine, :] = jnp.concatenate(parts, axis=1).astype(BF16)


def chunk_rows(order, c, cols):
    return pl.ds(pl.multiple_of(order[c] * cols, cols), cols)


def between(order, x, ctx, w_out, vectors, top, middle, hidden, hidden_t, top_t):
    chunks, _, cols = ctx.shape
    total = x[...].astype(F32) + vectors[2:3, :]
    for c in range(chunks):
        total += mm(ctx[c], w_out[chunk_rows(order, c, cols), :])
    middle[...] = total
    hat, _ = norm_parts(total)
    low = hat * vectors[3:4, :] + vectors[4:5, :]
    hidden[...] = low.astype(BF16)
    hidden_t[...] = low.T.astype(BF16)
    top_t[...] = top[...].astype(F32).T.astype(BF16)


def feed_forward(
    last,
    hidden,
    hidden_t,
    top,
    top_t,
    *rest,
):
    ups, downs, b_up, rest = rest[:4], rest[4:8], rest[8], rest[9:]
    if last:
        in_y, in_h, order, middle, w_out, vectors = rest[:6]
        rest = rest[6:]
    gup_near, gup_far, gdown_near, gdown_far, out_bu = rest[:5]
    if last:
        out_y, out_gm, out_ga, out_gc, out_sums, sum_y, sum_h = rest[5:]
    else:
        sum_y, sum_h = rest[5:]
    t, n = pl.program_id(0), pl.program_id(1)

    @pl.when((t == 0) & (n == 0))
    def _():
        if last:
            sum_y[...] = in_y[...]
            sum_h[...] = in_h[...]
        else:
            sum_y[...] = jnp.zeros_like(sum_y)
            sum_h[...] = jnp.zeros_like(sum_h)

    def work(up_refs, down_refs, gup, gdown):
        w_up = jnp.concatenate([ref[...] for ref in up_refs], axis=0)
        w_down_t = jnp.concatenate([ref[...] for ref in down_refs], axis=0)
        up = mm(hidden[...], w_up) + b_up[0]
        phi = 0.5 * (1.0 + lax.erf(up * (0.5**0.5)))
        active = (up * phi).astype(BF16)
        slope = phi + up * jnp.exp(-0.5 * up * up) * ((2.0 * jnp.pi) ** -0.5)
        grad_up = (mm(top[...], w_down_t) * slope).astype(BF16)
        sum_y[...] += mm_t(active, w_down_t)
        sum_h[...] += mm_t(grad_up, w_up)
        gdown[...] = mm(top_t[...], active).astype(BF16)
        gup[...] = mm(hidden_t[...], grad_up).astype(BF16)
        out_bu[0] = column_sum(grad_up)

    @pl.when(t == 0)
    def _():
        work(ups[:2], downs[:2], gup_near, gdown_near)

    @pl.when(t == 1)
    def _():
        work(ups[2:], downs[2:], gup_far, gdown_far)

    if not last:
        return

    @pl.when((t == 1) & (n == pl.num_programs(1) - 1))
    def _():
        chunks, _, cols = out_gc.shape
        gain = vectors[3:4, :]
        hat, root = norm_parts(middle[...])
        out_y[...] = (middle[...] + (sum_y[...] + vectors[5:6, :])).astype(BF16)
        grad_hidden = sum_h[...]
        grad_top = top[...].astype(F32)
        grad_middle = grad_top + norm_back(grad_hidden, gain, hat, root)
        out_gm[...] = grad_middle
        grad_attn = grad_middle.astype(BF16)
        out_ga[...] = grad_attn
        out_sums[0:1, :] = column_sum(grad_attn)
        out_sums[1:2, :] = column_sum(grad_hidden * hat)
        out_sums[2:3, :] = column_sum(grad_hidden)
        out_sums[3:4, :] = column_sum(grad_top)
        for c in range(chunks):
            out_gc[c] = mm_t(grad_attn, w_out[chunk_rows(order, c, cols), :]).astype(BF16)


def out_gradient(order, ctx, grad_attn, turn, out_go):
    chunks, _, cols = ctx.shape
    for c in range(chunks):
        grad_out = t_mm(ctx[c], grad_attn[...]).astype(BF16)
        out_go[chunk_rows(order, c, cols), :] = mm_t(grad_out, turn[...]).astype(BF16)


def attention_backward(
    items,
    x,
    vectors,
    qk_near,
    qk_far,
    vo_near,
    vo_far,
    query,
    key,
    value,
    probs,
    grad_ctx,
    grad_middle,
    out_x,
    gqk_near,
    gqk_far,
    gvo_near,
    gvo_far,
    out_b,
    out_sums,
    hat,
    root,
    normed_t,
    sum_n,
):
    rows = x.shape[0] // items
    cols = query.shape[2]
    heads = cols // HEAD_DIM
    scale = HEAD_DIM**-0.5
    t = pl.program_id(0)
    gain = vectors[0:1, :]

    @pl.when(t == 0)
    def _():
        hat_one, root_one = norm_parts(x[...].astype(F32))
        hat[...] = hat_one
        root[...] = root_one
        normed_t[...] = (hat_one * gain + vectors[1:2, :]).T.astype(BF16)
        sum_n[...] = jnp.zeros_like(sum_n)

    whole_q, whole_k, whole_v = [], [], []
    for item in range(items):
        mine = slice(item * rows, (item + 1) * rows)
        parts_q, parts_k, parts_v = [], [], []
        for head in range(heads):
            lanes = slice(head * HEAD_DIM, (head + 1) * HEAD_DIM)
            p = probs[0, item * heads + head]
            g = grad_ctx[0, mine, lanes]
            grad_p = mm_t(g, value[0, mine, lanes])
            parts_v.append(t_mm(p.astype(BF16), g))
            row = jnp.sum(p * grad_p, axis=-1, keepdims=True)
            grad_s = (p * (grad_p - row)).astype(BF16)
            parts_q.append(mm(grad_s, key[0, mine, lanes]) * scale)
            parts_k.append(t_mm(grad_s, query[0, mine, lanes]) * scale)
        whole_q.append(jnp.concatenate(parts_q, axis=1))
        whole_k.append(jnp.concatenate(parts_k, axis=1))
        whole_v.append(jnp.concatenate(parts_v, axis=1))
    grad_all = jnp.concatenate(
        [jnp.concatenate(parts, axis=0) for parts in (whole_q, whole_k, whole_v)], axis=1
    ).astype(BF16)
    out_b[0] = column_sum(grad_all)
    grad_qk, grad_v = grad_all[:, : 2 * cols], grad_all[:, 2 * cols :]
    store(t, gqk_near, gqk_far, mm(normed_t[...], grad_qk).astype(BF16))
    grad_weight = mm(normed_t[...], grad_v).astype(BF16)
    store(t, gvo_near, gvo_far, grad_weight)
    sum_n[...] += mm_t(grad_qk, nearer(t, qk_near, qk_far))
    sum_n[...] += mm_t(grad_v, nearer(t, vo_near, vo_far)[:, :cols])

    @pl.when(t == pl.num_programs(0) - 1)
    def _():
        grad_normed = sum_n[...]
        back = norm_back(grad_normed, gain, hat[...], root[...])
        out_x[...] = (grad_middle[...] + back).astype(BF16)
        out_sums[0:1, :] = column_sum(grad_normed * hat[...])
        out_sums[1:2, :] = column_sum(grad_normed)


def call(body, grid, in_specs, outs, scratch, flops, moved, *args):
    return pl.pallas_call(
        body,
        grid=grid,
        in_specs=in_specs,
        out_specs=[o[1] for o in outs],
        out_shape=[jax.ShapeDtypeStruct(*o[0]) for o in outs],
        scratch_shapes=scratch,
        compiler_params=pltpu.CompilerParams(
            dimension_semantics=("arbitrary",) * len(grid), vmem_limit_bytes=60 * 1024 * 1024
        ),
        cost_estimate=pl.CostEstimate(flops=flops // 8, bytes_accessed=moved // 8, transcendentals=0),
    )(*args)


def local(
    n_dp,
    n_head,
    tokens,
    caption_len,
    first_gain,
    first_shift,
    qkv_weight,
    qkv_bias,
    out_weight,
    out_bias,
    second_gain,
    second_shift,
    up_weight,
    up_bias,
    down_weight,
    down_bias,
    output_grad,
):
    rows, width = tokens.shape
    hidden = up_weight.shape[1] * n_head
    devices = n_dp * n_head
    item_count = caption_len.shape[0] // n_head
    seq = rows // item_count
    dp_bits = [("dp", 1 << i) for i in reversed(range(n_dp.bit_length() - 1))]
    head_bits = [("head", 1 << i) for i in reversed(range(n_head.bit_length() - 1))]
    held = (dp_bits + head_bits)[::-1]
    along_z, along_x, along_y = dp_bits[:-1], dp_bits[-1:], head_bits[:-1]
    core = head_bits[-1]

    def flip(piece, step):
        axis, bit = step
        count = n_dp if axis == "dp" else n_head
        rows_first = Layout(tuple(range(piece.ndim)))
        piece = with_layout_constraint(piece, rows_first)
        piece = lax.ppermute(piece, axis, [(i, i ^ bit) for i in range(count)])
        return with_layout_constraint(piece, rows_first)

    def together(*values):
        return lax.optimization_barrier(values)

    def place_of(step, have):
        return sum(held.index(h) < held.index(step) for h in have)

    def grow(piece, step, have):
        other = flip(piece, step)
        piece = jnp.stack([piece, other], axis=place_of(step, have))
        have.append(step)
        return piece

    def side(terms, which, place):
        return [lax.index_in_dim(term, which, place, False) for term in terms]

    def total(terms):
        return sum(term.astype(F32) for term in terms)

    def shrink(terms, step, have):
        place = have.index(step)
        have.remove(step)
        away = total(side(terms, 1, place)).astype(BF16)
        return side(terms, 0, place) + [flip(away, step)]

    def reverse_bits(value, count):
        return sum(
            ((value >> i) & 1) << (count.bit_length() - 2 - i) for i in range(count.bit_length() - 1)
        )

    my_dp, my_head = lax.axis_index("dp"), lax.axis_index("head")
    order_chunks = my_head ^ reverse_bits(jnp.arange(n_head, dtype=jnp.int32), n_head)
    order_blocks = my_dp ^ reverse_bits(jnp.arange(n_dp, dtype=jnp.int32), n_dp)

    def exchange(blocks):
        return lax.all_to_all(blocks, ALL, 0, 0, tiled=True)

    per = first_gain.shape[0]
    smem = pl.BlockSpec(memory_space=pltpu.SMEM)
    pieces = [first_gain, first_shift, out_bias, second_gain, second_shift, down_bias]
    pieces += [qkv_bias[0], qkv_bias[1], up_bias]
    small_size = sum(piece.shape[0] for piece in pieces)
    smalls, start = 0, 0
    for piece in pieces:
        stop = start + piece.shape[0]
        smalls += jnp.pad(piece, (start, small_size - stop))
        start = stop
    part_rows = width // n_dp
    part_cols = width // n_head
    part_hidden = up_weight.shape[1]
    part_hidden = up_weight.shape[1]
    features = jnp.arange(width, dtype=jnp.int32)
    place = jnp.repeat(order_blocks, part_rows) * part_rows + features % part_rows
    turn = (features[:, None] == place[None, :]).astype(BF16)

    def turned(piece):
        return mm(piece, turn).astype(BF16)

    def turned_back(piece):
        return mm_t(piece, turn).astype(BF16)

    ranks = order_blocks[None, :] * n_head + order_chunks[:, None]
    ranks = ranks.reshape(-1)
    chunk_of = reverse_bits(my_head ^ jnp.arange(n_head, dtype=jnp.int32), n_head)
    block_of = reverse_bits(my_dp ^ jnp.arange(n_dp, dtype=jnp.int32), n_dp)
    ranks_back = (chunk_of[None, :] * n_dp + block_of[:, None]).reshape(-1)
    padded = -(-seq // 16) * 16
    total_rows = item_count * padded

    def pad(piece):
        piece = piece.reshape(item_count, seq, width)
        return jnp.pad(piece, ((0, 0), (0, padded - seq), (0, 0))).reshape(total_rows, width)

    def unpad(piece):
        return piece.reshape(item_count, padded, width)[:, :seq].reshape(rows, width)

    def out_pack(piece):
        return piece.reshape(-1, n_head, part_cols).transpose(1, 0, 2).reshape(part_rows, part_cols)

    have, have_rest = [], []
    first = [qkv_weight.reshape(part_rows, 3 * part_cols), out_pack(out_weight)]
    first = jnp.concatenate(first, axis=1)
    rest = jnp.concatenate([up_weight, down_weight.T])
    for step in along_z[:-1]:
        first = grow(first, step, have)
    first, smalls, turn = together(first, smalls, turn)
    x, top = turned(pad(tokens)), turned(pad(output_grad))
    smalls = exchange(jnp.broadcast_to(smalls[None], (devices,) + smalls.shape))

    part_cols = width // n_head
    vectors, b_qv, b_up = call(
        functools.partial(spread_vectors, per),
        (1,),
        [smem, whole(smalls.shape), whole((width, width))],
        [
            (((6, width), F32), whole((6, width))),
            (((n_head, 2, part_cols), F32), whole((n_head, 2, part_cols))),
            (((n_head, 1, hidden // n_head), F32), whole((n_head, 1, hidden // n_head))),
        ],
        [],
        0,
        4 * width * width,
        order_chunks,
        smalls,
        turn,
    )
    first = grow(first, along_z[-1], have)
    first, rest, x, top = together(first, rest, x, top)
    w_qk, w_vo = first[..., : 2 * part_cols], first[..., 2 * part_cols :]
    have_qk, have_vo = list(have), list(have)
    w_qk, w_vo = grow(w_qk, along_x[0], have_qk), grow(w_vo, along_y[0], have_vo)
    rest = grow(rest, along_z[0], have_rest)
    w_qk, w_vo, rest, vectors, b_qv, b_up = together(w_qk, w_vo, rest, vectors, b_qv, b_up)
    for step in along_z[1:-1]:
        rest = grow(rest, step, have_rest)
    for step in along_y[:-1]:
        w_qk = grow(w_qk, step, have_qk)
    for step in along_y[1:]:
        w_vo = grow(w_vo, step, have_vo)
    w_qk, w_vo = grow(w_qk, along_y[-1], have_qk), grow(w_vo, along_x[0], have_vo)
    rest = grow(rest, along_z[-1], have_rest)
    w_up, w_down = rest[..., :part_rows, :], rest[..., part_rows:, :]
    pair_shape = (-1, width, 2 * part_cols)
    near_qk, near_vo, w_up, w_down = together(
        w_qk.reshape(pair_shape), w_vo.reshape(pair_shape), w_up, w_down
    )
    far_qk, far_vo = flip(near_qk, core), flip(near_vo, core)
    step_x, step_y = along_x[0], along_y[0]
    up_x, down_x = flip(w_up, step_x), flip(w_down, step_x)
    up_y, down_y = flip(w_up, step_y), flip(w_down, step_y)


    lengths = lax.dynamic_slice_in_dim(caption_len, my_head * item_count, item_count)
    pairs = item_count * (part_cols // HEAD_DIM)

    full = (total_rows, width)
    slab = (total_rows, part_cols)
    slab_out = (((n_head,) + slab, BF16), chunk(slab))
    probs_out = (((n_head, pairs, padded, padded), F32), chunk((pairs, padded, padded)))
    weights = width * width

    half = n_head // 2

    def near(shape):
        return spec((1,) + shape, lambda t: (jnp.minimum(t, half - 1), 0, 0))

    def far(shape):
        return spec((1,) + shape, lambda t: (jnp.maximum(t - half, 0), 0, 0))

    two_cols, one_col = (width, 2 * part_cols), (width, part_cols)
    first_specs = [near(two_cols), far(two_cols)] * 2
    query, key, value, probs, context = call(
        functools.partial(attention_forward, item_count, seq),
        (n_head,),
        [smem, smem, whole(full), whole(vectors.shape)]
        + first_specs
        + [whole(b_qv.shape)],
        [slab_out, slab_out, slab_out, probs_out, slab_out],
        [pltpu.VMEM(full, BF16)],
        8 * total_rows * weights,
        12 * weights,
        lengths,
        order_chunks,
        x,
        vectors,
        near_qk,
        far_qk,
        near_vo,
        far_vo,
        b_qv,
    )

    w_out = jnp.concatenate([near_vo[..., part_cols:], far_vo[..., part_cols:]])
    w_out = w_out.reshape(devices, n_head, -1, part_cols).transpose(0, 2, 1, 3)
    w_out = w_out.reshape(devices, -1, width)
    w_out = turned(w_out[ranks_back].reshape(width, width))
    middle, low, low_t, top_t = call(
        between,
        (1,),
        [smem, whole(full), whole((n_head,) + slab), whole((width, width))]
        + [whole(vectors.shape), whole(full)],
        [
            ((full, F32), whole(full)),
            ((full, BF16), whole(full)),
            ((full[::-1], BF16), whole(full[::-1])),
            ((full[::-1], BF16), whole(full[::-1])),
        ],
        [],
        2 * total_rows * weights,
        8 * weights,
        order_chunks,
        x,
        context,
        w_out,
        vectors,
        top,
    )

    up_x, down_x, up_y, down_y, low = together(up_x, down_x, up_y, down_y, low)
    up_d, down_d = flip(up_x, step_y), flip(down_y, step_x)
    own = [w_up, up_x, w_down, down_x]
    own_far = [flip(piece, core) for piece in own]
    other = [up_y, up_d, down_y, down_d]
    early_far = [flip(piece, core) for piece in other[::2]]
    *own_far, late_0, late_1 = together(*own_far, *early_far)
    early_far = [late_0, late_1]

    def arranged(near, far):
        pieces = near[:2] + far[:2] + near[2:] + far[2:]
        return [piece.reshape(-1, part_hidden) for piece in pieces]

    steps, block = 1, part_hidden
    bias_strip = spec((1, 1, block), lambda t, n: (t, 0, n))
    b_up = b_up.reshape(2, half, 1, part_hidden)
    strips = [whole((width // 2, part_hidden))] * 8
    strip_outs = [(((width, part_hidden), BF16), whole((width, part_hidden)))] * 4
    strip_outs += [(((2, 1, part_hidden), F32), bias_strip)]
    cost = 6 * total_rows * width * hidden, 10 * weights
    *g_own, gb_own, sum_y, sum_h = call(
        functools.partial(feed_forward, False),
        (2, steps),
        [whole(full), whole(full[::-1])] * 2 + strips + [bias_strip],
        strip_outs + [((full, F32), whole(full))] * 2,
        [],
        *cost,
        low,
        low_t,
        top,
        top_t,
        *arranged(own, own_far),
        b_up[:, 0],
    )
    other[1], other[3], sum_y = together(other[1], other[3], sum_y)
    late_far = [flip(piece, core) for piece in other[1::2]]
    other_far = [early_far[0], late_far[0], early_far[1], late_far[1]]

    rest_bits = held[1:]
    shape = (2,) * len(rest_bits)
    tile = (part_rows, part_hidden)

    def pair(near, far, tile):
        near = near.reshape(shape[1:] + tile)
        return [near, flip(far.reshape(near.shape), core)]

    gup_own, gdown_own = pair(*g_own[:2], tile), pair(*g_own[2:], tile)
    *g_other, gb_other, layer_out, grad_middle, grad_attn, grad_context, sums_two = call(
        functools.partial(feed_forward, True),
        (2, steps),
        [whole(full), whole(full[::-1])] * 2
        + strips
        + [bias_strip, whole(full), whole(full), smem, whole(full)]
        + [whole((width, width)), whole(vectors.shape)],
        strip_outs
        + [
            ((full, BF16), whole(full)),
            ((full, F32), whole(full)),
            ((full, BF16), whole(full)),
            (((n_head,) + slab, BF16), whole((n_head,) + slab)),
            (((4, width), F32), whole((4, width))),
        ],
        [pltpu.VMEM(full, F32), pltpu.VMEM(full, F32)],
        *cost,
        low,
        low_t,
        top,
        top_t,
        *arranged(other, other_far),
        b_up[:, 1],
        sum_y,
        sum_h,
        order_chunks,
        middle,
        w_out,
        vectors,
    )
    g_bu = jnp.stack([gb_own, gb_other], axis=1).reshape(n_head, 1, part_hidden)
    gup_other, gdown_other = pair(*g_other[:2], tile), pair(*g_other[2:], tile)

    def low_total(terms):
        return total(terms).astype(BF16)

    away = [
        low_total(side(gdown_own, 1, 0)),
        low_total(side(gup_other, 1, 0)),
        low_total(side(gdown_other, 1, 0)),
        low_total(side(gup_other, 0, 0)),
    ]
    down_01, up_11 = flip(away[0], step_x), flip(away[1], step_y)
    down_11, up_10 = flip(away[2], step_x), flip(away[3], step_y)
    grad_context, *_ = together(grad_context, *away)
    tokens_grad, gqk_near, gqk_far, gvo_near, gvo_far, g_b, sums_one = call(
        functools.partial(attention_backward, item_count),
        (n_head,),
        [whole(full), whole(vectors.shape)]
        + first_specs
        + [chunk(slab)] * 3
        + [chunk((pairs, padded, padded)), chunk(slab), whole(full)],
        [
            ((full, BF16), whole(full)),
            (((half,) + two_cols, BF16), near(two_cols)),
            (((half,) + two_cols, BF16), far(two_cols)),
            (((half,) + one_col, BF16), near(one_col)),
            (((half,) + one_col, BF16), far(one_col)),
            (((n_head, 1, 3 * part_cols), F32), chunk((1, 3 * part_cols))),
            (((2, width), F32), whole((2, width))),
        ],
        [
            pltpu.VMEM(full, F32),
            pltpu.VMEM((total_rows, 1), F32),
            pltpu.VMEM(full[::-1], BF16),
            pltpu.VMEM(full, F32),
        ],
        16 * total_rows * weights,
        12 * weights,
        x,
        vectors,
        near_qk,
        far_qk,
        near_vo,
        far_vo,
        query,
        key,
        value,
        probs,
        grad_context,
        grad_middle,
    )
    two = (part_rows, 2 * part_cols)
    down_01, up_11, down_11, up_10, gqk_near, gqk_far, gvo_near, gvo_far = together(
        down_01, up_11, down_11, up_10, gqk_near, gqk_far, gvo_near, gvo_far
    )

    def pair_first(near, far):
        return [near.reshape(shape + two), flip(far.reshape(shape + two), core)]

    away_up = low_total(side(gup_own, 1, 0) + [up_11])
    away_down = low_total(side(gdown_other, 0, 0) + [down_11])
    up_01, down_10 = flip(away_up, step_x), flip(away_down, step_y)
    qk_terms = pair_first(gqk_near, gqk_far)
    grad_attn, *_ = together(grad_attn, away_up, away_down, gqk_far)
    (g_out,) = call(
        out_gradient,
        (1,),
        [smem, whole((n_head,) + slab), whole(full), whole((width, width))],
        [(((width, width), BF16), whole((width, width)))],
        [],
        0,
        0,
        order_chunks,
        context,
        grad_attn,
        turn,
    )
    g_out = g_out.reshape(devices, -1, width)[ranks]
    g_out = g_out.reshape(devices, -1, n_head, part_cols).transpose(0, 2, 1, 3)
    g_out = g_out.reshape(n_head, width, part_cols)
    gvo_near = jnp.concatenate([gvo_near, g_out[:half]], axis=2)
    gvo_far = jnp.concatenate([gvo_far, g_out[half:]], axis=2)
    up_01, down_10, gvo_near, gvo_far, *qk_terms = together(
        up_01, down_10, gvo_near, gvo_far, *qk_terms
    )
    vo_terms = pair_first(gvo_near, gvo_far)
    have_qk, have_vo = list(rest_bits), list(rest_bits)
    up_terms = side(gup_own, 0, 0) + [up_10, up_01]
    down_terms = side(gdown_own, 0, 0) + [down_01, down_10]
    have_up = list(dp_bits[:-1][::-1])

    def descend(terms, steps, have):
        for step in steps:
            terms = shrink(terms, step, have)
        return terms

    def lockstep(*chains):
        flat = together(*(chain[-1] for chain in chains))
        return [chain[:-1] + [last] for chain, last in zip(chains, flat)]

    def descend_joined(one, other, axis, step, have):
        place = have.index(step)
        have.remove(step)
        away = [total(side(terms, 1, place)).astype(BF16) for terms in (one, other)]
        near = [total(side(terms, 0, place)) for terms in (one, other)]
        away = flip(jnp.concatenate(away, axis=axis), step)
        return [jnp.concatenate(near, axis=axis).astype(BF16), away]

    qk_terms = descend(qk_terms, along_y[:1], have_qk)
    vo_terms = descend(vo_terms, along_x, have_vo)
    back_z = along_z[::-1]
    rest_terms = descend_joined(up_terms, down_terms, -2, back_z[0], have_up)
    sums_shape = (devices, small_size)
    (sums,) = call(
        functools.partial(collect_vectors, per),
        (1,),
        [smem, whole(sums_one.shape), whole(sums_two.shape), whole(g_b.shape), whole(g_bu.shape)]
        + [whole((width, width))],
        [((sums_shape, F32), whole(sums_shape))],
        [],
        0,
        4 * width * width,
        order_chunks,
        sums_one,
        sums_two,
        g_b,
        g_bu,
        turn,
    )
    layer_out = turned_back(layer_out)
    rest_terms, qk_terms, vo_terms, swapped, (layer_out,) = lockstep(
        rest_terms, qk_terms, vo_terms, [sums], [layer_out]
    )
    qk_terms = descend(qk_terms, along_y[1:] + along_x, have_qk)
    vo_terms = descend(vo_terms, along_y, have_vo)
    rest_terms = descend(rest_terms, back_z[1:], have_up)
    layer_out = unpad(layer_out)
    tokens_grad = unpad(turned_back(tokens_grad))

    rest_terms, qk_terms, vo_terms, swapped = lockstep(
        rest_terms, qk_terms, vo_terms, [exchange(swapped[0])]
    )
    first_terms = descend_joined(qk_terms, vo_terms, -1, back_z[0], have_qk)
    first_terms = descend(first_terms, back_z[1:], have_qk)
    rest = total(rest_terms)
    g_up, g_down_t = rest[:part_rows], rest[part_rows:]
    first = total(first_terms)
    g_qkv = first[:, : 3 * part_cols].reshape(part_rows, 3, part_cols)
    g_out = first[:, 3 * part_cols :].reshape(n_head, -1, part_cols).transpose(1, 0, 2)
    g_out = g_out.reshape(out_weight.shape)
    sums = jnp.sum(swapped[0], axis=0)

    def part(index):
        return sums[index * per : (index + 1) * per]

    return (
        layer_out,
        tokens_grad,
        part(0),
        part(1),
        g_qkv,
        sums[6 * per : 8 * per].reshape(2, per),
        g_out,
        part(2),
        part(3),
        part(4),
        g_up,
        sums[8 * per :],
        g_down_t.T,
        part(5),
    )


def solution(mesh):
    n_dp, n_head = mesh.shape["dp"], mesh.shape["head"]

    def run(*args):
        return local(n_dp, n_head, *args)

    return jax.shard_map(
        run,
        mesh=mesh,
        in_specs=(
            P(ALL, None),
            P("dp"),
            P(ALL),
            P(ALL),
            P("dp", None, "head"),
            P(None, ("head", "dp")),
            P(ALL, None),
            P(ALL),
            P(ALL),
            P(ALL),
            P("dp", "head"),
            P(("head", "dp")),
            P("head", "dp"),
            P(ALL),
            P(ALL, None),
        ),
        out_specs=(
            P(ALL, None),
            P(ALL, None),
            P(ALL),
            P(ALL),
            P("dp", None, "head"),
            P(None, ("head", "dp")),
            P(ALL, None),
            P(ALL),
            P(ALL),
            P(ALL),
            P("dp", "head"),
            P(("head", "dp")),
            P("head", "dp"),
            P(ALL),
        ),
        check_vma=False,
    )
```

```python
import functools

import jax
import jax.numpy as jnp
from jax import lax
from jax.experimental.layout import Layout, with_layout_constraint
from jax.experimental import pallas as pl
from jax.experimental.pallas import tpu as pltpu
from jax.sharding import PartitionSpec as P

HEAD_DIM = 64
TEXT = 40
ALL = ("dp", "head")
F32 = jnp.float32
BF16 = jnp.bfloat16


def mm(a, b):
    return jnp.dot(a, b, preferred_element_type=F32)


def mm_t(a, b):
    return lax.dot_general(a, b, (((1,), (1,)), ((), ())), preferred_element_type=F32)


def t_mm(a, b):
    return lax.dot_general(a, b, (((0,), (0,)), ((), ())), preferred_element_type=F32)


def norm_parts(values):
    spread = values - jnp.mean(values, axis=-1, keepdims=True)
    root = lax.rsqrt(jnp.mean(spread * spread, axis=-1, keepdims=True) + 1e-06)
    return spread * root, root


def norm_back(grad, gain, hat, root):
    scaled = grad * gain
    first = jnp.mean(scaled, axis=-1, keepdims=True)
    second = jnp.mean(scaled * hat, axis=-1, keepdims=True)
    return root * (scaled - first - hat * second)


VMEM = pltpu.VMEM


def spec(shape, index):
    return pl.BlockSpec(shape, index, memory_space=VMEM)


def whole(shape):
    return spec(shape, lambda *_: (0,) * len(shape))


def chunk(shape):
    return spec((1,) + shape, lambda j, *_: (j,) + (0,) * len(shape))


def nearer(t, near, far):
    return jnp.where(t < pl.num_programs(0) // 2, near[0], far[0])


def store(t, near, far, value):
    half = pl.num_programs(0) // 2

    @pl.when(t < half)
    def _():
        near[0] = value

    @pl.when(t >= half)
    def _():
        far[0] = value


def column_sum(matrix):
    return jnp.sum(matrix.astype(F32), axis=0, keepdims=True)


def counting(shape, axis):
    return lax.broadcasted_iota(jnp.int32, shape, axis)


def repeats(part, size):
    return (counting((part, size), 1) % part == counting((part, size), 0)).astype(F32)


def owners(devices, part, size):
    return counting((devices, size), 1) // part, counting((devices, size), 0)


def spread_vectors(per, order, smalls, turn, vectors, b_qv, b_up):
    devices, width = smalls.shape[0], turn.shape[0]
    chunks, _, part = b_up.shape
    values = smalls[...].astype(F32)
    plain = vectors.shape[0]
    pattern = repeats(per, width).astype(BF16)
    block, device = owners(devices, per, width)
    rows = []
    for v in range(plain):
        row = mm(values[:, v * per : (v + 1) * per].astype(BF16), pattern)
        rows.append(jnp.sum(jnp.where(block == device, row, 0.0), axis=0, keepdims=True))
    vectors[...] = mm(jnp.concatenate(rows, axis=0).astype(BF16), turn[...])

    def by_chunk(first, size, length, out):
        tall = mm(
            values[:, first : first + size].astype(BF16), repeats(size, length).astype(BF16)
        )
        block, device = owners(devices, size, length)
        for t in range(chunks):
            mine = device == block * chunks + order[t]
            out(t, jnp.sum(jnp.where(mine, tall, 0.0), axis=0, keepdims=True))

    def set_query(t, row):
        b_qv[t, 0:1, :] = row

    def set_value(t, row):
        b_qv[t, 1:2, :] = row

    def set_up(t, row):
        b_up[t] = row

    cols = b_qv.shape[2]
    by_chunk(plain * per, per, cols, set_query)
    by_chunk((plain + 1) * per, per, cols, set_value)
    by_chunk((plain + 2) * per, values.shape[1] - (plain + 2) * per, part, set_up)


def collect_vectors(per, order, sums_one, sums_two, g_b, g_bu, turn, out):
    devices, width = out.shape[0], turn.shape[0]
    chunks, _, part = g_bu.shape

    def exact(a, b):
        high = a.astype(BF16)
        left = a - high.astype(F32)
        mid = left.astype(BF16)
        low = (left - mid.astype(F32)).astype(BF16)
        count = a.shape[0]
        parts = mm_t(jnp.concatenate([part.astype(F32) for part in (high, mid, low)]).astype(BF16), b)
        return parts[:count] + (parts[count : 2 * count] + parts[2 * count :])

    plain = sums_one.shape[0] + sums_two.shape[0]
    rows = jnp.concatenate([sums_one[...], sums_two[...]], axis=0)
    rows = exact(rows, turn[...])
    block, device = owners(devices, per, width)
    tall = [jnp.where(block == device, rows[v : v + 1, :], 0.0) for v in range(plain)]
    tall = exact(jnp.concatenate(tall, axis=0), repeats(per, width).astype(BF16))
    columns = [tall[v * devices : (v + 1) * devices, :] for v in range(plain)]

    def by_chunk(row_of, size, length):
        block, device = owners(devices, size, length)
        tall = jnp.zeros((devices, length), F32)
        for t in range(chunks):
            tall = jnp.where(device == block * chunks + order[t], row_of(t), tall)
        columns.append(exact(tall, repeats(size, length).astype(BF16)))

    cols = g_b.shape[2] // 3
    by_chunk(lambda t: g_b[t][:, :cols], per, cols)
    by_chunk(lambda t: g_b[t][:, 2 * cols :], per, cols)
    by_chunk(lambda t: g_bu[t], out.shape[1] - (plain + 2) * per, part)
    out[...] = jnp.concatenate(columns, axis=1)


def attention_forward(
    items,
    seq,
    lengths,
    order,
    x,
    vectors,
    qk_near,
    qk_far,
    vo_near,
    vo_far,
    b_qv,
    out_q,
    out_k,
    out_v,
    out_p,
    out_c,
    normed,
):
    t = pl.program_id(0)
    rows = x.shape[0] // items
    cols = out_q.shape[2]
    scale = HEAD_DIM**-0.5

    @pl.when(t == 0)
    def _():
        hat, _ = norm_parts(x[...].astype(F32))
        normed[...] = (hat * vectors[0:1, :] + vectors[1:2, :]).astype(BF16)

    bias = b_qv[t]
    both = mm(normed[...], nearer(t, qk_near, qk_far))
    query = (both[:, :cols] + bias[0:1, :]).astype(BF16)
    key = both[:, cols:].astype(BF16)
    value = (mm(normed[...], nearer(t, vo_near, vo_far)[:, :cols]) + bias[1:2, :]).astype(BF16)
    out_q[0] = query
    out_k[0] = key
    out_v[0] = value
    heads = cols // HEAD_DIM
    at = lax.broadcasted_iota(jnp.int32, (rows, rows), 1)
    jobs = [
        (item, head, slice(item * rows, (item + 1) * rows))
        for item in range(items)
        for head in range(heads)
    ]
    visible = [((at >= TEXT) & (at < seq)) | (at < lengths[item]) for item in range(items)]

    def lanes(head):
        return slice(head * HEAD_DIM, (head + 1) * HEAD_DIM)

    scores = [
        mm_t(query[mine, lanes(head)], key[mine, lanes(head)]) * scale for _, head, mine in jobs
    ]
    parts = []
    for (item, head, _), score in zip(jobs, scores):
        score = jnp.where(visible[item], score, -1000000000.0)
        raised = jnp.exp(score - jnp.max(score, axis=-1, keepdims=True))
        probs = raised / jnp.sum(raised, axis=-1, keepdims=True)
        out_p[0, item * heads + head] = probs
        parts.append(probs.astype(BF16))
    parts = [mm(low, value[mine, lanes(head)]) for (_, head, mine), low in zip(jobs, parts)]
    for item in range(items):
        mine = slice(item * rows, (item + 1) * rows)
        whole_item = jnp.concatenate(parts[item * heads : (item + 1) * heads], axis=1)
        out_c[0, mine, :] = whole_item.astype(BF16)


def chunk_rows(order, c, cols):
    return pl.ds(pl.multiple_of(order[c] * cols, cols), cols)


def between(order, x, ctx, w_out, vectors, top, middle, hidden, hidden_t, top_t):
    chunks, _, cols = ctx.shape
    total = x[...].astype(F32) + vectors[2:3, :]
    for c in range(chunks):
        total += mm(ctx[c], w_out[chunk_rows(order, c, cols), :])
    middle[...] = total
    hat, _ = norm_parts(total)
    low = hat * vectors[3:4, :] + vectors[4:5, :]
    hidden[...] = low.astype(BF16)
    hidden_t[...] = low.T.astype(BF16)
    top_t[...] = top[...].astype(F32).T.astype(BF16)


def feed_forward(last, hidden, hidden_t, top, top_t, *rest):
    ups, downs, b_up, rest = rest[:4], rest[4:8], rest[8], rest[9:]
    late = []
    if last:
        order, vectors, *late = rest[:6]
        rest = rest[6:]
    grads_out, out_bu, rest = rest[:4], rest[4], rest[5:]
    if last:
        out_y, out_gm, out_ga, out_gc, out_sums, *rest = rest
    sum_y, sum_h, weights, grads, in_sems, out_sems, *late_here = rest
    half = weights.shape[1] // 2

    loads = []
    for i, piece in enumerate(ups[2:] + downs[2:]):
        here = weights.at[i // 2, pl.ds(i % 2 * half, half)]
        loads.append(pltpu.make_async_copy(piece, here, in_sems.at[i]))
    for i, (piece, here) in enumerate(zip(late, late_here)):
        loads.append(pltpu.make_async_copy(piece, here, in_sems.at[4 + i]))
    for load in loads:
        load.start()
    sends = [
        pltpu.make_async_copy(grads.at[i], grads_out[i], out_sems.at[i]) for i in range(4)
    ]

    def work(which, w_up, w_down_t):
        up = mm(hidden[...], w_up) + b_up[which]
        phi = 0.5 * (1.0 + lax.erf(up * (0.5**0.5)))
        active = (up * phi).astype(BF16)
        slope = phi + up * jnp.exp(-0.5 * up * up) * ((2.0 * jnp.pi) ** -0.5)
        grad_up = (mm(top[...], w_down_t) * slope).astype(BF16)
        grads[2 + which] = mm(top_t[...], active).astype(BF16)
        sends[2 + which].start()
        grads[which] = mm(hidden_t[...], grad_up).astype(BF16)
        sends[which].start()
        out_bu[which] = column_sum(grad_up)
        part_y, part_h = mm_t(active, w_down_t), mm_t(grad_up, w_up)
        if which == 0:
            sum_y[...] = part_y
            sum_h[...] = part_h
        else:
            sum_y[...] += part_y
            sum_h[...] += part_h

    near = [jnp.concatenate([ref[...] for ref in refs[:2]], axis=0) for refs in (ups, downs)]
    work(0, *near)
    for load in loads:
        load.wait()
    work(1, weights[0], weights[1])
    if last:
        middle, w_out, in_y, in_h = late_here
        chunks, _, cols = out_gc.shape
        gain = vectors[3:4, :]
        hat, root = norm_parts(middle[...])
        total_y = in_y[...] + sum_y[...]
        out_y[...] = (middle[...] + (total_y + vectors[5:6, :])).astype(BF16)
        grad_hidden = in_h[...] + sum_h[...]
        grad_top = top[...].astype(F32)
        grad_middle = grad_top + norm_back(grad_hidden, gain, hat, root)
        out_gm[...] = grad_middle
        grad_attn = grad_middle.astype(BF16)
        out_ga[...] = grad_attn
        out_sums[0:1, :] = column_sum(grad_attn)
        out_sums[1:2, :] = column_sum(grad_hidden * hat)
        out_sums[2:3, :] = column_sum(grad_hidden)
        out_sums[3:4, :] = column_sum(grad_top)
        for c in range(chunks):
            out_gc[c] = mm_t(grad_attn, w_out[chunk_rows(order, c, cols), :]).astype(BF16)
    for send in sends:
        send.wait()


def out_gradient(order, ctx, grad_attn, turn, out_go):
    chunks, _, cols = ctx.shape
    for c in range(chunks):
        grad_out = t_mm(ctx[c], grad_attn[...]).astype(BF16)
        out_go[chunk_rows(order, c, cols), :] = mm_t(grad_out, turn[...]).astype(BF16)


def attention_backward(
    items,
    x,
    vectors,
    qk_near,
    qk_far,
    vo_near,
    vo_far,
    query,
    key,
    value,
    probs,
    grad_ctx,
    grad_middle,
    out_x,
    gqk_near,
    gqk_far,
    gvo_near,
    gvo_far,
    out_b,
    out_sums,
    hat,
    root,
    normed_t,
    sum_n,
):
    rows = x.shape[0] // items
    cols = query.shape[2]
    heads = cols // HEAD_DIM
    scale = HEAD_DIM**-0.5
    t = pl.program_id(0)
    gain = vectors[0:1, :]

    @pl.when(t == 0)
    def _():
        hat_one, root_one = norm_parts(x[...].astype(F32))
        hat[...] = hat_one
        root[...] = root_one
        normed_t[...] = (hat_one * gain + vectors[1:2, :]).T.astype(BF16)
        sum_n[...] = jnp.zeros_like(sum_n)

    jobs = [
        (item, head, slice(item * rows, (item + 1) * rows))
        for item in range(items)
        for head in range(heads)
    ]

    def lanes(head):
        return slice(head * HEAD_DIM, (head + 1) * HEAD_DIM)

    grads_p = [
        mm_t(grad_ctx[0, mine, lanes(head)], value[0, mine, lanes(head)]) for _, head, mine in jobs
    ]
    parts_v = [
        t_mm(probs[0, item * heads + head].astype(BF16), grad_ctx[0, mine, lanes(head)])
        for item, head, mine in jobs
    ]
    grads_s = []
    for (item, head, _), grad_p in zip(jobs, grads_p):
        p = probs[0, item * heads + head]
        row = jnp.sum(p * grad_p, axis=-1, keepdims=True)
        grads_s.append((p * (grad_p - row)).astype(BF16))
    parts_q = [
        mm(grad_s, key[0, mine, lanes(head)]) * scale for (_, head, mine), grad_s in zip(jobs, grads_s)
    ]
    parts_k = [
        t_mm(grad_s, query[0, mine, lanes(head)]) * scale
        for (_, head, mine), grad_s in zip(jobs, grads_s)
    ]

    def gathered(parts):
        items_of = [
            jnp.concatenate(parts[item * heads : (item + 1) * heads], axis=1)
            for item in range(items)
        ]
        return jnp.concatenate(items_of, axis=0).astype(BF16)

    grad_all = jnp.concatenate([gathered(p) for p in (parts_q, parts_k, parts_v)], axis=1)
    out_b[0] = column_sum(grad_all)
    grad_qk, grad_v = grad_all[:, : 2 * cols], grad_all[:, 2 * cols :]
    store(t, gqk_near, gqk_far, mm(normed_t[...], grad_qk).astype(BF16))
    grad_weight = mm(normed_t[...], grad_v).astype(BF16)
    store(t, gvo_near, gvo_far, grad_weight)
    sum_n[...] += mm_t(grad_qk, nearer(t, qk_near, qk_far))
    sum_n[...] += mm_t(grad_v, nearer(t, vo_near, vo_far)[:, :cols])

    @pl.when(t == pl.num_programs(0) - 1)
    def _():
        grad_normed = sum_n[...]
        back = norm_back(grad_normed, gain, hat[...], root[...])
        out_x[...] = (grad_middle[...] + back).astype(BF16)
        out_sums[0:1, :] = column_sum(grad_normed * hat[...])
        out_sums[1:2, :] = column_sum(grad_normed)


def call(body, grid, in_specs, outs, scratch, flops, moved, *args):
    return pl.pallas_call(
        body,
        grid=grid,
        in_specs=in_specs,
        out_specs=[o[1] for o in outs],
        out_shape=[jax.ShapeDtypeStruct(*o[0]) for o in outs],
        scratch_shapes=scratch,
        compiler_params=pltpu.CompilerParams(
            dimension_semantics=("arbitrary",) * len(grid), vmem_limit_bytes=60 * 1024 * 1024
        ),
        cost_estimate=pl.CostEstimate(flops=flops // 8, bytes_accessed=moved // 8, transcendentals=0),
    )(*args)


def local(
    n_dp,
    n_head,
    tokens,
    caption_len,
    first_gain,
    first_shift,
    qkv_weight,
    qkv_bias,
    out_weight,
    out_bias,
    second_gain,
    second_shift,
    up_weight,
    up_bias,
    down_weight,
    down_bias,
    output_grad,
):
    rows, width = tokens.shape
    hidden = up_weight.shape[1] * n_head
    devices = n_dp * n_head
    item_count = caption_len.shape[0] // n_head
    seq = rows // item_count
    dp_bits = [("dp", 1 << i) for i in reversed(range(n_dp.bit_length() - 1))]
    head_bits = [("head", 1 << i) for i in reversed(range(n_head.bit_length() - 1))]
    held = (dp_bits + head_bits)[::-1]
    along_z, along_x, along_y = dp_bits[:-1], dp_bits[-1:], head_bits[:-1]
    core = head_bits[-1]

    def flip(piece, step):
        axis, bit = step
        count = n_dp if axis == "dp" else n_head
        rows_first = Layout(tuple(range(piece.ndim)))
        piece = with_layout_constraint(piece, rows_first)
        piece = lax.ppermute(piece, axis, [(i, i ^ bit) for i in range(count)])
        return with_layout_constraint(piece, rows_first)

    def together(*values):
        return lax.optimization_barrier(values)

    def place_of(step, have):
        return sum(held.index(h) < held.index(step) for h in have)

    def grow(piece, step, have):
        other = flip(piece, step)
        piece = jnp.stack([piece, other], axis=place_of(step, have))
        have.append(step)
        return piece

    def both(step, other):
        return step[0], step[1] | other[1]

    def grow_two(piece, step, other, have):
        pieces = [piece, flip(piece, step), flip(piece, other), flip(piece, both(step, other))]
        have.extend([step, other])
        return jnp.stack(pieces).reshape((2, 2) + piece.shape)

    def side(terms, which, place):
        return [lax.index_in_dim(term, which, place, False) for term in terms]

    def total(terms):
        return sum(term.astype(F32) for term in terms)

    def shrink(terms, step, have):
        place = have.index(step)
        have.remove(step)
        away = total(side(terms, 1, place)).astype(BF16)
        return side(terms, 0, place) + [flip(away, step)]

    def reverse_bits(value, count):
        return sum(
            ((value >> i) & 1) << (count.bit_length() - 2 - i) for i in range(count.bit_length() - 1)
        )

    my_dp, my_head = lax.axis_index("dp"), lax.axis_index("head")
    order_chunks = my_head ^ reverse_bits(jnp.arange(n_head, dtype=jnp.int32), n_head)
    order_blocks = my_dp ^ reverse_bits(jnp.arange(n_dp, dtype=jnp.int32), n_dp)

    def exchange(blocks):
        return lax.all_to_all(blocks, ALL, 0, 0, tiled=True)

    per = first_gain.shape[0]
    smem = pl.BlockSpec(memory_space=pltpu.SMEM)
    pieces = [first_gain, first_shift, out_bias, second_gain, second_shift, down_bias]
    pieces += [qkv_bias[0], qkv_bias[1], up_bias]
    small_size = sum(piece.shape[0] for piece in pieces)
    smalls, start = 0, 0
    for piece in pieces:
        stop = start + piece.shape[0]
        smalls += jnp.pad(piece, (start, small_size - stop))
        start = stop
    part_rows = width // n_dp
    part_cols = width // n_head
    part_hidden = up_weight.shape[1]
    part_hidden = up_weight.shape[1]
    features = jnp.arange(width, dtype=jnp.int32)
    place = jnp.repeat(order_blocks, part_rows) * part_rows + features % part_rows
    turn = (features[:, None] == place[None, :]).astype(BF16)

    def turned(piece):
        return mm(piece, turn).astype(BF16)

    def turned_back(piece):
        return mm_t(piece, turn).astype(BF16)

    ranks = order_blocks[None, :] * n_head + order_chunks[:, None]
    ranks = ranks.reshape(-1)
    chunk_of = reverse_bits(my_head ^ jnp.arange(n_head, dtype=jnp.int32), n_head)
    block_of = reverse_bits(my_dp ^ jnp.arange(n_dp, dtype=jnp.int32), n_dp)
    ranks_back = (chunk_of[None, :] * n_dp + block_of[:, None]).reshape(-1)
    padded = -(-seq // 16) * 16
    total_rows = item_count * padded

    def pad(piece):
        piece = piece.reshape(item_count, seq, width)
        return jnp.pad(piece, ((0, 0), (0, padded - seq), (0, 0))).reshape(total_rows, width)

    def unpad(piece):
        return piece.reshape(item_count, padded, width)[:, :seq].reshape(rows, width)

    def out_pack(piece):
        return piece.reshape(-1, n_head, part_cols).transpose(1, 0, 2).reshape(part_rows, part_cols)

    have, have_rest = [], []
    first = [qkv_weight.reshape(part_rows, 3 * part_cols), out_pack(out_weight)]
    first = jnp.concatenate(first, axis=1)
    rest = jnp.concatenate([up_weight, down_weight.T])
    for step in along_z[:-2]:
        first = grow(first, step, have)
    first = grow_two(first, *along_z[-2:], have)
    x, top = turned(pad(tokens)), turned(pad(output_grad))
    smalls = exchange(jnp.broadcast_to(smalls[None], (devices,) + smalls.shape))
    first, rest, x, top, smalls = together(first, rest, x, top, smalls)

    part_cols = width // n_head
    vectors, b_qv, b_up = call(
        functools.partial(spread_vectors, per),
        (1,),
        [smem, whole(smalls.shape), whole((width, width))],
        [
            (((6, width), F32), whole((6, width))),
            (((n_head, 2, part_cols), F32), whole((n_head, 2, part_cols))),
            (((n_head, 1, hidden // n_head), F32), whole((n_head, 1, hidden // n_head))),
        ],
        [],
        0,
        4 * width * width,
        order_chunks,
        smalls,
        turn,
    )
    w_qk, w_vo = first[..., : 2 * part_cols], first[..., 2 * part_cols :]
    have_qk, have_vo = list(have), list(have)
    w_qk, w_vo = grow(w_qk, along_x[0], have_qk), grow(w_vo, along_y[0], have_vo)
    rest = grow(rest, along_z[0], have_rest)
    w_qk, w_vo, rest, vectors, b_qv, b_up = together(w_qk, w_vo, rest, vectors, b_qv, b_up)
    for step in along_z[1:-1]:
        rest = grow(rest, step, have_rest)
    for step in along_y[:-1]:
        w_qk = grow(w_qk, step, have_qk)
    for step in along_y[1:]:
        w_vo = grow(w_vo, step, have_vo)
    w_qk, w_vo = grow(w_qk, along_y[-1], have_qk), grow(w_vo, along_x[0], have_vo)
    rest = grow(rest, along_z[-1], have_rest)
    w_up, w_down = rest[..., :part_rows, :], rest[..., part_rows:, :]
    pair_shape = (-1, width, 2 * part_cols)
    near_qk, near_vo, w_up, w_down = together(
        w_qk.reshape(pair_shape), w_vo.reshape(pair_shape), w_up, w_down
    )
    far_qk, far_vo = flip(near_qk, core), flip(near_vo, core)
    step_x, step_y = along_x[0], along_y[0]
    up_x, down_x = flip(w_up, step_x), flip(w_down, step_x)
    up_y, down_y = flip(w_up, step_y), flip(w_down, step_y)


    lengths = lax.dynamic_slice_in_dim(caption_len, my_head * item_count, item_count)
    pairs = item_count * (part_cols // HEAD_DIM)

    full = (total_rows, width)
    slab = (total_rows, part_cols)
    slab_out = (((n_head,) + slab, BF16), chunk(slab))
    probs_out = (((n_head, pairs, padded, padded), F32), chunk((pairs, padded, padded)))
    weights = width * width

    half = n_head // 2

    def near(shape):
        return spec((1,) + shape, lambda t: (jnp.minimum(t, half - 1), 0, 0))

    def far(shape):
        return spec((1,) + shape, lambda t: (jnp.maximum(t - half, 0), 0, 0))

    two_cols, one_col = (width, 2 * part_cols), (width, part_cols)
    first_specs = [near(two_cols), far(two_cols)] * 2
    query, key, value, probs, context = call(
        functools.partial(attention_forward, item_count, seq),
        (n_head,),
        [smem, smem, whole(full), whole(vectors.shape)]
        + first_specs
        + [whole(b_qv.shape)],
        [slab_out, slab_out, slab_out, probs_out, slab_out],
        [pltpu.VMEM(full, BF16)],
        8 * total_rows * weights,
        12 * weights,
        lengths,
        order_chunks,
        x,
        vectors,
        near_qk,
        far_qk,
        near_vo,
        far_vo,
        b_qv,
    )

    w_out = jnp.concatenate([near_vo[..., part_cols:], far_vo[..., part_cols:]])
    w_out = w_out.reshape(devices, n_head, -1, part_cols).transpose(0, 2, 1, 3)
    w_out = w_out.reshape(devices, -1, width)
    w_out = turned(w_out[ranks_back].reshape(width, width))
    middle, low, low_t, top_t = call(
        between,
        (1,),
        [smem, whole(full), whole((n_head,) + slab), whole((width, width))]
        + [whole(vectors.shape), whole(full)],
        [
            ((full, F32), whole(full)),
            ((full, BF16), whole(full)),
            ((full[::-1], BF16), whole(full[::-1])),
            ((full[::-1], BF16), whole(full[::-1])),
        ],
        [],
        2 * total_rows * weights,
        8 * weights,
        order_chunks,
        x,
        context,
        w_out,
        vectors,
        top,
    )

    up_x, down_x, up_y, down_y, low = together(up_x, down_x, up_y, down_y, low)
    up_d, down_d = flip(up_x, step_y), flip(down_y, step_x)
    own = [w_up, up_x, w_down, down_x]
    own_far = [flip(piece, core) for piece in own]
    other = [up_y, up_d, down_y, down_d]
    early_far = [flip(piece, core) for piece in other[::2]]
    *own_far, late_0, late_1 = together(*own_far, *early_far)
    early_far = [late_0, late_1]

    def arranged(near, far):
        pieces = near[:2] + far[:2] + near[2:] + far[2:]
        return [piece.reshape(-1, part_hidden) for piece in pieces]

    b_up = b_up.reshape(2, half, 1, part_hidden)
    anywhere = pl.BlockSpec(memory_space=pl.ANY)
    piece = whole((width // 2, part_hidden))
    strips = [piece, piece, anywhere, anywhere] * 2
    strip_outs = [(((width, part_hidden), BF16), anywhere)] * 4
    strip_outs += [(((2, 1, part_hidden), F32), whole((2, 1, part_hidden)))]
    copied = [
        pltpu.VMEM((2, width, part_hidden), BF16),
        pltpu.VMEM((4, width, part_hidden), BF16),
        pltpu.SemaphoreType.DMA((8,)),
        pltpu.SemaphoreType.DMA((4,)),
    ]
    cost = 6 * total_rows * width * hidden, 10 * weights
    *g_own, gb_own, sum_y, sum_h = call(
        functools.partial(feed_forward, False),
        (1,),
        [whole(full), whole(full[::-1])] * 2 + strips + [whole((2, 1, part_hidden))],
        strip_outs + [((full, F32), whole(full))] * 2,
        copied,
        *cost,
        low,
        low_t,
        top,
        top_t,
        *arranged(own, own_far),
        b_up[:, 0],
    )
    other[1], other[3], sum_y = together(other[1], other[3], sum_y)
    late_far = [flip(piece, core) for piece in other[1::2]]
    other_far = [early_far[0], late_far[0], early_far[1], late_far[1]]

    rest_bits = held[1:]
    shape = (2,) * len(rest_bits)
    tile = (part_rows, part_hidden)

    def pair(near, far, tile):
        near = near.reshape(shape[1:] + tile)
        return [near, flip(far.reshape(near.shape), core)]

    gup_own, gdown_own = pair(*g_own[:2], tile), pair(*g_own[2:], tile)
    *g_other, gb_other, layer_out, grad_middle, grad_attn, grad_context, sums_two = call(
        functools.partial(feed_forward, True),
        (1,),
        [whole(full), whole(full[::-1])] * 2
        + strips
        + [whole((2, 1, part_hidden)), smem, whole(vectors.shape)]
        + [anywhere] * 4,
        strip_outs
        + [
            ((full, BF16), whole(full)),
            ((full, F32), whole(full)),
            ((full, BF16), whole(full)),
            (((n_head,) + slab, BF16), whole((n_head,) + slab)),
            (((4, width), F32), whole((4, width))),
        ],
        [pltpu.VMEM(full, F32)] * 2
        + copied
        + [pltpu.VMEM(full, F32), pltpu.VMEM((width, width), BF16)]
        + [pltpu.VMEM(full, F32)] * 2,
        *cost,
        low,
        low_t,
        top,
        top_t,
        *arranged(other, other_far),
        b_up[:, 1],
        order_chunks,
        vectors,
        middle,
        w_out,
        sum_y,
        sum_h,
    )
    g_bu = jnp.stack([gb_own, gb_other], axis=1).reshape(n_head, 1, part_hidden)
    gup_other, gdown_other = pair(*g_other[:2], tile), pair(*g_other[2:], tile)

    def low_total(terms):
        return total(terms).astype(BF16)

    away = [
        low_total(side(gdown_own, 1, 0)),
        low_total(side(gup_other, 1, 0)),
        low_total(side(gdown_other, 1, 0)),
        low_total(side(gup_other, 0, 0)),
    ]
    down_01, up_11 = flip(away[0], step_x), flip(away[1], step_y)
    down_11, up_10 = flip(away[2], step_x), flip(away[3], step_y)
    grad_context, *_ = together(grad_context, *away)
    tokens_grad, gqk_near, gqk_far, gvo_near, gvo_far, g_b, sums_one = call(
        functools.partial(attention_backward, item_count),
        (n_head,),
        [whole(full), whole(vectors.shape)]
        + first_specs
        + [chunk(slab)] * 3
        + [chunk((pairs, padded, padded)), chunk(slab), whole(full)],
        [
            ((full, BF16), whole(full)),
            (((half,) + two_cols, BF16), near(two_cols)),
            (((half,) + two_cols, BF16), far(two_cols)),
            (((half,) + one_col, BF16), near(one_col)),
            (((half,) + one_col, BF16), far(one_col)),
            (((n_head, 1, 3 * part_cols), F32), chunk((1, 3 * part_cols))),
            (((2, width), F32), whole((2, width))),
        ],
        [
            pltpu.VMEM(full, F32),
            pltpu.VMEM((total_rows, 1), F32),
            pltpu.VMEM(full[::-1], BF16),
            pltpu.VMEM(full, F32),
        ],
        16 * total_rows * weights,
        12 * weights,
        x,
        vectors,
        near_qk,
        far_qk,
        near_vo,
        far_vo,
        query,
        key,
        value,
        probs,
        grad_context,
        grad_middle,
    )
    two = (part_rows, 2 * part_cols)
    down_01, up_11, down_11, up_10, gqk_near, gqk_far, gvo_near, gvo_far = together(
        down_01, up_11, down_11, up_10, gqk_near, gqk_far, gvo_near, gvo_far
    )

    def pair_first(near, far):
        return [near.reshape(shape + two), flip(far.reshape(shape + two), core)]

    away_up = low_total(side(gup_own, 1, 0) + [up_11])
    away_down = low_total(side(gdown_other, 0, 0) + [down_11])
    up_01, down_10 = flip(away_up, step_x), flip(away_down, step_y)
    qk_terms = pair_first(gqk_near, gqk_far)
    grad_attn, *_ = together(grad_attn, away_up, away_down, gqk_far)
    (g_out,) = call(
        out_gradient,
        (1,),
        [smem, whole((n_head,) + slab), whole(full), whole((width, width))],
        [(((width, width), BF16), whole((width, width)))],
        [],
        0,
        0,
        order_chunks,
        context,
        grad_attn,
        turn,
    )
    g_out = g_out.reshape(devices, -1, width)[ranks]
    g_out = g_out.reshape(devices, -1, n_head, part_cols).transpose(0, 2, 1, 3)
    g_out = g_out.reshape(n_head, width, part_cols)
    gvo_near = jnp.concatenate([gvo_near, g_out[:half]], axis=2)
    gvo_far = jnp.concatenate([gvo_far, g_out[half:]], axis=2)
    up_01, down_10, gvo_near, gvo_far, *qk_terms = together(
        up_01, down_10, gvo_near, gvo_far, *qk_terms
    )
    vo_terms = pair_first(gvo_near, gvo_far)
    have_qk, have_vo = list(rest_bits), list(rest_bits)
    up_terms = side(gup_own, 0, 0) + [up_10, up_01]
    down_terms = side(gdown_own, 0, 0) + [down_01, down_10]
    have_up = list(dp_bits[:-1][::-1])

    def descend(terms, steps, have):
        for step in steps:
            terms = shrink(terms, step, have)
        return terms

    def lockstep(*chains):
        flat = together(*(chain[-1] for chain in chains))
        return [chain[:-1] + [last] for chain, last in zip(chains, flat)]

    def descend_joined(one, other, axis, step, have):
        place = have.index(step)
        have.remove(step)
        away = [total(side(terms, 1, place)).astype(BF16) for terms in (one, other)]
        near = [total(side(terms, 0, place)) for terms in (one, other)]
        away = flip(jnp.concatenate(away, axis=axis), step)
        return [jnp.concatenate(near, axis=axis).astype(BF16), away]

    qk_terms = descend(qk_terms, along_y[:1], have_qk)
    vo_terms = descend(vo_terms, along_x, have_vo)
    back_z = along_z[::-1]
    rest_terms = descend_joined(up_terms, down_terms, -2, back_z[0], have_up)
    sums_shape = (devices, small_size)
    (sums,) = call(
        functools.partial(collect_vectors, per),
        (1,),
        [smem, whole(sums_one.shape), whole(sums_two.shape), whole(g_b.shape), whole(g_bu.shape)]
        + [whole((width, width))],
        [((sums_shape, F32), whole(sums_shape))],
        [],
        0,
        4 * width * width,
        order_chunks,
        sums_one,
        sums_two,
        g_b,
        g_bu,
        turn,
    )
    layer_out = turned_back(layer_out)
    rest_terms, qk_terms, vo_terms, swapped, (layer_out,) = lockstep(
        rest_terms, qk_terms, vo_terms, [exchange(sums)], [layer_out]
    )
    qk_terms = descend(qk_terms, along_y[1:] + along_x, have_qk)
    vo_terms = descend(vo_terms, along_y, have_vo)
    rest_terms = descend(rest_terms, back_z[1:], have_up)
    layer_out = unpad(layer_out)
    tokens_grad = unpad(turned_back(tokens_grad))

    rest_terms, qk_terms, vo_terms = lockstep(rest_terms, qk_terms, vo_terms)
    chains = [qk_terms, vo_terms]
    for step in back_z[:-2]:
        chains = [descend(terms, [step], list(have_qk)) for terms in chains]
        have_qk.remove(step)

    def corner(i, j):
        return jnp.concatenate(
            [total(side(side(terms, i, 0), j, 0)) for terms in chains], axis=-1
        )

    step, other = back_z[-2:]
    first = [
        corner(0, 0),
        flip(corner(1, 1).astype(BF16), both(step, other)),
        flip(corner(1, 0).astype(BF16), step),
        flip(corner(0, 1).astype(BF16), other),
    ]
    rest = total(rest_terms)
    g_up, g_down_t = rest[:part_rows], rest[part_rows:]
    first = total(first)
    g_qkv = first[:, : 3 * part_cols].reshape(part_rows, 3, part_cols)
    g_out = first[:, 3 * part_cols :].reshape(n_head, -1, part_cols).transpose(1, 0, 2)
    g_out = g_out.reshape(out_weight.shape)
    sums = jnp.sum(swapped[0], axis=0)

    def part(index):
        return sums[index * per : (index + 1) * per]

    return (
        layer_out,
        tokens_grad,
        part(0),
        part(1),
        g_qkv,
        sums[6 * per : 8 * per].reshape(2, per),
        g_out,
        part(2),
        part(3),
        part(4),
        g_up,
        sums[8 * per :],
        g_down_t.T,
        part(5),
    )


def solution(mesh):
    n_dp, n_head = mesh.shape["dp"], mesh.shape["head"]

    def run(*args):
        return local(n_dp, n_head, *args)

    return jax.shard_map(
        run,
        mesh=mesh,
        in_specs=(
            P(ALL, None),
            P("dp"),
            P(ALL),
            P(ALL),
            P("dp", None, "head"),
            P(None, ("head", "dp")),
            P(ALL, None),
            P(ALL),
            P(ALL),
            P(ALL),
            P("dp", "head"),
            P(("head", "dp")),
            P("head", "dp"),
            P(ALL),
            P(ALL, None),
        ),
        out_specs=(
            P(ALL, None),
            P(ALL, None),
            P(ALL),
            P(ALL),
            P("dp", None, "head"),
            P(None, ("head", "dp")),
            P(ALL, None),
            P(ALL),
            P(ALL),
            P(ALL),
            P("dp", "head"),
            P(("head", "dp")),
            P("head", "dp"),
            P(ALL),
        ),
        check_vma=False,
    )
```

```python
import functools
import math

import jax
import jax.numpy as jnp
from jax import lax
from jax.experimental.layout import Layout, with_layout_constraint
from jax.experimental import pallas as pl
from jax.experimental.pallas import tpu as pltpu
from jax.sharding import PartitionSpec as P

HEAD_DIM = 64
TEXT = 40
ALL = ("dp", "head")
F32 = jnp.float32
BF16 = jnp.bfloat16


def mm(a, b):
    return jnp.dot(a, b, preferred_element_type=F32)


def mm_t(a, b):
    return lax.dot_general(a, b, (((1,), (1,)), ((), ())), preferred_element_type=F32)


def t_mm(a, b):
    return lax.dot_general(a, b, (((0,), (0,)), ((), ())), preferred_element_type=F32)


def norm_parts(values):
    spread = values - jnp.mean(values, axis=-1, keepdims=True)
    root = lax.rsqrt(jnp.mean(spread * spread, axis=-1, keepdims=True) + 1e-06)
    return spread * root, root


def norm_back(grad, gain, hat, root):
    scaled = grad * gain
    first = jnp.mean(scaled, axis=-1, keepdims=True)
    second = jnp.mean(scaled * hat, axis=-1, keepdims=True)
    return root * (scaled - first - hat * second)


VMEM = pltpu.VMEM


def spec(shape, index):
    return pl.BlockSpec(shape, index, memory_space=VMEM)


def whole(shape):
    return spec(shape, lambda *_: (0,) * len(shape))


def chunk(shape):
    return spec((1,) + shape, lambda j, *_: (j,) + (0,) * len(shape))


def nearer(t, near, far):
    return jnp.where(t < pl.num_programs(0) // 2, near[0], far[0])


def store(t, near, far, value):
    half = pl.num_programs(0) // 2

    @pl.when(t < half)
    def _():
        near[0] = value

    @pl.when(t >= half)
    def _():
        far[0] = value


def column_sum(matrix):
    return jnp.sum(matrix.astype(F32), axis=0, keepdims=True)


def counting(shape, axis):
    return lax.broadcasted_iota(jnp.int32, shape, axis)


def repeats(part, size):
    return (counting((part, size), 1) % part == counting((part, size), 0)).astype(F32)


def owners(devices, part, size):
    return counting((devices, size), 1) // part, counting((devices, size), 0)


def spread_vectors(per, order, smalls, turn, vectors, b_qv, b_up):
    devices, width = smalls.shape[0], turn.shape[0]
    chunks, _, part = b_up.shape
    values = smalls[...].astype(F32)
    plain = vectors.shape[0]
    pattern = repeats(per, width).astype(BF16)
    block, device = owners(devices, per, width)
    rows = []
    for v in range(plain):
        row = mm(values[:, v * per : (v + 1) * per].astype(BF16), pattern)
        rows.append(jnp.sum(jnp.where(block == device, row, 0.0), axis=0, keepdims=True))
    vectors[...] = mm(jnp.concatenate(rows, axis=0).astype(BF16), turn[...])

    def by_chunk(first, size, length, out):
        tall = mm(
            values[:, first : first + size].astype(BF16), repeats(size, length).astype(BF16)
        )
        block, device = owners(devices, size, length)
        for t in range(chunks):
            mine = device == block * chunks + order[t]
            out(t, jnp.sum(jnp.where(mine, tall, 0.0), axis=0, keepdims=True))

    def set_query(t, row):
        b_qv[t, 0:1, :] = row

    def set_value(t, row):
        b_qv[t, 1:2, :] = row

    def set_up(t, row):
        b_up[t] = row

    cols = b_qv.shape[2]
    by_chunk(plain * per, per, cols, set_query)
    by_chunk((plain + 1) * per, per, cols, set_value)
    by_chunk((plain + 2) * per, values.shape[1] - (plain + 2) * per, part, set_up)


def collect_vectors(per, order, sums_one, sums_two, g_b, g_bu, turn, out):
    devices, width = out.shape[0], turn.shape[0]
    chunks, _, part = g_bu.shape

    def exact(a, b):
        high = a.astype(BF16)
        left = a - high.astype(F32)
        mid = left.astype(BF16)
        low = (left - mid.astype(F32)).astype(BF16)
        count = a.shape[0]
        parts = mm_t(jnp.concatenate([part.astype(F32) for part in (high, mid, low)]).astype(BF16), b)
        return parts[:count] + (parts[count : 2 * count] + parts[2 * count :])

    plain = sums_one.shape[0] + sums_two.shape[0]
    rows = jnp.concatenate([sums_one[...], sums_two[...]], axis=0)
    rows = exact(rows, turn[...])
    block, device = owners(devices, per, width)
    tall = [jnp.where(block == device, rows[v : v + 1, :], 0.0) for v in range(plain)]
    tall = exact(jnp.concatenate(tall, axis=0), repeats(per, width).astype(BF16))
    columns = [tall[v * devices : (v + 1) * devices, :] for v in range(plain)]

    def by_chunk(row_of, size, length):
        block, device = owners(devices, size, length)
        tall = jnp.zeros((devices, length), F32)
        for t in range(chunks):
            tall = jnp.where(device == block * chunks + order[t], row_of(t), tall)
        columns.append(exact(tall, repeats(size, length).astype(BF16)))

    cols = g_b.shape[2] // 3
    by_chunk(lambda t: g_b[t][:, :cols], per, cols)
    by_chunk(lambda t: g_b[t][:, 2 * cols :], per, cols)
    by_chunk(lambda t: g_bu[t], out.shape[1] - (plain + 2) * per, part)
    out[...] = jnp.concatenate(columns, axis=1)


def attention_forward(
    items,
    seq,
    lengths,
    order,
    x,
    vectors,
    qk_near,
    qk_far,
    vo_near,
    vo_far,
    b_qv,
    out_q,
    out_k,
    out_v,
    out_p,
    out_c,
    normed,
):
    t = pl.program_id(0)
    rows = x.shape[0] // items
    cols = out_q.shape[2]
    scale = HEAD_DIM**-0.5

    @pl.when(t == 0)
    def _():
        def some(span, nothing):
            hat, _ = norm_parts(x[span, :].astype(F32))
            normed[span, :] = (hat * vectors[0:1, :] + vectors[1:2, :]).astype(BF16)
            return nothing

        by_rows(x.shape[0], 0, some)

    bias = b_qv[t]
    both = mm(normed[...], nearer(t, qk_near, qk_far))
    query = (both[:, :cols] + bias[0:1, :]).astype(BF16)
    key = both[:, cols:].astype(BF16)
    value = (mm(normed[...], nearer(t, vo_near, vo_far)[:, :cols]) + bias[1:2, :]).astype(BF16)
    out_q[0] = query
    out_k[0] = key
    out_v[0] = value
    heads = cols // HEAD_DIM
    at = lax.broadcasted_iota(jnp.int32, (rows, rows), 1)
    jobs = [
        (item, head, slice(item * rows, (item + 1) * rows))
        for item in range(items)
        for head in range(heads)
    ]
    visible = [((at >= TEXT) & (at < seq)) | (at < lengths[item]) for item in range(items)]

    def lanes(head):
        return slice(head * HEAD_DIM, (head + 1) * HEAD_DIM)

    scores = [
        mm_t(query[mine, lanes(head)], key[mine, lanes(head)]) * scale for _, head, mine in jobs
    ]
    parts = []
    for (item, head, _), score in zip(jobs, scores):
        score = jnp.where(visible[item], score, -1000000000.0)
        raised = jnp.exp(score - jnp.max(score, axis=-1, keepdims=True))
        probs = raised / jnp.sum(raised, axis=-1, keepdims=True)
        out_p[0, item * heads + head] = probs
        parts.append(probs.astype(BF16))
    parts = [mm(low, value[mine, lanes(head)]) for (_, head, mine), low in zip(jobs, parts)]
    for item in range(items):
        mine = slice(item * rows, (item + 1) * rows)
        whole_item = jnp.concatenate(parts[item * heads : (item + 1) * heads], axis=1)
        out_c[0, mine, :] = whole_item.astype(BF16)


def by_rows(count, carry, body):
    part = math.gcd(count, 128)

    def one(i, carry):
        return body(pl.ds(pl.multiple_of(i * part, part), part), carry)

    return lax.fori_loop(0, count // part, one, carry)


def chunk_rows(order, c, cols):
    return pl.ds(pl.multiple_of(order[c] * cols, cols), cols)


def between(order, x, ctx, w_out, vectors, top, middle, hidden, hidden_t, top_t):
    chunks, _, cols = ctx.shape
    total = x[...].astype(F32) + vectors[2:3, :]
    for c in range(chunks):
        total += mm(ctx[c], w_out[chunk_rows(order, c, cols), :])
    middle[...] = total

    def some(span, nothing):
        hat, _ = norm_parts(middle[span, :])
        low = hat * vectors[3:4, :] + vectors[4:5, :]
        hidden[span, :] = low.astype(BF16)
        hidden_t[:, span] = low.T.astype(BF16)
        top_t[:, span] = top[span, :].astype(F32).T.astype(BF16)
        return nothing

    by_rows(x.shape[0], 0, some)


def feed_forward(last, hidden, hidden_t, top, top_t, *rest):
    ups, downs, b_up, rest = rest[:4], rest[4:8], rest[8], rest[9:]
    late = []
    if last:
        order, vectors, *late = rest[:6]
        rest = rest[6:]
    grads_out, out_bu, rest = rest[:4], rest[4], rest[5:]
    if last:
        out_y, out_gm, out_ga, out_gc, out_sums, *rest = rest
    sum_y, sum_h, weights, grads, in_sems, out_sems, *late_here = rest
    half = weights.shape[2] // 2

    loads = []
    for i, piece in enumerate(ups + downs):
        here = weights.at[i // 2 % 2, i // 4, pl.ds(i % 2 * half, half)]
        loads.append(pltpu.make_async_copy(piece, here, in_sems.at[i]))
    for i, (piece, here) in enumerate(zip(late, late_here)):
        loads.append(pltpu.make_async_copy(piece, here, in_sems.at[8 + i]))
    near_loads = loads[:2] + loads[4:6]
    far_loads = loads[2:4] + loads[6:]
    for load in near_loads + far_loads:
        load.start()
    sends = [
        pltpu.make_async_copy(grads.at[i % 2, i // 2], grads_out[i], out_sems.at[i])
        for i in range(4)
    ]
    sum_y[...] = jnp.zeros_like(sum_y)
    sum_h[...] = jnp.zeros_like(sum_h)

    def work(which, nothing):
        @pl.when(which == 0)
        def _():
            for load in near_loads:
                load.wait()

        @pl.when(which == 1)
        def _():
            for load in far_loads:
                load.wait()

        w_up, w_down_t = weights[which, 0], weights[which, 1]
        up = mm(hidden[...], w_up) + b_up[which]
        phi = 0.5 * (1.0 + lax.erf(up * (0.5**0.5)))
        active = (up * phi).astype(BF16)
        slope = phi + up * jnp.exp(-0.5 * up * up) * ((2.0 * jnp.pi) ** -0.5)
        grad_up = (mm(top[...], w_down_t) * slope).astype(BF16)
        grads[which, 1] = mm(top_t[...], active).astype(BF16)
        grads[which, 0] = mm(hidden_t[...], grad_up).astype(BF16)

        @pl.when(which == 0)
        def _():
            sends[0].start()
            sends[2].start()

        @pl.when(which == 1)
        def _():
            sends[1].start()
            sends[3].start()

        out_bu[which] = column_sum(grad_up)
        sum_y[...] += mm_t(active, w_down_t)
        sum_h[...] += mm_t(grad_up, w_up)
        return nothing

    lax.fori_loop(0, 2, work, 0)
    if last:
        middle, w_out, in_y, in_h = late_here
        chunks, _, cols = out_gc.shape
        gain = vectors[3:4, :]
        zero = jnp.zeros((1, out_y.shape[1]), F32)

        def some(span, sums):
            hat, root = norm_parts(middle[span, :])
            total_y = in_y[span, :] + sum_y[span, :]
            out_y[span, :] = (middle[span, :] + (total_y + vectors[5:6, :])).astype(BF16)
            grad_hidden = in_h[span, :] + sum_h[span, :]
            grad_top = top[span, :].astype(F32)
            grad_middle = grad_top + norm_back(grad_hidden, gain, hat, root)
            out_gm[span, :] = grad_middle
            grad_attn = grad_middle.astype(BF16)
            out_ga[span, :] = grad_attn
            fresh = grad_attn, grad_hidden * hat, grad_hidden, grad_top
            return tuple(one + column_sum(other) for one, other in zip(sums, fresh))

        sums = by_rows(out_y.shape[0], (zero,) * 4, some)
        out_sums[...] = jnp.concatenate(sums, axis=0)
        grad_attn = out_ga[...]

        def one_chunk(c, nothing):
            out_gc[c] = mm_t(grad_attn, w_out[chunk_rows(order, c, cols), :]).astype(BF16)
            return nothing

        lax.fori_loop(0, chunks, one_chunk, 0)
    for send in sends:
        send.wait()


def out_gradient(order, ctx, grad_attn, turn, out_go):
    chunks, _, cols = ctx.shape

    def one_chunk(c, nothing):
        grad_out = t_mm(ctx[c], grad_attn[...]).astype(BF16)
        out_go[chunk_rows(order, c, cols), :] = mm_t(grad_out, turn[...]).astype(BF16)
        return nothing

    lax.fori_loop(0, chunks, one_chunk, 0)


def attention_backward(
    items,
    x,
    vectors,
    qk_near,
    qk_far,
    vo_near,
    vo_far,
    query,
    key,
    value,
    probs,
    grad_ctx,
    grad_middle,
    out_x,
    gqk_near,
    gqk_far,
    gvo_near,
    gvo_far,
    out_b,
    out_sums,
    hat,
    root,
    normed_t,
    sum_n,
):
    rows = x.shape[0] // items
    cols = query.shape[2]
    heads = cols // HEAD_DIM
    scale = HEAD_DIM**-0.5
    t = pl.program_id(0)
    gain = vectors[0:1, :]

    @pl.when(t == 0)
    def _():
        def some(span, nothing):
            hat_one, root_one = norm_parts(x[span, :].astype(F32))
            hat[span, :] = hat_one
            root[span, :] = root_one
            normed_t[:, span] = (hat_one * gain + vectors[1:2, :]).T.astype(BF16)
            return nothing

        by_rows(x.shape[0], 0, some)
        sum_n[...] = jnp.zeros_like(sum_n)

    jobs = [
        (item, head, slice(item * rows, (item + 1) * rows))
        for item in range(items)
        for head in range(heads)
    ]

    def lanes(head):
        return slice(head * HEAD_DIM, (head + 1) * HEAD_DIM)

    grads_p = [
        mm_t(grad_ctx[0, mine, lanes(head)], value[0, mine, lanes(head)]) for _, head, mine in jobs
    ]
    parts_v = [
        t_mm(probs[0, item * heads + head].astype(BF16), grad_ctx[0, mine, lanes(head)])
        for item, head, mine in jobs
    ]
    grads_s = []
    for (item, head, _), grad_p in zip(jobs, grads_p):
        p = probs[0, item * heads + head]
        row = jnp.sum(p * grad_p, axis=-1, keepdims=True)
        grads_s.append((p * (grad_p - row)).astype(BF16))
    parts_q = [
        mm(grad_s, key[0, mine, lanes(head)]) * scale for (_, head, mine), grad_s in zip(jobs, grads_s)
    ]
    parts_k = [
        t_mm(grad_s, query[0, mine, lanes(head)]) * scale
        for (_, head, mine), grad_s in zip(jobs, grads_s)
    ]

    def gathered(parts):
        items_of = [
            jnp.concatenate(parts[item * heads : (item + 1) * heads], axis=1)
            for item in range(items)
        ]
        return jnp.concatenate(items_of, axis=0).astype(BF16)

    grad_all = jnp.concatenate([gathered(p) for p in (parts_q, parts_k, parts_v)], axis=1)
    out_b[0] = column_sum(grad_all)
    grad_qk, grad_v = grad_all[:, : 2 * cols], grad_all[:, 2 * cols :]
    store(t, gqk_near, gqk_far, mm(normed_t[...], grad_qk).astype(BF16))
    grad_weight = mm(normed_t[...], grad_v).astype(BF16)
    store(t, gvo_near, gvo_far, grad_weight)
    sum_n[...] += mm_t(grad_qk, nearer(t, qk_near, qk_far))
    sum_n[...] += mm_t(grad_v, nearer(t, vo_near, vo_far)[:, :cols])

    @pl.when(t == pl.num_programs(0) - 1)
    def _():
        zero = jnp.zeros((1, x.shape[1]), F32)

        def some(span, sums):
            grad_normed = sum_n[span, :]
            back = norm_back(grad_normed, gain, hat[span, :], root[span, :])
            out_x[span, :] = (grad_middle[span, :] + back).astype(BF16)
            fresh = grad_normed * hat[span, :], grad_normed
            return tuple(one + column_sum(other) for one, other in zip(sums, fresh))

        out_sums[...] = jnp.concatenate(by_rows(x.shape[0], (zero,) * 2, some), axis=0)


def call(body, grid, in_specs, outs, scratch, flops, moved, *args):
    return pl.pallas_call(
        body,
        grid=grid,
        in_specs=in_specs,
        out_specs=[o[1] for o in outs],
        out_shape=[jax.ShapeDtypeStruct(*o[0]) for o in outs],
        scratch_shapes=scratch,
        compiler_params=pltpu.CompilerParams(
            dimension_semantics=("arbitrary",) * len(grid), vmem_limit_bytes=60 * 1024 * 1024
        ),
        cost_estimate=pl.CostEstimate(flops=flops // 8, bytes_accessed=moved // 8, transcendentals=0),
    )(*args)


def local(
    n_dp,
    n_head,
    tokens,
    caption_len,
    first_gain,
    first_shift,
    qkv_weight,
    qkv_bias,
    out_weight,
    out_bias,
    second_gain,
    second_shift,
    up_weight,
    up_bias,
    down_weight,
    down_bias,
    output_grad,
):
    rows, width = tokens.shape
    hidden = up_weight.shape[1] * n_head
    devices = n_dp * n_head
    item_count = caption_len.shape[0] // n_head
    seq = rows // item_count
    dp_bits = [("dp", 1 << i) for i in reversed(range(n_dp.bit_length() - 1))]
    head_bits = [("head", 1 << i) for i in reversed(range(n_head.bit_length() - 1))]
    held = (dp_bits + head_bits)[::-1]
    along_z, along_x, along_y = dp_bits[:-1], dp_bits[-1:], head_bits[:-1]
    core = head_bits[-1]

    def flip(piece, step):
        axis, bit = step
        count = n_dp if axis == "dp" else n_head
        rows_first = Layout(tuple(range(piece.ndim)))
        piece = with_layout_constraint(piece, rows_first)
        piece = lax.ppermute(piece, axis, [(i, i ^ bit) for i in range(count)])
        return with_layout_constraint(piece, rows_first)

    def together(*values):
        return lax.optimization_barrier(values)

    def place_of(step, have):
        return sum(held.index(h) < held.index(step) for h in have)

    def grow(piece, step, have):
        other = flip(piece, step)
        piece = jnp.stack([piece, other], axis=place_of(step, have))
        have.append(step)
        return piece

    def both(step, other):
        return step[0], step[1] | other[1]

    def grow_two(piece, step, other, have):
        pieces = [piece, flip(piece, step), flip(piece, other), flip(piece, both(step, other))]
        have.extend([step, other])
        return jnp.stack(pieces).reshape((2, 2) + piece.shape)

    def side(terms, which, place):
        return [lax.index_in_dim(term, which, place, False) for term in terms]

    def total(terms):
        return sum(term.astype(F32) for term in terms)

    def shrink(terms, step, have):
        place = have.index(step)
        have.remove(step)
        away = total(side(terms, 1, place)).astype(BF16)
        return side(terms, 0, place) + [flip(away, step)]

    def reverse_bits(value, count):
        return sum(
            ((value >> i) & 1) << (count.bit_length() - 2 - i) for i in range(count.bit_length() - 1)
        )

    my_dp, my_head = lax.axis_index("dp"), lax.axis_index("head")
    order_chunks = my_head ^ reverse_bits(jnp.arange(n_head, dtype=jnp.int32), n_head)
    order_blocks = my_dp ^ reverse_bits(jnp.arange(n_dp, dtype=jnp.int32), n_dp)

    def exchange(blocks):
        return lax.all_to_all(blocks, ALL, 0, 0, tiled=True)

    per = first_gain.shape[0]
    smem = pl.BlockSpec(memory_space=pltpu.SMEM)
    pieces = [first_gain, first_shift, out_bias, second_gain, second_shift, down_bias]
    pieces += [qkv_bias[0], qkv_bias[1], up_bias]
    small_size = sum(piece.shape[0] for piece in pieces)
    smalls, start = 0, 0
    for piece in pieces:
        stop = start + piece.shape[0]
        smalls += jnp.pad(piece, (start, small_size - stop))
        start = stop
    part_rows = width // n_dp
    part_cols = width // n_head
    part_hidden = up_weight.shape[1]
    part_hidden = up_weight.shape[1]
    features = jnp.arange(width, dtype=jnp.int32)
    place = jnp.repeat(order_blocks, part_rows) * part_rows + features % part_rows
    turn = (features[:, None] == place[None, :]).astype(BF16)

    def turned(piece):
        return mm(piece, turn).astype(BF16)

    def turned_back(piece):
        return mm_t(piece, turn).astype(BF16)

    ranks = order_blocks[None, :] * n_head + order_chunks[:, None]
    ranks = ranks.reshape(-1)
    chunk_of = reverse_bits(my_head ^ jnp.arange(n_head, dtype=jnp.int32), n_head)
    block_of = reverse_bits(my_dp ^ jnp.arange(n_dp, dtype=jnp.int32), n_dp)
    ranks_back = (chunk_of[None, :] * n_dp + block_of[:, None]).reshape(-1)
    padded = -(-seq // 16) * 16
    total_rows = item_count * padded

    def pad(piece):
        piece = piece.reshape(item_count, seq, width)
        return jnp.pad(piece, ((0, 0), (0, padded - seq), (0, 0))).reshape(total_rows, width)

    def unpad(piece):
        return piece.reshape(item_count, padded, width)[:, :seq].reshape(rows, width)

    def out_pack(piece):
        return piece.reshape(-1, n_head, part_cols).transpose(1, 0, 2).reshape(part_rows, part_cols)

    have, have_rest = [], []
    first = [qkv_weight.reshape(part_rows, 3 * part_cols), out_pack(out_weight)]
    first = jnp.concatenate(first, axis=1)
    rest = jnp.concatenate([up_weight, down_weight.T])
    for step in along_z[:-2]:
        first = grow(first, step, have)
    first = grow_two(first, *along_z[-2:], have)
    x, top = turned(pad(tokens)), turned(pad(output_grad))
    smalls = exchange(jnp.broadcast_to(smalls[None], (devices,) + smalls.shape))
    first, rest, x, top, smalls = together(first, rest, x, top, smalls)

    part_cols = width // n_head
    vectors, b_qv, b_up = call(
        functools.partial(spread_vectors, per),
        (1,),
        [smem, whole(smalls.shape), whole((width, width))],
        [
            (((6, width), F32), whole((6, width))),
            (((n_head, 2, part_cols), F32), whole((n_head, 2, part_cols))),
            (((n_head, 1, hidden // n_head), F32), whole((n_head, 1, hidden // n_head))),
        ],
        [],
        0,
        4 * width * width,
        order_chunks,
        smalls,
        turn,
    )
    w_qk, w_vo = first[..., : 2 * part_cols], first[..., 2 * part_cols :]
    have_qk, have_vo = list(have), list(have)
    w_qk, w_vo = grow(w_qk, along_x[0], have_qk), grow(w_vo, along_y[0], have_vo)
    rest = grow(rest, along_z[0], have_rest)
    w_qk, w_vo, rest, vectors, b_qv, b_up = together(w_qk, w_vo, rest, vectors, b_qv, b_up)
    for step in along_z[1:-1]:
        rest = grow(rest, step, have_rest)
    for step in along_y[:-1]:
        w_qk = grow(w_qk, step, have_qk)
    for step in along_y[1:]:
        w_vo = grow(w_vo, step, have_vo)
    w_qk, w_vo = grow(w_qk, along_y[-1], have_qk), grow(w_vo, along_x[0], have_vo)
    rest = grow(rest, along_z[-1], have_rest)
    w_up, w_down = rest[..., :part_rows, :], rest[..., part_rows:, :]
    pair_shape = (-1, width, 2 * part_cols)
    near_qk, near_vo, w_up, w_down = together(
        w_qk.reshape(pair_shape), w_vo.reshape(pair_shape), w_up, w_down
    )
    far_qk, far_vo = flip(near_qk, core), flip(near_vo, core)
    step_x, step_y = along_x[0], along_y[0]
    up_x, down_x = flip(w_up, step_x), flip(w_down, step_x)
    up_y, down_y = flip(w_up, step_y), flip(w_down, step_y)


    lengths = lax.dynamic_slice_in_dim(caption_len, my_head * item_count, item_count)
    pairs = item_count * (part_cols // HEAD_DIM)

    full = (total_rows, width)
    slab = (total_rows, part_cols)
    slab_out = (((n_head,) + slab, BF16), chunk(slab))
    probs_out = (((n_head, pairs, padded, padded), F32), chunk((pairs, padded, padded)))
    weights = width * width

    half = n_head // 2

    def near(shape):
        return spec((1,) + shape, lambda t: (jnp.minimum(t, half - 1), 0, 0))

    def far(shape):
        return spec((1,) + shape, lambda t: (jnp.maximum(t - half, 0), 0, 0))

    two_cols, one_col = (width, 2 * part_cols), (width, part_cols)
    first_specs = [near(two_cols), far(two_cols)] * 2
    query, key, value, probs, context = call(
        functools.partial(attention_forward, item_count, seq),
        (n_head,),
        [smem, smem, whole(full), whole(vectors.shape)]
        + first_specs
        + [whole(b_qv.shape)],
        [slab_out, slab_out, slab_out, probs_out, slab_out],
        [pltpu.VMEM(full, BF16)],
        8 * total_rows * weights,
        12 * weights,
        lengths,
        order_chunks,
        x,
        vectors,
        near_qk,
        far_qk,
        near_vo,
        far_vo,
        b_qv,
    )

    w_out = jnp.concatenate([near_vo[..., part_cols:], far_vo[..., part_cols:]])
    w_out = w_out.reshape(devices, n_head, -1, part_cols).transpose(0, 2, 1, 3)
    w_out = w_out.reshape(devices, -1, width)
    w_out = turned(w_out[ranks_back].reshape(width, width))
    middle, low, low_t, top_t = call(
        between,
        (1,),
        [smem, whole(full), whole((n_head,) + slab), whole((width, width))]
        + [whole(vectors.shape), whole(full)],
        [
            ((full, F32), whole(full)),
            ((full, BF16), whole(full)),
            ((full[::-1], BF16), whole(full[::-1])),
            ((full[::-1], BF16), whole(full[::-1])),
        ],
        [],
        2 * total_rows * weights,
        8 * weights,
        order_chunks,
        x,
        context,
        w_out,
        vectors,
        top,
    )

    up_x, down_x, up_y, down_y, low = together(up_x, down_x, up_y, down_y, low)
    up_d, down_d = flip(up_x, step_y), flip(down_y, step_x)
    own = [w_up, up_x, w_down, down_x]
    own_far = [flip(piece, core) for piece in own]
    other = [up_y, up_d, down_y, down_d]
    early_far = [flip(piece, core) for piece in other[::2]]
    *own_far, late_0, late_1 = together(*own_far, *early_far)
    early_far = [late_0, late_1]

    def arranged(near, far):
        pieces = near[:2] + far[:2] + near[2:] + far[2:]
        return [piece.reshape(-1, part_hidden) for piece in pieces]

    b_up = b_up.reshape(2, half, 1, part_hidden)
    anywhere = pl.BlockSpec(memory_space=pl.ANY)
    strips = [anywhere] * 8
    strip_outs = [(((width, part_hidden), BF16), anywhere)] * 4
    strip_outs += [(((2, 1, part_hidden), F32), whole((2, 1, part_hidden)))]
    copied = [
        pltpu.VMEM((2, 2, width, part_hidden), BF16),
        pltpu.VMEM((2, 2, width, part_hidden), BF16),
        pltpu.SemaphoreType.DMA((12,)),
        pltpu.SemaphoreType.DMA((4,)),
    ]
    cost = 6 * total_rows * width * hidden, 10 * weights
    *g_own, gb_own, sum_y, sum_h = call(
        functools.partial(feed_forward, False),
        (1,),
        [whole(full), whole(full[::-1])] * 2 + strips + [whole((2, 1, part_hidden))],
        strip_outs + [((full, F32), whole(full))] * 2,
        copied,
        *cost,
        low,
        low_t,
        top,
        top_t,
        *arranged(own, own_far),
        b_up[:, 0],
    )
    other[1], other[3], sum_y = together(other[1], other[3], sum_y)
    late_far = [flip(piece, core) for piece in other[1::2]]
    other_far = [early_far[0], late_far[0], early_far[1], late_far[1]]

    rest_bits = held[1:]
    shape = (2,) * len(rest_bits)
    tile = (part_rows, part_hidden)

    def pair(near, far, tile):
        near = near.reshape(shape[1:] + tile)
        return [near, flip(far.reshape(near.shape), core)]

    gup_own, gdown_own = pair(*g_own[:2], tile), pair(*g_own[2:], tile)
    *g_other, gb_other, layer_out, grad_middle, grad_attn, grad_context, sums_two = call(
        functools.partial(feed_forward, True),
        (1,),
        [whole(full), whole(full[::-1])] * 2
        + strips
        + [whole((2, 1, part_hidden)), smem, whole(vectors.shape)]
        + [anywhere] * 4,
        strip_outs
        + [
            ((full, BF16), whole(full)),
            ((full, F32), whole(full)),
            ((full, BF16), whole(full)),
            (((n_head,) + slab, BF16), whole((n_head,) + slab)),
            (((4, width), F32), whole((4, width))),
        ],
        [pltpu.VMEM(full, F32)] * 2
        + copied
        + [pltpu.VMEM(full, F32), pltpu.VMEM((width, width), BF16)]
        + [pltpu.VMEM(full, F32)] * 2,
        *cost,
        low,
        low_t,
        top,
        top_t,
        *arranged(other, other_far),
        b_up[:, 1],
        order_chunks,
        vectors,
        middle,
        w_out,
        sum_y,
        sum_h,
    )
    g_bu = jnp.stack([gb_own, gb_other], axis=1).reshape(n_head, 1, part_hidden)
    gup_other, gdown_other = pair(*g_other[:2], tile), pair(*g_other[2:], tile)

    def low_total(terms):
        return total(terms).astype(BF16)

    away = [
        low_total(side(gdown_own, 1, 0)),
        low_total(side(gup_other, 1, 0)),
        low_total(side(gdown_other, 1, 0)),
        low_total(side(gup_other, 0, 0)),
    ]
    down_01, up_11 = flip(away[0], step_x), flip(away[1], step_y)
    down_11, up_10 = flip(away[2], step_x), flip(away[3], step_y)
    grad_context, *_ = together(grad_context, *away)
    tokens_grad, gqk_near, gqk_far, gvo_near, gvo_far, g_b, sums_one = call(
        functools.partial(attention_backward, item_count),
        (n_head,),
        [whole(full), whole(vectors.shape)]
        + first_specs
        + [chunk(slab)] * 3
        + [chunk((pairs, padded, padded)), chunk(slab), whole(full)],
        [
            ((full, BF16), whole(full)),
            (((half,) + two_cols, BF16), near(two_cols)),
            (((half,) + two_cols, BF16), far(two_cols)),
            (((half,) + one_col, BF16), near(one_col)),
            (((half,) + one_col, BF16), far(one_col)),
            (((n_head, 1, 3 * part_cols), F32), chunk((1, 3 * part_cols))),
            (((2, width), F32), whole((2, width))),
        ],
        [
            pltpu.VMEM(full, F32),
            pltpu.VMEM((total_rows, 1), F32),
            pltpu.VMEM(full[::-1], BF16),
            pltpu.VMEM(full, F32),
        ],
        16 * total_rows * weights,
        12 * weights,
        x,
        vectors,
        near_qk,
        far_qk,
        near_vo,
        far_vo,
        query,
        key,
        value,
        probs,
        grad_context,
        grad_middle,
    )
    two = (part_rows, 2 * part_cols)
    down_01, up_11, down_11, up_10, gqk_near, gqk_far, gvo_near, gvo_far = together(
        down_01, up_11, down_11, up_10, gqk_near, gqk_far, gvo_near, gvo_far
    )

    def pair_first(near, far):
        return [near.reshape(shape + two), flip(far.reshape(shape + two), core)]

    away_up = low_total(side(gup_own, 1, 0) + [up_11])
    away_down = low_total(side(gdown_other, 0, 0) + [down_11])
    up_01, down_10 = flip(away_up, step_x), flip(away_down, step_y)
    qk_terms = pair_first(gqk_near, gqk_far)
    grad_attn, *_ = together(grad_attn, away_up, away_down, gqk_far)
    (g_out,) = call(
        out_gradient,
        (1,),
        [smem, whole((n_head,) + slab), whole(full), whole((width, width))],
        [(((width, width), BF16), whole((width, width)))],
        [],
        0,
        0,
        order_chunks,
        context,
        grad_attn,
        turn,
    )
    g_out = g_out.reshape(devices, -1, width)[ranks]
    g_out = g_out.reshape(devices, -1, n_head, part_cols).transpose(0, 2, 1, 3)
    g_out = g_out.reshape(n_head, width, part_cols)
    gvo_near = jnp.concatenate([gvo_near, g_out[:half]], axis=2)
    gvo_far = jnp.concatenate([gvo_far, g_out[half:]], axis=2)
    up_01, down_10, gvo_near, gvo_far, *qk_terms = together(
        up_01, down_10, gvo_near, gvo_far, *qk_terms
    )
    vo_terms = pair_first(gvo_near, gvo_far)
    have_qk, have_vo = list(rest_bits), list(rest_bits)
    up_terms = side(gup_own, 0, 0) + [up_10, up_01]
    down_terms = side(gdown_own, 0, 0) + [down_01, down_10]
    have_up = list(dp_bits[:-1][::-1])

    def descend(terms, steps, have):
        for step in steps:
            terms = shrink(terms, step, have)
        return terms

    def lockstep(*chains):
        flat = together(*(chain[-1] for chain in chains))
        return [chain[:-1] + [last] for chain, last in zip(chains, flat)]

    def descend_joined(one, other, axis, step, have):
        place = have.index(step)
        have.remove(step)
        away = [total(side(terms, 1, place)).astype(BF16) for terms in (one, other)]
        near = [total(side(terms, 0, place)) for terms in (one, other)]
        away = flip(jnp.concatenate(away, axis=axis), step)
        return [jnp.concatenate(near, axis=axis).astype(BF16), away]

    qk_terms = descend(qk_terms, along_y[:1], have_qk)
    vo_terms = descend(vo_terms, along_x, have_vo)
    back_z = along_z[::-1]
    rest_terms = descend_joined(up_terms, down_terms, -2, back_z[0], have_up)
    sums_shape = (devices, small_size)
    (sums,) = call(
        functools.partial(collect_vectors, per),
        (1,),
        [smem, whole(sums_one.shape), whole(sums_two.shape), whole(g_b.shape), whole(g_bu.shape)]
        + [whole((width, width))],
        [((sums_shape, F32), whole(sums_shape))],
        [],
        0,
        4 * width * width,
        order_chunks,
        sums_one,
        sums_two,
        g_b,
        g_bu,
        turn,
    )
    layer_out = turned_back(layer_out)
    rest_terms, qk_terms, vo_terms, swapped, (layer_out,) = lockstep(
        rest_terms, qk_terms, vo_terms, [exchange(sums)], [layer_out]
    )
    qk_terms = descend(qk_terms, along_y[1:] + along_x, have_qk)
    vo_terms = descend(vo_terms, along_y, have_vo)
    rest_terms = descend(rest_terms, back_z[1:], have_up)
    layer_out = unpad(layer_out)
    tokens_grad = unpad(turned_back(tokens_grad))

    rest_terms, qk_terms, vo_terms = lockstep(rest_terms, qk_terms, vo_terms)
    chains = [qk_terms, vo_terms]
    for step in back_z[:-2]:
        chains = [descend(terms, [step], list(have_qk)) for terms in chains]
        have_qk.remove(step)

    def corner(i, j):
        return jnp.concatenate(
            [total(side(side(terms, i, 0), j, 0)) for terms in chains], axis=-1
        )

    step, other = back_z[-2:]
    first = [
        corner(0, 0),
        flip(corner(1, 1).astype(BF16), both(step, other)),
        flip(corner(1, 0).astype(BF16), step),
        flip(corner(0, 1).astype(BF16), other),
    ]
    rest = total(rest_terms)
    g_up, g_down_t = rest[:part_rows], rest[part_rows:]
    first = total(first)
    g_qkv = first[:, : 3 * part_cols].reshape(part_rows, 3, part_cols)
    g_out = first[:, 3 * part_cols :].reshape(n_head, -1, part_cols).transpose(1, 0, 2)
    g_out = g_out.reshape(out_weight.shape)
    sums = jnp.sum(swapped[0], axis=0)

    def part(index):
        return sums[index * per : (index + 1) * per]

    return (
        layer_out,
        tokens_grad,
        part(0),
        part(1),
        g_qkv,
        sums[6 * per : 8 * per].reshape(2, per),
        g_out,
        part(2),
        part(3),
        part(4),
        g_up,
        sums[8 * per :],
        g_down_t.T,
        part(5),
    )


def solution(mesh):
    n_dp, n_head = mesh.shape["dp"], mesh.shape["head"]

    def run(*args):
        return local(n_dp, n_head, *args)

    return jax.shard_map(
        run,
        mesh=mesh,
        in_specs=(
            P(ALL, None),
            P("dp"),
            P(ALL),
            P(ALL),
            P("dp", None, "head"),
            P(None, ("head", "dp")),
            P(ALL, None),
            P(ALL),
            P(ALL),
            P(ALL),
            P("dp", "head"),
            P(("head", "dp")),
            P("head", "dp"),
            P(ALL),
            P(ALL, None),
        ),
        out_specs=(
            P(ALL, None),
            P(ALL, None),
            P(ALL),
            P(ALL),
            P("dp", None, "head"),
            P(None, ("head", "dp")),
            P(ALL, None),
            P(ALL),
            P(ALL),
            P(ALL),
            P("dp", "head"),
            P(("head", "dp")),
            P("head", "dp"),
            P(ALL),
        ),
        check_vma=False,
    )
```

```python
import functools
import math

import jax
import jax.numpy as jnp
from jax import lax
from jax.experimental.layout import Layout, with_layout_constraint
from jax.experimental import pallas as pl
from jax.experimental.pallas import tpu as pltpu
from jax.sharding import PartitionSpec as P

HEAD_DIM = 64
TEXT = 40
ALL = ("dp", "head")
F32 = jnp.float32
BF16 = jnp.bfloat16


def mm(a, b):
    return jnp.dot(a, b, preferred_element_type=F32)


def mm_t(a, b):
    return lax.dot_general(a, b, (((1,), (1,)), ((), ())), preferred_element_type=F32)


def t_mm(a, b):
    return lax.dot_general(a, b, (((0,), (0,)), ((), ())), preferred_element_type=F32)


def norm_parts(values):
    spread = values - jnp.mean(values, axis=-1, keepdims=True)
    root = lax.rsqrt(jnp.mean(spread * spread, axis=-1, keepdims=True) + 1e-06)
    return spread * root, root


def norm_back(grad, gain, hat, root):
    scaled = grad * gain
    first = jnp.mean(scaled, axis=-1, keepdims=True)
    second = jnp.mean(scaled * hat, axis=-1, keepdims=True)
    return root * (scaled - first - hat * second)


VMEM = pltpu.VMEM


def spec(shape, index):
    return pl.BlockSpec(shape, index, memory_space=VMEM)


def whole(shape):
    return spec(shape, lambda *_: (0,) * len(shape))


def chunk(shape):
    return spec((1,) + shape, lambda j, *_: (j,) + (0,) * len(shape))


def nearer(t, near, far):
    return jnp.where(t < pl.num_programs(0) // 2, near[0], far[0])


def store(t, near, far, value):
    half = pl.num_programs(0) // 2

    @pl.when(t < half)
    def _():
        near[0] = value

    @pl.when(t >= half)
    def _():
        far[0] = value


def column_sum(matrix):
    return jnp.sum(matrix.astype(F32), axis=0, keepdims=True)


def counting(shape, axis):
    return lax.broadcasted_iota(jnp.int32, shape, axis)


def repeats(part, size):
    return (counting((part, size), 1) % part == counting((part, size), 0)).astype(F32)


def owners(devices, part, size):
    return counting((devices, size), 1) // part, counting((devices, size), 0)


def spread_vectors(per, order, smalls, turn, vectors, b_qv, b_up):
    devices, width = smalls.shape[0], turn.shape[0]
    chunks, _, part = b_up.shape
    values = smalls[...].astype(F32)
    plain = vectors.shape[0]
    pattern = repeats(per, width).astype(BF16)
    block, device = owners(devices, per, width)
    rows = []
    for v in range(plain):
        row = mm(values[:, v * per : (v + 1) * per].astype(BF16), pattern)
        rows.append(jnp.sum(jnp.where(block == device, row, 0.0), axis=0, keepdims=True))
    vectors[...] = mm(jnp.concatenate(rows, axis=0).astype(BF16), turn[...])

    def by_chunk(first, size, length, out):
        tall = mm(
            values[:, first : first + size].astype(BF16), repeats(size, length).astype(BF16)
        )
        block, device = owners(devices, size, length)
        for t in range(chunks):
            mine = device == block * chunks + order[t]
            out(t, jnp.sum(jnp.where(mine, tall, 0.0), axis=0, keepdims=True))

    def set_query(t, row):
        b_qv[t, 0:1, :] = row

    def set_value(t, row):
        b_qv[t, 1:2, :] = row

    def set_up(t, row):
        b_up[t] = row

    cols = b_qv.shape[2]
    by_chunk(plain * per, per, cols, set_query)
    by_chunk((plain + 1) * per, per, cols, set_value)
    by_chunk((plain + 2) * per, values.shape[1] - (plain + 2) * per, part, set_up)


def collect_vectors(per, order, sums_one, sums_two, g_b, g_bu, turn, out):
    devices, width = out.shape[0], turn.shape[0]
    chunks, _, part = g_bu.shape

    def exact(a, b):
        high = a.astype(BF16)
        left = a - high.astype(F32)
        mid = left.astype(BF16)
        low = (left - mid.astype(F32)).astype(BF16)
        count = a.shape[0]
        parts = mm_t(jnp.concatenate([part.astype(F32) for part in (high, mid, low)]).astype(BF16), b)
        return parts[:count] + (parts[count : 2 * count] + parts[2 * count :])

    plain = sums_one.shape[0] + sums_two.shape[0]
    rows = jnp.concatenate([sums_one[...], sums_two[...]], axis=0)
    rows = exact(rows, turn[...])
    block, device = owners(devices, per, width)
    tall = [jnp.where(block == device, rows[v : v + 1, :], 0.0) for v in range(plain)]
    tall = exact(jnp.concatenate(tall, axis=0), repeats(per, width).astype(BF16))
    columns = [tall[v * devices : (v + 1) * devices, :] for v in range(plain)]

    def by_chunk(row_of, size, length):
        block, device = owners(devices, size, length)
        tall = jnp.zeros((devices, length), F32)
        for t in range(chunks):
            tall = jnp.where(device == block * chunks + order[t], row_of(t), tall)
        columns.append(exact(tall, repeats(size, length).astype(BF16)))

    cols = g_b.shape[2] // 3
    by_chunk(lambda t: g_b[t][:, :cols], per, cols)
    by_chunk(lambda t: g_b[t][:, 2 * cols :], per, cols)
    by_chunk(lambda t: g_bu[t], out.shape[2] - (plain + 2) * per, part)
    out[:, 0, :] = jnp.concatenate(columns, axis=1)


def attention_forward(
    items,
    seq,
    lengths,
    order,
    x,
    vectors,
    qk_near,
    qk_far,
    vo_near,
    vo_far,
    b_qv,
    out_q,
    out_k,
    out_v,
    out_p,
    out_c,
    normed,
):
    t = pl.program_id(0)
    rows = x.shape[0] // items
    cols = out_q.shape[2]
    scale = HEAD_DIM**-0.5

    @pl.when(t == 0)
    def _():
        def some(span, nothing):
            hat, _ = norm_parts(x[span, :].astype(F32))
            normed[span, :] = (hat * vectors[0:1, :] + vectors[1:2, :]).astype(BF16)
            return nothing

        by_rows(x.shape[0], 0, some)

    bias = b_qv[t]
    both = mm(normed[...], nearer(t, qk_near, qk_far))
    query = (both[:, :cols] + bias[0:1, :]).astype(BF16)
    key = both[:, cols:].astype(BF16)
    value = (mm(normed[...], nearer(t, vo_near, vo_far)[:, :cols]) + bias[1:2, :]).astype(BF16)
    out_q[0] = query
    out_k[0] = key
    out_v[0] = value
    heads = cols // HEAD_DIM
    at = lax.broadcasted_iota(jnp.int32, (rows, rows), 1)
    jobs = [
        (item, head, slice(item * rows, (item + 1) * rows))
        for item in range(items)
        for head in range(heads)
    ]
    visible = [((at >= TEXT) & (at < seq)) | (at < lengths[item]) for item in range(items)]

    def lanes(head):
        return slice(head * HEAD_DIM, (head + 1) * HEAD_DIM)

    scores = [
        mm_t(query[mine, lanes(head)], key[mine, lanes(head)]) * scale for _, head, mine in jobs
    ]
    parts = []
    for (item, head, _), score in zip(jobs, scores):
        score = jnp.where(visible[item], score, -1000000000.0)
        raised = jnp.exp(score - jnp.max(score, axis=-1, keepdims=True))
        probs = raised / jnp.sum(raised, axis=-1, keepdims=True)
        out_p[0, item * heads + head] = probs
        parts.append(probs.astype(BF16))
    parts = [mm(low, value[mine, lanes(head)]) for (_, head, mine), low in zip(jobs, parts)]
    for item in range(items):
        mine = slice(item * rows, (item + 1) * rows)
        whole_item = jnp.concatenate(parts[item * heads : (item + 1) * heads], axis=1)
        out_c[0, mine, :] = whole_item.astype(BF16)


def by_rows(count, carry, body):
    part = math.gcd(count, 128)

    def one(i, carry):
        return body(pl.ds(pl.multiple_of(i * part, part), part), carry)

    return lax.fori_loop(0, count // part, one, carry)


def chunk_rows(order, c, cols):
    return pl.ds(pl.multiple_of(order[c] * cols, cols), cols)


def between(order, x, ctx, w_out, vectors, top, middle, hidden, hidden_t, top_t):
    chunks, _, cols = ctx.shape
    total = x[...].astype(F32) + vectors[2:3, :]
    for c in range(chunks):
        total += mm(ctx[c], w_out[chunk_rows(order, c, cols), :])
    middle[...] = total

    def some(span, nothing):
        hat, _ = norm_parts(middle[span, :])
        low = hat * vectors[3:4, :] + vectors[4:5, :]
        hidden[span, :] = low.astype(BF16)
        hidden_t[:, span] = low.T.astype(BF16)
        top_t[:, span] = top[span, :].astype(F32).T.astype(BF16)
        return nothing

    by_rows(x.shape[0], 0, some)


def feed_forward(last, hidden, hidden_t, top, top_t, *rest):
    ups, downs, b_up, rest = rest[:4], rest[4:8], rest[8], rest[9:]
    late = []
    if last:
        order, vectors, *late = rest[:6]
        rest = rest[6:]
    grads_out, out_bu, rest = rest[:4], rest[4], rest[5:]
    if last:
        out_y, out_gm, out_ga, out_gc, out_sums, *rest = rest
    sum_y, sum_h, weights, grads, in_sems, out_sems, *late_here = rest
    half = weights.shape[2] // 2

    loads = []
    for i, piece in enumerate(ups + downs):
        here = weights.at[i // 2 % 2, i // 4, pl.ds(i % 2 * half, half)]
        loads.append(pltpu.make_async_copy(piece, here, in_sems.at[i]))
    for i, (piece, here) in enumerate(zip(late, late_here)):
        loads.append(pltpu.make_async_copy(piece, here, in_sems.at[8 + i]))
    near_loads = loads[:2] + loads[4:6]
    far_loads = loads[2:4] + loads[6:]
    for load in near_loads + far_loads:
        load.start()
    sends = [
        pltpu.make_async_copy(grads.at[i % 2, i // 2], grads_out[i], out_sems.at[i])
        for i in range(4)
    ]
    sum_y[...] = jnp.zeros_like(sum_y)
    sum_h[...] = jnp.zeros_like(sum_h)

    def work(which, nothing):
        @pl.when(which == 0)
        def _():
            for load in near_loads:
                load.wait()

        @pl.when(which == 1)
        def _():
            for load in far_loads:
                load.wait()

        w_up, w_down_t = weights[which, 0], weights[which, 1]
        up = mm(hidden[...], w_up) + b_up[which]
        phi = 0.5 * (1.0 + lax.erf(up * (0.5**0.5)))
        active = (up * phi).astype(BF16)
        slope = phi + up * jnp.exp(-0.5 * up * up) * ((2.0 * jnp.pi) ** -0.5)
        grad_up = (mm(top[...], w_down_t) * slope).astype(BF16)
        grads[which, 1] = mm(top_t[...], active).astype(BF16)
        grads[which, 0] = mm(hidden_t[...], grad_up).astype(BF16)

        @pl.when(which == 0)
        def _():
            sends[0].start()
            sends[2].start()

        @pl.when(which == 1)
        def _():
            sends[1].start()
            sends[3].start()

        out_bu[which] = column_sum(grad_up)
        sum_y[...] += mm_t(active, w_down_t)
        sum_h[...] += mm_t(grad_up, w_up)
        return nothing

    lax.fori_loop(0, 2, work, 0)
    if last:
        middle, w_out, in_y, in_h = late_here
        chunks, _, cols = out_gc.shape
        gain = vectors[3:4, :]
        zero = jnp.zeros((1, out_y.shape[1]), F32)

        def some(span, sums):
            hat, root = norm_parts(middle[span, :])
            total_y = in_y[span, :] + sum_y[span, :]
            out_y[span, :] = (middle[span, :] + (total_y + vectors[5:6, :])).astype(BF16)
            grad_hidden = in_h[span, :] + sum_h[span, :]
            grad_top = top[span, :].astype(F32)
            grad_middle = grad_top + norm_back(grad_hidden, gain, hat, root)
            out_gm[span, :] = grad_middle
            grad_attn = grad_middle.astype(BF16)
            out_ga[span, :] = grad_attn
            fresh = grad_attn, grad_hidden * hat, grad_hidden, grad_top
            return tuple(one + column_sum(other) for one, other in zip(sums, fresh))

        sums = by_rows(out_y.shape[0], (zero,) * 4, some)
        out_sums[...] = jnp.concatenate(sums, axis=0)
        grad_attn = out_ga[...]

        def one_chunk(c, nothing):
            out_gc[c] = mm_t(grad_attn, w_out[chunk_rows(order, c, cols), :]).astype(BF16)
            return nothing

        lax.fori_loop(0, chunks, one_chunk, 0)
    for send in sends:
        send.wait()


def out_gradient(order, ctx, grad_attn, turn, out_go):
    chunks, _, cols = ctx.shape

    def one_chunk(c, nothing):
        grad_out = t_mm(ctx[c], grad_attn[...]).astype(BF16)
        out_go[chunk_rows(order, c, cols), :] = mm_t(grad_out, turn[...]).astype(BF16)
        return nothing

    lax.fori_loop(0, chunks, one_chunk, 0)


def attention_backward(
    items,
    x,
    vectors,
    qk_near,
    qk_far,
    vo_near,
    vo_far,
    query,
    key,
    value,
    probs,
    grad_ctx,
    grad_middle,
    out_x,
    gqk_near,
    gqk_far,
    gvo_near,
    gvo_far,
    out_b,
    out_sums,
    hat,
    root,
    normed_t,
    sum_n,
):
    rows = x.shape[0] // items
    cols = query.shape[2]
    heads = cols // HEAD_DIM
    scale = HEAD_DIM**-0.5
    t = pl.program_id(0)
    gain = vectors[0:1, :]

    @pl.when(t == 0)
    def _():
        def some(span, nothing):
            hat_one, root_one = norm_parts(x[span, :].astype(F32))
            hat[span, :] = hat_one
            root[span, :] = root_one
            normed_t[:, span] = (hat_one * gain + vectors[1:2, :]).T.astype(BF16)
            return nothing

        by_rows(x.shape[0], 0, some)
        sum_n[...] = jnp.zeros_like(sum_n)

    jobs = [
        (item, head, slice(item * rows, (item + 1) * rows))
        for item in range(items)
        for head in range(heads)
    ]

    def lanes(head):
        return slice(head * HEAD_DIM, (head + 1) * HEAD_DIM)

    grads_p = [
        mm_t(grad_ctx[0, mine, lanes(head)], value[0, mine, lanes(head)]) for _, head, mine in jobs
    ]
    parts_v = [
        t_mm(probs[0, item * heads + head].astype(BF16), grad_ctx[0, mine, lanes(head)])
        for item, head, mine in jobs
    ]
    grads_s = []
    for (item, head, _), grad_p in zip(jobs, grads_p):
        p = probs[0, item * heads + head]
        row = jnp.sum(p * grad_p, axis=-1, keepdims=True)
        grads_s.append((p * (grad_p - row)).astype(BF16))
    parts_q = [
        mm(grad_s, key[0, mine, lanes(head)]) * scale for (_, head, mine), grad_s in zip(jobs, grads_s)
    ]
    parts_k = [
        t_mm(grad_s, query[0, mine, lanes(head)]) * scale
        for (_, head, mine), grad_s in zip(jobs, grads_s)
    ]

    def gathered(parts):
        items_of = [
            jnp.concatenate(parts[item * heads : (item + 1) * heads], axis=1)
            for item in range(items)
        ]
        return jnp.concatenate(items_of, axis=0).astype(BF16)

    grad_all = jnp.concatenate([gathered(p) for p in (parts_q, parts_k, parts_v)], axis=1)
    out_b[0] = column_sum(grad_all)
    grad_qk, grad_v = grad_all[:, : 2 * cols], grad_all[:, 2 * cols :]
    store(t, gqk_near, gqk_far, mm(normed_t[...], grad_qk).astype(BF16))
    grad_weight = mm(normed_t[...], grad_v).astype(BF16)
    store(t, gvo_near, gvo_far, grad_weight)
    sum_n[...] += mm_t(grad_qk, nearer(t, qk_near, qk_far))
    sum_n[...] += mm_t(grad_v, nearer(t, vo_near, vo_far)[:, :cols])

    @pl.when(t == pl.num_programs(0) - 1)
    def _():
        zero = jnp.zeros((1, x.shape[1]), F32)

        def some(span, sums):
            grad_normed = sum_n[span, :]
            back = norm_back(grad_normed, gain, hat[span, :], root[span, :])
            out_x[span, :] = (grad_middle[span, :] + back).astype(BF16)
            fresh = grad_normed * hat[span, :], grad_normed
            return tuple(one + column_sum(other) for one, other in zip(sums, fresh))

        out_sums[...] = jnp.concatenate(by_rows(x.shape[0], (zero,) * 2, some), axis=0)


def call(body, grid, in_specs, outs, scratch, flops, moved, *args):
    return pl.pallas_call(
        body,
        grid=grid,
        in_specs=in_specs,
        out_specs=[o[1] for o in outs],
        out_shape=[jax.ShapeDtypeStruct(*o[0]) for o in outs],
        scratch_shapes=scratch,
        compiler_params=pltpu.CompilerParams(
            dimension_semantics=("arbitrary",) * len(grid), vmem_limit_bytes=60 * 1024 * 1024
        ),
        cost_estimate=pl.CostEstimate(flops=flops // 8, bytes_accessed=moved // 8, transcendentals=0),
    )(*args)


def local(
    n_dp,
    n_head,
    tokens,
    caption_len,
    first_gain,
    first_shift,
    qkv_weight,
    qkv_bias,
    out_weight,
    out_bias,
    second_gain,
    second_shift,
    up_weight,
    up_bias,
    down_weight,
    down_bias,
    output_grad,
):
    rows, width = tokens.shape
    hidden = up_weight.shape[1] * n_head
    devices = n_dp * n_head
    item_count = caption_len.shape[0] // n_head
    seq = rows // item_count
    dp_bits = [("dp", 1 << i) for i in reversed(range(n_dp.bit_length() - 1))]
    head_bits = [("head", 1 << i) for i in reversed(range(n_head.bit_length() - 1))]
    held = (dp_bits + head_bits)[::-1]
    along_z, along_x, along_y = dp_bits[:-1], dp_bits[-1:], head_bits[:-1]
    core = head_bits[-1]

    def flip(piece, step):
        axis, bit = step
        count = n_dp if axis == "dp" else n_head
        rows_first = Layout(tuple(range(piece.ndim)))
        piece = with_layout_constraint(piece, rows_first)
        piece = lax.ppermute(piece, axis, [(i, i ^ bit) for i in range(count)])
        return with_layout_constraint(piece, rows_first)

    def together(*values):
        return lax.optimization_barrier(values)

    def place_of(step, have):
        return sum(held.index(h) < held.index(step) for h in have)

    def grow(piece, step, have):
        other = flip(piece, step)
        piece = jnp.stack([piece, other], axis=place_of(step, have))
        have.append(step)
        return piece

    def both(step, other):
        return step[0], step[1] | other[1]

    def grow_two(piece, step, other, have):
        pieces = [piece, flip(piece, step), flip(piece, other), flip(piece, both(step, other))]
        have.extend([step, other])
        return jnp.stack(pieces).reshape((2, 2) + piece.shape)

    def side(terms, which, place):
        return [lax.index_in_dim(term, which, place, False) for term in terms]

    def total(terms):
        return sum(term.astype(F32) for term in terms)

    def shrink(terms, step, have):
        place = have.index(step)
        have.remove(step)
        away = total(side(terms, 1, place)).astype(BF16)
        return side(terms, 0, place) + [flip(away, step)]

    def reverse_bits(value, count):
        return sum(
            ((value >> i) & 1) << (count.bit_length() - 2 - i) for i in range(count.bit_length() - 1)
        )

    my_dp, my_head = lax.axis_index("dp"), lax.axis_index("head")
    order_chunks = my_head ^ reverse_bits(jnp.arange(n_head, dtype=jnp.int32), n_head)
    order_blocks = my_dp ^ reverse_bits(jnp.arange(n_dp, dtype=jnp.int32), n_dp)

    def exchange(blocks):
        return lax.all_to_all(blocks, ALL, 0, 0, tiled=True)

    per = first_gain.shape[0]
    smem = pl.BlockSpec(memory_space=pltpu.SMEM)
    pieces = [first_gain, first_shift, out_bias, second_gain, second_shift, down_bias]
    pieces += [qkv_bias[0], qkv_bias[1], up_bias]
    small_size = sum(piece.shape[0] for piece in pieces)
    smalls, start = 0, 0
    for piece in pieces:
        stop = start + piece.shape[0]
        smalls += jnp.pad(piece, (start, small_size - stop))
        start = stop
    part_rows = width // n_dp
    part_cols = width // n_head
    part_hidden = up_weight.shape[1]
    part_hidden = up_weight.shape[1]
    features = jnp.arange(width, dtype=jnp.int32)
    place = jnp.repeat(order_blocks, part_rows) * part_rows + features % part_rows
    turn = (features[:, None] == place[None, :]).astype(BF16)

    def turned(piece):
        return mm(piece, turn).astype(BF16)

    def turned_back(piece):
        return mm_t(piece, turn).astype(BF16)

    ranks = order_blocks[None, :] * n_head + order_chunks[:, None]
    ranks = ranks.reshape(-1)
    chunk_of = reverse_bits(my_head ^ jnp.arange(n_head, dtype=jnp.int32), n_head)
    block_of = reverse_bits(my_dp ^ jnp.arange(n_dp, dtype=jnp.int32), n_dp)
    ranks_back = (chunk_of[None, :] * n_dp + block_of[:, None]).reshape(-1)
    padded = -(-seq // 16) * 16
    total_rows = item_count * padded

    def pad(piece):
        piece = piece.reshape(item_count, seq, width)
        return jnp.pad(piece, ((0, 0), (0, padded - seq), (0, 0))).reshape(total_rows, width)

    def unpad(piece):
        return piece.reshape(item_count, padded, width)[:, :seq].reshape(rows, width)

    def out_pack(piece):
        return piece.reshape(-1, n_head, part_cols).transpose(1, 0, 2).reshape(part_rows, part_cols)

    have, have_rest = [], []
    first = [qkv_weight.reshape(part_rows, 3 * part_cols), out_pack(out_weight)]
    first = jnp.concatenate(first, axis=1)
    rest = jnp.concatenate([up_weight, down_weight.T])
    for step in along_z[:-2]:
        first = grow(first, step, have)
    first = grow_two(first, *along_z[-2:], have)
    x, top = turned(pad(tokens)), turned(pad(output_grad))
    smalls = exchange(jnp.broadcast_to(smalls[None], (devices,) + smalls.shape))
    first, rest, x, top, smalls = together(first, rest, x, top, smalls)

    part_cols = width // n_head
    vectors, b_qv, b_up = call(
        functools.partial(spread_vectors, per),
        (1,),
        [smem, whole(smalls.shape), whole((width, width))],
        [
            (((6, width), F32), whole((6, width))),
            (((n_head, 2, part_cols), F32), whole((n_head, 2, part_cols))),
            (((n_head, 1, hidden // n_head), F32), whole((n_head, 1, hidden // n_head))),
        ],
        [],
        0,
        4 * width * width,
        order_chunks,
        smalls,
        turn,
    )
    w_qk, w_vo = first[..., : 2 * part_cols], first[..., 2 * part_cols :]
    have_qk, have_vo = list(have), list(have)
    w_qk, w_vo = grow(w_qk, along_x[0], have_qk), grow(w_vo, along_y[0], have_vo)
    rest = grow(rest, along_z[0], have_rest)
    w_qk, w_vo, rest, vectors, b_qv, b_up = together(w_qk, w_vo, rest, vectors, b_qv, b_up)
    for step in along_z[1:-1]:
        rest = grow(rest, step, have_rest)
    for step in along_y[:-1]:
        w_qk = grow(w_qk, step, have_qk)
    for step in along_y[1:]:
        w_vo = grow(w_vo, step, have_vo)
    w_qk, w_vo = grow(w_qk, along_y[-1], have_qk), grow(w_vo, along_x[0], have_vo)
    rest = grow(rest, along_z[-1], have_rest)
    w_up, w_down = rest[..., :part_rows, :], rest[..., part_rows:, :]
    pair_shape = (-1, width, 2 * part_cols)
    near_qk, near_vo, w_up, w_down = together(
        w_qk.reshape(pair_shape), w_vo.reshape(pair_shape), w_up, w_down
    )
    far_qk, far_vo = flip(near_qk, core), flip(near_vo, core)
    step_x, step_y = along_x[0], along_y[0]
    up_x, down_x = flip(w_up, step_x), flip(w_down, step_x)
    up_y, down_y = flip(w_up, step_y), flip(w_down, step_y)


    lengths = lax.dynamic_slice_in_dim(caption_len, my_head * item_count, item_count)
    pairs = item_count * (part_cols // HEAD_DIM)

    full = (total_rows, width)
    slab = (total_rows, part_cols)
    slab_out = (((n_head,) + slab, BF16), chunk(slab))
    probs_out = (((n_head, pairs, padded, padded), F32), chunk((pairs, padded, padded)))
    weights = width * width

    half = n_head // 2

    def near(shape):
        return spec((1,) + shape, lambda t: (jnp.minimum(t, half - 1), 0, 0))

    def far(shape):
        return spec((1,) + shape, lambda t: (jnp.maximum(t - half, 0), 0, 0))

    two_cols, one_col = (width, 2 * part_cols), (width, part_cols)
    first_specs = [near(two_cols), far(two_cols)] * 2
    query, key, value, probs, context = call(
        functools.partial(attention_forward, item_count, seq),
        (n_head,),
        [smem, smem, whole(full), whole(vectors.shape)]
        + first_specs
        + [whole(b_qv.shape)],
        [slab_out, slab_out, slab_out, probs_out, slab_out],
        [pltpu.VMEM(full, BF16)],
        8 * total_rows * weights,
        12 * weights,
        lengths,
        order_chunks,
        x,
        vectors,
        near_qk,
        far_qk,
        near_vo,
        far_vo,
        b_qv,
    )

    w_out = jnp.concatenate([near_vo[..., part_cols:], far_vo[..., part_cols:]])
    w_out = w_out.reshape(devices, n_head, -1, part_cols).transpose(0, 2, 1, 3)
    w_out = w_out.reshape(devices, -1, width)
    w_out = turned(w_out[ranks_back].reshape(width, width))
    middle, low, low_t, top_t = call(
        between,
        (1,),
        [smem, whole(full), whole((n_head,) + slab), whole((width, width))]
        + [whole(vectors.shape), whole(full)],
        [
            ((full, F32), whole(full)),
            ((full, BF16), whole(full)),
            ((full[::-1], BF16), whole(full[::-1])),
            ((full[::-1], BF16), whole(full[::-1])),
        ],
        [],
        2 * total_rows * weights,
        8 * weights,
        order_chunks,
        x,
        context,
        w_out,
        vectors,
        top,
    )

    up_x, down_x, up_y, down_y, low = together(up_x, down_x, up_y, down_y, low)
    up_d, down_d = flip(up_x, step_y), flip(down_y, step_x)
    own = [w_up, up_x, w_down, down_x]
    own_far = [flip(piece, core) for piece in own]
    other = [up_y, up_d, down_y, down_d]
    early_far = [flip(piece, core) for piece in other[::2]]
    *own_far, late_0, late_1 = together(*own_far, *early_far)
    early_far = [late_0, late_1]

    def arranged(near, far):
        pieces = near[:2] + far[:2] + near[2:] + far[2:]
        return [piece.reshape(-1, part_hidden) for piece in pieces]

    b_up = b_up.reshape(2, half, 1, part_hidden)
    anywhere = pl.BlockSpec(memory_space=pl.ANY)
    strips = [anywhere] * 8
    strip_outs = [(((width, part_hidden), BF16), anywhere)] * 4
    strip_outs += [(((2, 1, part_hidden), F32), whole((2, 1, part_hidden)))]
    copied = [
        pltpu.VMEM((2, 2, width, part_hidden), BF16),
        pltpu.VMEM((2, 2, width, part_hidden), BF16),
        pltpu.SemaphoreType.DMA((12,)),
        pltpu.SemaphoreType.DMA((4,)),
    ]
    cost = 6 * total_rows * width * hidden, 10 * weights
    *g_own, gb_own, sum_y, sum_h = call(
        functools.partial(feed_forward, False),
        (1,),
        [whole(full), whole(full[::-1])] * 2 + strips + [whole((2, 1, part_hidden))],
        strip_outs + [((full, F32), whole(full))] * 2,
        copied,
        *cost,
        low,
        low_t,
        top,
        top_t,
        *arranged(own, own_far),
        b_up[:, 0],
    )
    other[1], other[3], sum_y = together(other[1], other[3], sum_y)
    late_far = [flip(piece, core) for piece in other[1::2]]
    other_far = [early_far[0], late_far[0], early_far[1], late_far[1]]

    rest_bits = held[1:]
    shape = (2,) * len(rest_bits)
    tile = (part_rows, part_hidden)

    def pair(near, far, tile):
        near = near.reshape(shape[1:] + tile)
        return [near, flip(far.reshape(near.shape), core)]

    gup_own, gdown_own = pair(*g_own[:2], tile), pair(*g_own[2:], tile)
    *g_other, gb_other, layer_out, grad_middle, grad_attn, grad_context, sums_two = call(
        functools.partial(feed_forward, True),
        (1,),
        [whole(full), whole(full[::-1])] * 2
        + strips
        + [whole((2, 1, part_hidden)), smem, whole(vectors.shape)]
        + [anywhere] * 4,
        strip_outs
        + [
            ((full, BF16), whole(full)),
            ((full, F32), whole(full)),
            ((full, BF16), whole(full)),
            (((n_head,) + slab, BF16), whole((n_head,) + slab)),
            (((4, width), F32), whole((4, width))),
        ],
        [pltpu.VMEM(full, F32)] * 2
        + copied
        + [pltpu.VMEM(full, F32), pltpu.VMEM((width, width), BF16)]
        + [pltpu.VMEM(full, F32)] * 2,
        *cost,
        low,
        low_t,
        top,
        top_t,
        *arranged(other, other_far),
        b_up[:, 1],
        order_chunks,
        vectors,
        middle,
        w_out,
        sum_y,
        sum_h,
    )
    g_bu = jnp.stack([gb_own, gb_other], axis=1).reshape(n_head, 1, part_hidden)
    gup_other, gdown_other = pair(*g_other[:2], tile), pair(*g_other[2:], tile)

    def low_total(terms):
        return total(terms).astype(BF16)

    away = [
        low_total(side(gdown_own, 1, 0)),
        low_total(side(gup_other, 1, 0)),
        low_total(side(gdown_other, 1, 0)),
        low_total(side(gup_other, 0, 0)),
    ]
    down_01, up_11 = flip(away[0], step_x), flip(away[1], step_y)
    down_11, up_10 = flip(away[2], step_x), flip(away[3], step_y)
    grad_context, *_ = together(grad_context, *away)
    tokens_grad, gqk_near, gqk_far, gvo_near, gvo_far, g_b, sums_one = call(
        functools.partial(attention_backward, item_count),
        (n_head,),
        [whole(full), whole(vectors.shape)]
        + first_specs
        + [chunk(slab)] * 3
        + [chunk((pairs, padded, padded)), chunk(slab), whole(full)],
        [
            ((full, BF16), whole(full)),
            (((half,) + two_cols, BF16), near(two_cols)),
            (((half,) + two_cols, BF16), far(two_cols)),
            (((half,) + one_col, BF16), near(one_col)),
            (((half,) + one_col, BF16), far(one_col)),
            (((n_head, 1, 3 * part_cols), F32), chunk((1, 3 * part_cols))),
            (((2, width), F32), whole((2, width))),
        ],
        [
            pltpu.VMEM(full, F32),
            pltpu.VMEM((total_rows, 1), F32),
            pltpu.VMEM(full[::-1], BF16),
            pltpu.VMEM(full, F32),
        ],
        16 * total_rows * weights,
        12 * weights,
        x,
        vectors,
        near_qk,
        far_qk,
        near_vo,
        far_vo,
        query,
        key,
        value,
        probs,
        grad_context,
        grad_middle,
    )
    two = (part_rows, 2 * part_cols)
    down_01, up_11, down_11, up_10, gqk_near, gqk_far, gvo_near, gvo_far = together(
        down_01, up_11, down_11, up_10, gqk_near, gqk_far, gvo_near, gvo_far
    )

    def pair_first(near, far):
        return [near.reshape(shape + two), flip(far.reshape(shape + two), core)]

    away_up = low_total(side(gup_own, 1, 0) + [up_11])
    away_down = low_total(side(gdown_other, 0, 0) + [down_11])
    up_01, down_10 = flip(away_up, step_x), flip(away_down, step_y)
    qk_terms = pair_first(gqk_near, gqk_far)
    grad_attn, *_ = together(grad_attn, away_up, away_down, gqk_far)
    (g_out,) = call(
        out_gradient,
        (1,),
        [smem, whole((n_head,) + slab), whole(full), whole((width, width))],
        [(((width, width), BF16), whole((width, width)))],
        [],
        0,
        0,
        order_chunks,
        context,
        grad_attn,
        turn,
    )
    g_out = g_out.reshape(devices, -1, width)[ranks]
    g_out = g_out.reshape(devices, -1, n_head, part_cols).transpose(0, 2, 1, 3)
    g_out = g_out.reshape(n_head, width, part_cols)
    gvo_near = jnp.concatenate([gvo_near, g_out[:half]], axis=2)
    gvo_far = jnp.concatenate([gvo_far, g_out[half:]], axis=2)
    up_01, down_10, gvo_near, gvo_far, *qk_terms = together(
        up_01, down_10, gvo_near, gvo_far, *qk_terms
    )
    vo_terms = pair_first(gvo_near, gvo_far)
    have_qk, have_vo = list(rest_bits), list(rest_bits)
    up_terms = side(gup_own, 0, 0) + [up_10, up_01]
    down_terms = side(gdown_own, 0, 0) + [down_01, down_10]
    have_up = list(dp_bits[:-1][::-1])

    def descend(terms, steps, have):
        for step in steps:
            terms = shrink(terms, step, have)
        return terms

    def lockstep(*chains):
        flat = together(*(chain[-1] for chain in chains))
        return [chain[:-1] + [last] for chain, last in zip(chains, flat)]

    def descend_joined(one, other, axis, step, have):
        place = have.index(step)
        have.remove(step)
        away = [total(side(terms, 1, place)).astype(BF16) for terms in (one, other)]
        near = [total(side(terms, 0, place)) for terms in (one, other)]
        away = flip(jnp.concatenate(away, axis=axis), step)
        return [jnp.concatenate(near, axis=axis).astype(BF16), away]

    qk_terms = descend(qk_terms, along_y[:1], have_qk)
    vo_terms = descend(vo_terms, along_x, have_vo)
    back_z = along_z[::-1]
    pair_ud = [up_terms, down_terms]
    for step in back_z[:-2]:
        pair_ud = [descend(terms, [step], list(have_up)) for terms in pair_ud]
        have_up.remove(step)

    def rest_corner(i, j):
        return jnp.concatenate(
            [total(side(side(terms, i, 0), j, 0)) for terms in pair_ud], axis=-2
        )

    step, other = back_z[-2:]
    rest_terms = [
        rest_corner(0, 0),
        flip(rest_corner(1, 1).astype(BF16), both(step, other)),
        flip(rest_corner(1, 0).astype(BF16), step),
        flip(rest_corner(0, 1).astype(BF16), other),
    ]
    sums_shape = (devices, 1, small_size)
    (sums,) = call(
        functools.partial(collect_vectors, per),
        (1,),
        [smem, whole(sums_one.shape), whole(sums_two.shape), whole(g_b.shape), whole(g_bu.shape)]
        + [whole((width, width))],
        [((sums_shape, F32), whole(sums_shape))],
        [],
        0,
        4 * width * width,
        order_chunks,
        sums_one,
        sums_two,
        g_b,
        g_bu,
        turn,
    )
    layer_out = turned_back(layer_out)
    qk_terms, vo_terms, swapped, (layer_out,) = lockstep(
        qk_terms, vo_terms, [exchange(sums)], [layer_out]
    )
    swapped = swapped[0]
    qk_terms = descend(qk_terms, along_y[1:] + along_x, have_qk)
    vo_terms = descend(vo_terms, along_y, have_vo)
    layer_out = unpad(layer_out)
    tokens_grad = unpad(turned_back(tokens_grad))

    rest_terms[1], rest_terms[2], rest_terms[3], qk_terms[-1], vo_terms[-1] = together(
        *rest_terms[1:], qk_terms[-1], vo_terms[-1]
    )
    chains = [qk_terms, vo_terms]
    for step in back_z[:-2]:
        chains = [descend(terms, [step], list(have_qk)) for terms in chains]
        have_qk.remove(step)

    def corner(i, j):
        return jnp.concatenate(
            [total(side(side(terms, i, 0), j, 0)) for terms in chains], axis=-1
        )

    step, other = back_z[-2:]
    first = [
        corner(0, 0),
        flip(corner(1, 1).astype(BF16), both(step, other)),
        flip(corner(1, 0).astype(BF16), step),
        flip(corner(0, 1).astype(BF16), other),
    ]
    rest = total(rest_terms)
    g_up, g_down_t = rest[:part_rows], rest[part_rows:]
    first = total(first)
    g_qkv = first[:, : 3 * part_cols].reshape(part_rows, 3, part_cols)
    g_out = first[:, 3 * part_cols :].reshape(n_head, -1, part_cols).transpose(1, 0, 2)
    g_out = g_out.reshape(out_weight.shape)
    sums = jnp.sum(swapped, axis=0)[0]

    def part(index):
        return sums[index * per : (index + 1) * per]

    return (
        layer_out,
        tokens_grad,
        part(0),
        part(1),
        g_qkv,
        sums[6 * per : 8 * per].reshape(2, per),
        g_out,
        part(2),
        part(3),
        part(4),
        g_up,
        sums[8 * per :],
        g_down_t.T,
        part(5),
    )


def solution(mesh):
    n_dp, n_head = mesh.shape["dp"], mesh.shape["head"]

    def run(*args):
        return local(n_dp, n_head, *args)

    return jax.shard_map(
        run,
        mesh=mesh,
        in_specs=(
            P(ALL, None),
            P("dp"),
            P(ALL),
            P(ALL),
            P("dp", None, "head"),
            P(None, ("head", "dp")),
            P(ALL, None),
            P(ALL),
            P(ALL),
            P(ALL),
            P("dp", "head"),
            P(("head", "dp")),
            P("head", "dp"),
            P(ALL),
            P(ALL, None),
        ),
        out_specs=(
            P(ALL, None),
            P(ALL, None),
            P(ALL),
            P(ALL),
            P("dp", None, "head"),
            P(None, ("head", "dp")),
            P(ALL, None),
            P(ALL),
            P(ALL),
            P(ALL),
            P("dp", "head"),
            P(("head", "dp")),
            P("head", "dp"),
            P(ALL),
        ),
        check_vma=False,
    )
```
